16 devices in a mesh: dp: 4 (over z, y), tp: 4 (over x, core).
Axes of the slice: x: 2, y: 2, z: 2, core: 2. Of those that a mesh axis runs over, the one named last changes fastest.
Arguments:
- hidden: bfloat16 [512, 2048], P('dp'), parts along dimension 0
- seq_lens: int32 [512], P('dp'), parts along dimension 0
- k_cache: bfloat16 [2, 512, 256, 8, 64], P(None, 'dp', None, 'tp'), parts along dimension 1
- v_cache: bfloat16 [2, 512, 256, 8, 64], P(None, 'dp', None, 'tp'), parts along dimension 1
- g_attn: bfloat16 [2, 2048], replicated
- w_q: bfloat16 [2, 2048, 2048], P(None, None, 'tp')
- w_k: bfloat16 [2, 2048, 512], P(None, None, 'tp')
- w_v: bfloat16 [2, 2048, 512], P(None, None, 'tp')
- w_o: bfloat16 [2, 2048, 2048], P(None, 'tp')
- g_mlp: bfloat16 [2, 2048], replicated
- w_gate: bfloat16 [2, 2048, 8192], P(None, None, 'tp')
- w_up: bfloat16 [2, 2048, 8192], P(None, None, 'tp')
- w_down: bfloat16 [2, 8192, 2048], P(None, 'tp')
Outputs:
- output 1: bfloat16 [512, 2048], P('dp'), parts along dimension 0
- output 2: bfloat16 [2, 512, 256, 8, 64], P(None, 'dp', None, 'tp'), parts along dimension 1
- output 3: bfloat16 [2, 512, 256, 8, 64], P(None, 'dp', None, 'tp'), parts along dimension 1
There are 4 independent parts. The reference program is written for one: setup_inputs(seed, part) draws one part's arguments, and reference() takes and returns one part's arrays. A program takes and returns all parts, laid end to end along the dimension named above; an argument that names none is the same for every part.
All inputs are finite; a program needn't handle non-finite values.
Results may differ from the reference program's by a relative error of at most 0.0171893.
Values are sent between devices in bfloat16 or wider.
A program may use at most 1 GiB of HBM per device.

```python
import jax
import jax.numpy as jnp
from jax import lax

D = 2048
HEADS = 32
KV_HEADS = 8
HEAD = 64
FF = 8192
BATCH = 128
SMAX = 256
LAYERS = 2

NORM_EPS = 1e-5
ROPE_THETA = 500000.0
ROPE_FACTOR = 8.0
LOW_FACTOR = 1.0
HIGH_FACTOR = 4.0
ORIG_CONTEXT = 8192.0


def rope_freqs():
    freq_expo = jnp.arange(0, HEAD, 2).astype(jnp.float32) / HEAD
    inv_freq = 1.0 / (ROPE_THETA ** freq_expo)
    wavelen = 2.0 * jnp.pi / inv_freq
    smooth = (ORIG_CONTEXT / wavelen - LOW_FACTOR) / (HIGH_FACTOR - LOW_FACTOR)
    blended = (1.0 - smooth) * inv_freq / ROPE_FACTOR + smooth * inv_freq
    return jnp.where(wavelen > ORIG_CONTEXT / LOW_FACTOR, inv_freq / ROPE_FACTOR,
                     jnp.where(wavelen < ORIG_CONTEXT / HIGH_FACTOR, inv_freq, blended))


def apply_rope(vectors, pos_angle):
    shaped = pos_angle.reshape(pos_angle.shape[:1] + (1,) * (vectors.ndim - 2) + pos_angle.shape[1:])
    cos_part = jnp.cos(shaped)
    sin_part = jnp.sin(shaped)
    half_dim = vectors.shape[-1] // 2
    lower_half = vectors[..., :half_dim]
    upper_half = vectors[..., half_dim:]
    return jnp.concatenate([lower_half * cos_part - upper_half * sin_part,
                            upper_half * cos_part + lower_half * sin_part], axis=-1)


def rms_norm(hidden, gain_vec):
    hidden_f = hidden.astype(jnp.float32)
    inv_rms = lax.rsqrt(jnp.mean(hidden_f * hidden_f, axis=-1, keepdims=True) + NORM_EPS)
    return (hidden_f * inv_rms * gain_vec.astype(jnp.float32)).astype(jnp.bfloat16)


def decode_layer(hidden, seq_lens, layer_parts):
    g_attn, w_q, w_k, w_v, w_o, g_mlp, w_gate, w_up, w_down, k_cache, v_cache = layer_parts
    batch_rows = hidden.shape[0]
    groups = HEADS // KV_HEADS
    pos_angle = seq_lens.astype(jnp.float32)[:, None] * rope_freqs()[None, :]
    normed = rms_norm(hidden, g_attn)
    q_full = jnp.dot(normed, w_q, preferred_element_type=jnp.float32).reshape(batch_rows, HEADS, HEAD)
    k_full = jnp.dot(normed, w_k, preferred_element_type=jnp.float32).reshape(batch_rows, KV_HEADS, HEAD)
    v_new = jnp.dot(normed, w_v, preferred_element_type=jnp.float32).reshape(batch_rows, KV_HEADS, HEAD).astype(jnp.bfloat16)
    q_rot = apply_rope(q_full, pos_angle).astype(jnp.bfloat16)
    k_new = apply_rope(k_full, pos_angle).astype(jnp.bfloat16)
    positions = jnp.arange(SMAX)
    at_new = (positions[None, :] == seq_lens[:, None])[:, :, None, None]
    k_cache = jnp.where(at_new, k_new[:, None], k_cache)
    v_cache = jnp.where(at_new, v_new[:, None], v_cache)
    q_grp = q_rot.reshape(batch_rows, KV_HEADS, groups, HEAD)
    scores = jnp.einsum("bkgh,bskh->bkgs", q_grp.astype(jnp.float32), k_cache.astype(jnp.float32)) * (HEAD ** -0.5)
    visible = (positions[None, :] <= seq_lens[:, None])[:, None, None, :]
    scores = jnp.where(visible, scores, -1e30)
    prob_all = jax.nn.softmax(scores, axis=-1).astype(jnp.bfloat16)
    attn_out = jnp.einsum("bkgs,bskh->bkgh", prob_all.astype(jnp.float32), v_cache.astype(jnp.float32))
    attn_out = attn_out.astype(jnp.bfloat16).reshape(batch_rows, HEADS * HEAD)
    hidden = (hidden.astype(jnp.float32) + jnp.dot(attn_out, w_o, preferred_element_type=jnp.float32)).astype(jnp.bfloat16)
    normed = rms_norm(hidden, g_mlp)
    gate_proj = jnp.dot(normed, w_gate, preferred_element_type=jnp.float32)
    up_proj = jnp.dot(normed, w_up, preferred_element_type=jnp.float32)
    mlp_act = (jax.nn.silu(gate_proj) * up_proj).astype(jnp.bfloat16)
    hidden = (hidden.astype(jnp.float32) + jnp.dot(mlp_act, w_down, preferred_element_type=jnp.float32)).astype(jnp.bfloat16)
    return hidden, (k_cache, v_cache)


def normal_weight(draw_key, arr_shape, fan_in):
    return (jax.random.normal(draw_key, arr_shape, jnp.float32) * fan_in ** -0.5).astype(jnp.bfloat16)


def setup_inputs(seed: int = 0, part: int = 0) -> dict:
    root_key = jax.random.key(seed)
    weight_keys = jax.random.split(root_key, 9)
    part_keys = jax.random.split(jax.random.fold_in(root_key, part), 6)
    hidden = jax.random.normal(part_keys[0], (BATCH, D), jnp.float32).astype(jnp.bfloat16)
    seq_lens = jax.random.randint(part_keys[1], (BATCH,), 1, SMAX, dtype=jnp.int32).at[0].set(SMAX - 1)
    cache_shape = (LAYERS, BATCH, SMAX, KV_HEADS, HEAD)
    trend_shape = (LAYERS, BATCH, 1, KV_HEADS, HEAD)
    k_cache = jax.random.normal(part_keys[2], cache_shape, jnp.float32).astype(jnp.bfloat16)
    v_base = jax.random.normal(part_keys[3], trend_shape, jnp.float32)
    v_slope = jax.random.normal(part_keys[4], trend_shape, jnp.float32)
    pos_ramp = (2.0 * jnp.arange(SMAX).astype(jnp.float32) / SMAX - 1.0)[None, None, :, None, None]
    v_noise = jax.random.normal(part_keys[5], cache_shape, jnp.float32)
    v_cache = (v_base + v_slope * pos_ramp + 0.5 * v_noise).astype(jnp.bfloat16)
    return {
        "hidden": hidden,
        "seq_lens": seq_lens,
        "k_cache": k_cache,
        "v_cache": v_cache,
        "g_attn": (1.0 + 0.4 * jax.random.normal(weight_keys[0], (LAYERS, D), jnp.float32)).astype(jnp.bfloat16),
        "w_q": normal_weight(weight_keys[1], (LAYERS, D, HEADS * HEAD), D),
        "w_k": normal_weight(weight_keys[2], (LAYERS, D, KV_HEADS * HEAD), D),
        "w_v": normal_weight(weight_keys[3], (LAYERS, D, KV_HEADS * HEAD), D),
        "w_o": normal_weight(weight_keys[4], (LAYERS, HEADS * HEAD, D), HEADS * HEAD),
        "g_mlp": (1.0 + 0.4 * jax.random.normal(weight_keys[5], (LAYERS, D), jnp.float32)).astype(jnp.bfloat16),
        "w_gate": normal_weight(weight_keys[6], (LAYERS, D, FF), D),
        "w_up": normal_weight(weight_keys[7], (LAYERS, D, FF), D),
        "w_down": normal_weight(weight_keys[8], (LAYERS, FF, D), FF),
    }


def reference(hidden, seq_lens, k_cache, v_cache, g_attn, w_q, w_k, w_v, w_o, g_mlp, w_gate, w_up, w_down):
    def layer_step(carry, layer_parts):
        return decode_layer(carry, seq_lens, layer_parts)
    hidden_out, cache_pair = lax.scan(layer_step, hidden,
                                      (g_attn, w_q, w_k, w_v, w_o, g_mlp, w_gate, w_up, w_down, k_cache, v_cache))
    return hidden_out, cache_pair[0], cache_pair[1]
```

```python
import functools

import jax
import jax.numpy as jnp
from jax import lax
from jax.experimental import pallas as pl
from jax.experimental.pallas import tpu as pltpu
from jax.sharding import PartitionSpec as P

NORM_EPS = 1e-5
ROPE_THETA = 500000.0
ROPE_FACTOR = 8.0
LOW_FACTOR = 1.0
HIGH_FACTOR = 4.0
ORIG_CONTEXT = 8192.0

ROWS = 128
D = 2048
SMAX = 256
HEAD = 64
KVD = 128
QD = 512
FF = 2048
SEQS = 8
STEPS = ROWS // SEQS
CW = 512
NCH = D // CW
F32 = jnp.float32
BF16 = jnp.bfloat16
MESH = pl.DeviceIdType.MESH
ANY = pl.BlockSpec(memory_space=pl.ANY)
VMEM = pl.BlockSpec(memory_space=pltpu.VMEM)
SMEM = pl.BlockSpec(memory_space=pltpu.SMEM)


def rope_freqs(head_dim):
    freq_expo = jnp.arange(0, head_dim, 2).astype(F32) / head_dim
    inv_freq = 1.0 / (ROPE_THETA ** freq_expo)
    wavelen = 2.0 * jnp.pi / inv_freq
    smooth = (ORIG_CONTEXT / wavelen - LOW_FACTOR) / (HIGH_FACTOR - LOW_FACTOR)
    blended = (1.0 - smooth) * inv_freq / ROPE_FACTOR + smooth * inv_freq
    return jnp.where(wavelen > ORIG_CONTEXT / LOW_FACTOR, inv_freq / ROPE_FACTOR,
                     jnp.where(wavelen < ORIG_CONTEXT / HIGH_FACTOR, inv_freq, blended))


def norm_rows(hidden_f, gain):
    inv_rms = lax.rsqrt(jnp.mean(hidden_f * hidden_f, axis=-1, keepdims=True) + NORM_EPS)
    return (hidden_f * inv_rms * gain.astype(F32)).astype(BF16)


def rope_slab(slab, cos, sin):
    lane = lax.broadcasted_iota(jnp.int32, slab.shape, 1)
    other = jnp.where(lane % HEAD < HEAD // 2, pltpu.roll(slab, 128 - HEAD // 2, 1), pltpu.roll(slab, HEAD // 2, 1))
    return slab * cos + other * sin


def attn_kernel(layer, aliased, *refs):
    if aliased:
        (seq_ref, h_ref, cos_ref, sin_ref, g_ref, wq_hbm, wk_hbm, wv_hbm, k_hbm, v_hbm, _, _,
         out_ref, ko_hbm, vo_hbm, wq, wk, wv, kbuf, vbuf, knew, vnew, qrow, orow, wsem, ksem, vsem, osem) = refs
    else:
        (seq_ref, h_ref, cos_ref, sin_ref, g_ref, wq_hbm, wk_hbm, wv_hbm, k_hbm, v_hbm,
         out_ref, ko_hbm, vo_hbm, wq, wk, wv, kbuf, vbuf, knew, vnew, qrow, orow, wsem, ksem, vsem, osem) = refs

    def load_w(i):
        src, dst = ((wk_hbm, wk), (wv_hbm, wv), (wq_hbm, wq))[i]
        return pltpu.make_async_copy(src.at[layer], dst, wsem.at[i])

    def load_k(i):
        return pltpu.make_async_copy(k_hbm.at[layer, pl.ds(i * SEQS, SEQS)], kbuf.at[pl.ds(i * SEQS, SEQS)], ksem.at[i])

    def load_v(i):
        return pltpu.make_async_copy(v_hbm.at[layer, pl.ds(i * SEQS, SEQS)], vbuf.at[pl.ds(i * SEQS, SEQS)], vsem.at[i])

    def store_k(i):
        return pltpu.make_async_copy(kbuf.at[pl.ds(i * SEQS, SEQS)], ko_hbm.at[layer, pl.ds(i * SEQS, SEQS)], osem.at[0, i])

    def store_v(i):
        return pltpu.make_async_copy(vbuf.at[pl.ds(i * SEQS, SEQS)], vo_hbm.at[layer, pl.ds(i * SEQS, SEQS)], osem.at[1, i])

    for i in range(3):
        load_w(i).start()
    for i in range(STEPS):
        load_k(i).start()
        load_v(i).start()

    normed = norm_rows(h_ref[...].astype(F32), g_ref[layer:layer + 1, :])
    cos = cos_ref[...]
    sin = sin_ref[...]
    load_w(0).wait()
    k_rot = rope_slab(jnp.dot(normed, wk[...], preferred_element_type=F32), cos, sin).astype(BF16).astype(F32).T
    load_w(1).wait()
    v_row = jnp.dot(normed, wv[...], preferred_element_type=F32).astype(BF16).astype(F32).T
    for i in range(STEPS):
        shift = (ROWS - i * SEQS) % ROWS
        knew[i] = (pltpu.roll(k_rot, shift, 1) if shift else k_rot).astype(BF16)
        vnew[i] = (pltpu.roll(v_row, shift, 1) if shift else v_row).astype(BF16)
    load_w(2).wait()
    lane = lax.broadcasted_iota(jnp.int32, (ROWS, 128), 1)
    for slab_idx in range(4):
        slab = jnp.dot(normed, wq[:, slab_idx * 128:(slab_idx + 1) * 128], preferred_element_type=F32)
        slab = rope_slab(slab, cos, sin).astype(BF16).astype(F32)
        turned = pltpu.roll(slab, HEAD, 1)
        for half in range(2):
            hg = slab_idx * 2 + half
            kv = hg // 4
            qrow[pl.ds(hg, ROWS, stride=8), :] = jnp.where(lane // HEAD == kv, slab if kv == half else turned, 0.0)

    def step(i, carry):
        load_k(i).wait()
        load_v(i).wait()
        lane16 = lax.broadcasted_iota(jnp.int16, (KVD, SMAX), 1)
        lane8 = lax.broadcasted_iota(jnp.int32, (8, SMAX), 1)
        row16 = lax.broadcasted_iota(jnp.int32, (16, 128), 0)
        row8 = lax.broadcasted_iota(jnp.int32, (8, 128), 0)
        lane_o = lax.broadcasted_iota(jnp.int32, (8, 128), 1)
        for j in range(SEQS):
            b = i * SEQS + j
            here = lane16 == seq_ref[b].astype(jnp.int16)
            kbuf[b] = jnp.where(here, jnp.broadcast_to(knew[i, :, j:j + 1], (KVD, SMAX)), kbuf[b])
            vbuf[b] = jnp.where(here, jnp.broadcast_to(vnew[i, :, j:j + 1], (KVD, SMAX)), vbuf[b])
        store_k(i).start()
        store_v(i).start()
        scores = []
        for p in range(SEQS // 2):
            b = i * SEQS + 2 * p
            q2 = qrow[pl.ds(b * 8, 16), :]
            qb = jnp.concatenate([jnp.where(row16 < 8, q2, 0.0), jnp.where(row16 >= 8, q2, 0.0)], axis=1).astype(BF16)
            kk = kbuf[pl.ds(b, 2)].reshape(2 * KVD, SMAX)
            scores.append(jnp.dot(qb, kk, preferred_element_type=F32) * (HEAD ** -0.5))
        for p in range(SEQS // 2):
            b = i * SEQS + 2 * p
            halves = []
            for j in range(2):
                s = jnp.where(lane8 <= seq_ref[b + j], scores[p][8 * j:8 * j + 8], -1e30)
                e = jnp.exp(s - jnp.max(s, axis=-1, keepdims=True))
                halves.append(e / jnp.sum(e, axis=-1, keepdims=True))
            prob = jnp.concatenate(halves, axis=0).astype(BF16)
            vv = vbuf[pl.ds(b, 2)].reshape(2 * KVD, SMAX)
            mix = lax.dot_general(prob, vv, (((1,), (1,)), ((), ())), preferred_element_type=F32)
            for j in range(2):
                m = mix[8 * j:8 * j + 8, 128 * j:128 * j + 128]
                orow[pl.ds((b + j) * 8, 8), :] = jnp.where((row8 < 4) == (lane_o < HEAD), m, pltpu.roll(m, HEAD, 1))
        return carry

    lax.fori_loop(0, STEPS, step, 0)
    for slab_idx in range(4):
        lower = orow[pl.ds(slab_idx * 2, ROWS, stride=8), :]
        upper = orow[pl.ds(slab_idx * 2 + 1, ROWS, stride=8), :]
        out_ref[:, slab_idx * 128:(slab_idx + 1) * 128] = jnp.where(lane < HEAD, lower, upper).astype(BF16)
    for i in range(STEPS):
        store_k(i).wait()
        store_v(i).wait()


def attn_call(layer, seq_lens, hidden, cos, sin, g_attn, w_q, w_k, w_v, k_cache, v_cache, outs=()):
    cache = jax.ShapeDtypeStruct(k_cache.shape, BF16)
    return pl.pallas_call(
        functools.partial(attn_kernel, layer, bool(outs)),
        out_shape=(jax.ShapeDtypeStruct((ROWS, QD), BF16), cache, cache),
        in_specs=[SMEM, VMEM, VMEM, VMEM, VMEM] + [ANY] * (5 + len(outs)),
        out_specs=(VMEM, ANY, ANY),
        scratch_shapes=[
            pltpu.VMEM((D, QD), BF16),
            pltpu.VMEM((D, KVD), BF16),
            pltpu.VMEM((D, KVD), BF16),
            pltpu.VMEM((ROWS, KVD, SMAX), BF16),
            pltpu.VMEM((ROWS, KVD, SMAX), BF16),
            pltpu.VMEM((STEPS, KVD, ROWS), BF16),
            pltpu.VMEM((STEPS, KVD, ROWS), BF16),
            pltpu.VMEM((ROWS * 8, 128), F32),
            pltpu.VMEM((ROWS * 8, 128), F32),
            pltpu.SemaphoreType.DMA((3,)),
            pltpu.SemaphoreType.DMA((STEPS,)),
            pltpu.SemaphoreType.DMA((STEPS,)),
            pltpu.SemaphoreType.DMA((2, STEPS)),
        ],
        input_output_aliases={10: 1, 11: 2} if outs else {},
        compiler_params=pltpu.CompilerParams(vmem_limit_bytes=50 * 2 ** 20),
        name=f"attn{layer}",
    )(seq_lens, hidden, cos, sin, g_attn, w_q, w_k, w_v, k_cache, v_cache, *outs)


def mlp_kernel(layer, attn_ref, h_ref, g_ref, wo_hbm, wg_hbm, wu_hbm, wd_hbm, out_ref,
               wo, wg, wu, wd, send1, recv1, pair, recv2, hbuf, act,
               wsem, s1_send, s1_recv, s2_send, s2_recv, s3_send, s3_recv):
    me = lax.axis_index("tp")
    core = lax.rem(me, 2)
    sibling = me + 1 - 2 * core
    peer = lax.rem(me + 2, 4)

    def load(kind, j):
        src = (wo_hbm, wg_hbm, wu_hbm, wd_hbm)[kind].at[layer, :, pl.ds(j * CW, CW)]
        return pltpu.make_async_copy(src, (wo, wg, wu, wd)[kind].at[j], wsem.at[kind, j])

    for j in range(NCH):
        load(0, j).start()
    for j in range(NCH):
        load(1, j).start()
        load(2, j).start()
    for j in range(NCH):
        load(3, j).start()

    barrier = pltpu.get_barrier_semaphore()
    for other in (sibling, peer):
        pl.semaphore_signal(barrier, inc=1, device_id={"tp": other}, device_id_type=MESH)

    def remote(src, dst, ss, rs, to):
        return pltpu.make_async_remote_copy(src_ref=src, dst_ref=dst, send_sem=ss, recv_sem=rs,
                                            device_id={"tp": to}, device_id_type=MESH)

    def cols(j):
        return pl.ds(pl.multiple_of(j * CW, CW), CW)

    def copy1(r, j):
        return remote(send1.at[r, j], recv1.at[r, j], s1_send.at[r, j], s1_recv.at[r, j], sibling)

    def copy2(r, j):
        return remote(pair.at[r, j], recv2.at[r, j], s2_send.at[r, j], s2_recv.at[r, j], peer)

    def copy3(r, j):
        mine = hbuf.at[r, core * 2 + j]
        return remote(mine, mine, s3_send.at[r, j], s3_recv.at[r, j], sibling)

    def copy3_in(r, j):
        theirs = hbuf.at[r, 2 - core * 2 + j]
        return remote(theirs, theirs, s3_send.at[r, j], s3_recv.at[r, j], sibling)

    def all_reduce(r, product, residual):
        for j in range(2):
            send1[r, j] = product(2 - core * 2 + j).astype(BF16)
            if r == 0 and j == 0:
                pl.semaphore_wait(barrier, 2)
            copy1(r, j).start()
        own = [product(core * 2 + j) for j in range(2)]
        for j in range(2):
            copy1(r, j).wait_recv()
            pair[r, j] = (own[j] + recv1[r, j].astype(F32)).astype(BF16)
            copy2(r, j).start()
        for j in range(2):
            copy2(r, j).wait_recv()
            total = pair[r, j].astype(F32) + recv2[r, j].astype(F32)
            hbuf[r, core * 2 + j] = (residual(core * 2 + j).astype(F32) + total).astype(BF16)
            copy3(r, j).start()
        for j in range(2):
            copy3_in(r, j).wait_recv()
        for j in range(2):
            copy1(r, j).wait_send()
            copy2(r, j).wait_send()
            copy3(r, j).wait_send()

    for j in range(NCH):
        load(0, j).wait()
    attn = attn_ref[...]
    all_reduce(0, lambda j: jnp.dot(attn, wo[j], preferred_element_type=F32), lambda j: h_ref[:, cols(j)])

    hidden = jnp.concatenate([hbuf[0, j] for j in range(NCH)], axis=1)
    normed = norm_rows(hidden.astype(F32), g_ref[layer:layer + 1, :])
    for j in range(NCH):
        load(1, j).wait()
        gate = jnp.dot(normed, wg[j], preferred_element_type=F32)
        load(2, j).wait()
        up = jnp.dot(normed, wu[j], preferred_element_type=F32)
        act[:, j * CW:(j + 1) * CW] = (gate * jax.nn.sigmoid(gate) * up).astype(BF16)
    for j in range(NCH):
        load(3, j).wait()
    all_reduce(1, lambda j: jnp.dot(act[...], wd[j], preferred_element_type=F32), lambda j: hbuf[0, j])
    for j in range(NCH):
        out_ref[:, j * CW:(j + 1) * CW] = hbuf[1, j]


def mlp_call(layer, attn, hidden, g_mlp, w_o, w_gate, w_up, w_down):
    chunk = pltpu.VMEM((2, 2, ROWS, CW), BF16)
    return pl.pallas_call(
        functools.partial(mlp_kernel, layer),
        out_shape=jax.ShapeDtypeStruct((ROWS, D), BF16),
        in_specs=[VMEM, VMEM, VMEM] + [ANY] * 4,
        out_specs=VMEM,
        scratch_shapes=[
            pltpu.VMEM((NCH, QD, CW), BF16),
            pltpu.VMEM((NCH, D, CW), BF16),
            pltpu.VMEM((NCH, D, CW), BF16),
            pltpu.VMEM((NCH, FF, CW), BF16),
            chunk, chunk, chunk, chunk,
            pltpu.VMEM((2, NCH, ROWS, CW), BF16),
            pltpu.VMEM((ROWS, FF), BF16),
            pltpu.SemaphoreType.DMA((4, NCH)),
        ] + [pltpu.SemaphoreType.DMA((2, 2))] * 6,
        compiler_params=pltpu.CompilerParams(vmem_limit_bytes=50 * 2 ** 20, collective_id=layer, has_side_effects=True),
        name=f"mlp{layer}",
    )(attn, hidden, g_mlp, w_o, w_gate, w_up, w_down)


def solution(mesh):
    cache_spec = P(None, "dp", None, "tp", None)
    col_spec = P(None, None, "tp")
    row_spec = P(None, "tp", None)
    in_specs = (P("dp", None), P("dp"), cache_spec, cache_spec, P(None, None), col_spec, col_spec, col_spec,
                row_spec, P(None, None), col_spec, col_spec, row_spec)
    out_specs = (P("dp", None), cache_spec, cache_spec)

    def local_step(hidden, seq_lens, k_cache, v_cache, g_attn, w_q, w_k, w_v, w_o, g_mlp, w_gate, w_up, w_down):
        layers = k_cache.shape[0]
        kt = k_cache.transpose(0, 1, 3, 4, 2).reshape(layers, ROWS, KVD, SMAX)
        vt = v_cache.transpose(0, 1, 3, 4, 2).reshape(layers, ROWS, KVD, SMAX)
        angle = seq_lens.astype(F32)[:, None] * rope_freqs(HEAD)[None, :]
        cos = jnp.tile(jnp.cos(angle), (1, 4))
        sin = jnp.sin(angle)
        sin = jnp.concatenate([-sin, sin, -sin, sin], axis=1)
        outs = ()
        for layer in range(layers):
            attn, *outs = attn_call(layer, seq_lens, hidden, cos, sin, g_attn, w_q, w_k, w_v, kt, vt, outs)
            hidden = mlp_call(layer, attn, hidden, g_mlp, w_o, w_gate, w_up, w_down)

        def back(cache):
            return cache.reshape(layers, ROWS, 2, HEAD, SMAX).transpose(0, 1, 4, 2, 3)

        return hidden, back(outs[0]), back(outs[1])

    return jax.shard_map(local_step, mesh=mesh, in_specs=in_specs, out_specs=out_specs, check_vma=False)
```

```python
import functools

import jax
import jax.numpy as jnp
import numpy as np
from jax import lax
from jax.experimental import pallas as pl
from jax.experimental.pallas import tpu as pltpu
from jax.sharding import PartitionSpec as P

NORM_EPS = 1e-5
ROPE_THETA = 500000.0
ROPE_FACTOR = 8.0
LOW_FACTOR = 1.0
HIGH_FACTOR = 4.0
ORIG_CONTEXT = 8192.0

ROWS = 128
D = 2048
SMAX = 256
HEAD = 64
KVD = 128
QD = 512
FF = 2048
SEQS = 16
STEPS = ROWS // SEQS
CW = 512
NCH = D // CW
F32 = jnp.float32
BF16 = jnp.bfloat16
MESH = pl.DeviceIdType.MESH
VMEM = pl.BlockSpec(memory_space=pltpu.VMEM)
HBM = pl.BlockSpec(memory_space=pltpu.HBM)


def rope_freqs(head_dim):
    freq_expo = np.arange(0, head_dim, 2).astype(np.float32) / np.float32(head_dim)
    inv_freq = 1.0 / (ROPE_THETA ** freq_expo.astype(np.float64))
    wavelen = 2.0 * np.pi / inv_freq
    smooth = (ORIG_CONTEXT / wavelen - LOW_FACTOR) / (HIGH_FACTOR - LOW_FACTOR)
    blended = (1.0 - smooth) * inv_freq / ROPE_FACTOR + smooth * inv_freq
    return np.where(wavelen > ORIG_CONTEXT / LOW_FACTOR, inv_freq / ROPE_FACTOR,
                    np.where(wavelen < ORIG_CONTEXT / HIGH_FACTOR, inv_freq, blended)).astype(np.float32)


def norm_rows(hidden_f, gain):
    inv_rms = lax.rsqrt(jnp.mean(hidden_f * hidden_f, axis=-1, keepdims=True) + NORM_EPS)
    return (hidden_f * inv_rms * gain.astype(F32)).astype(BF16)


def rope_slab(slab, cos, sin):
    lane = lax.broadcasted_iota(jnp.int32, slab.shape, 1)
    other = jnp.where(lane % HEAD < HEAD // 2, pltpu.roll(slab, 128 - HEAD // 2, 1), pltpu.roll(slab, HEAD // 2, 1))
    return slab * cos + other * sin


def attn_kernel(layer, aliased, *refs):
    seq_hbm, seqv_hbm, freq_hbm, h_hbm, g_hbm, wq_hbm, wk_hbm, wv_hbm, k_hbm, v_hbm = refs[:10]
    (out_ref, ko_hbm, vo_hbm, seq_ref, seqv, freq, h_ref, g_ref, wq, wk, wv, kbuf, vbuf, knew, vnew, qrow, orow,
     sem, ksem, vsem, osem) = refs[12 if aliased else 10:]

    def small(i):
        src, dst = ((seqv_hbm, seqv), (freq_hbm, freq), (h_hbm, h_ref), (g_hbm, g_ref), (wk_hbm.at[layer], wk),
                    (wv_hbm.at[layer], wv), (wq_hbm.at[layer], wq), (seq_hbm, seq_ref))[i]
        return pltpu.make_async_copy(src, dst, sem.at[i])

    def load_k(i):
        return pltpu.make_async_copy(k_hbm.at[layer, pl.ds(i * SEQS, SEQS)], kbuf.at[pl.ds(i * SEQS, SEQS)], ksem.at[i])

    def load_v(i):
        return pltpu.make_async_copy(v_hbm.at[layer, pl.ds(i * SEQS, SEQS)], vbuf.at[pl.ds(i * SEQS, SEQS)], vsem.at[i])

    def store_k(i):
        return pltpu.make_async_copy(kbuf.at[pl.ds(i * SEQS, SEQS)], ko_hbm.at[layer, pl.ds(i * SEQS, SEQS)], osem.at[0, i])

    def store_v(i):
        return pltpu.make_async_copy(vbuf.at[pl.ds(i * SEQS, SEQS)], vo_hbm.at[layer, pl.ds(i * SEQS, SEQS)], osem.at[1, i])

    for i in range(8):
        small(i).start()
    load_k(0).start()
    load_v(0).start()

    small(0).wait()
    small(1).wait()
    angle = jnp.broadcast_to(seqv[...].astype(F32), (ROWS, 128)).T * freq[...]
    cos = jnp.cos(angle)
    sin = jnp.sin(angle)
    lane = lax.broadcasted_iota(jnp.int32, (ROWS, 128), 1)
    sin = jnp.where(lane % HEAD < HEAD // 2, -sin, sin)
    small(2).wait()
    small(3).wait()
    normed = norm_rows(h_ref[...].astype(F32), g_ref[layer:layer + 1, :])
    small(4).wait()
    small(5).wait()
    small(6).wait()
    for i in range(1, STEPS):
        load_k(i).start()
        load_v(i).start()
    knew[...] = rope_slab(jnp.dot(normed, wk[...], preferred_element_type=F32), cos, sin).astype(BF16).astype(F32).T
    vnew[...] = jnp.dot(normed, wv[...], preferred_element_type=F32).astype(BF16).astype(F32).T
    for slab_idx in range(4):
        slab = jnp.dot(normed, wq[:, slab_idx * 128:(slab_idx + 1) * 128], preferred_element_type=F32)
        slab = rope_slab(slab, cos, sin).astype(BF16).astype(F32)
        turned = pltpu.roll(slab, HEAD, 1)
        for half in range(2):
            hg = slab_idx * 2 + half
            kv = hg // 4
            qrow[pl.ds(hg, ROWS, stride=8), :] = jnp.where(lane // HEAD == kv, slab if kv == half else turned, 0.0)
    small(7).wait()

    def step(i, carry):
        load_k(i).wait()
        load_v(i).wait()
        lane16 = lax.broadcasted_iota(jnp.int16, (KVD, SMAX), 1)
        lane8 = lax.broadcasted_iota(jnp.int32, (8, SMAX), 1)
        row16 = lax.broadcasted_iota(jnp.int32, (16, 128), 0)
        row8 = lax.broadcasted_iota(jnp.int32, (8, 128), 0)
        lane_o = lax.broadcasted_iota(jnp.int32, (8, 128), 1)
        shift = lax.rem(ROWS - i * SEQS, ROWS)

        def insert(buf, new_ref):
            new = pltpu.roll(new_ref[...], shift, 1)
            for j in range(SEQS):
                b = i * SEQS + j
                column = jnp.broadcast_to(new[:, j:j + 1], (KVD, 128)).astype(BF16)
                here = lane16 == seq_ref[0, b].astype(jnp.int16)
                buf[b] = jnp.where(here, jnp.concatenate([column, column], axis=1), buf[b])

        insert(kbuf, knew)
        store_k(i).start()
        insert(vbuf, vnew)
        store_v(i).start()
        scores = []
        for p in range(SEQS // 2):
            b = i * SEQS + 2 * p
            q2 = qrow[pl.ds(b * 8, 16), :]
            qb = jnp.concatenate([jnp.where(row16 < 8, q2, 0.0), jnp.where(row16 >= 8, q2, 0.0)], axis=1).astype(BF16)
            kk = kbuf[pl.ds(b, 2)].reshape(2 * KVD, SMAX)
            scores.append(jnp.dot(qb, kk, preferred_element_type=F32) * (HEAD ** -0.5))
        for p in range(SEQS // 2):
            b = i * SEQS + 2 * p
            halves = []
            for j in range(2):
                s = jnp.where(lane8 <= seq_ref[0, b + j], scores[p][8 * j:8 * j + 8], -1e30)
                e = jnp.exp(s - jnp.max(s, axis=-1, keepdims=True))
                halves.append(e / jnp.sum(e, axis=-1, keepdims=True))
            prob = jnp.concatenate(halves, axis=0).astype(BF16)
            vv = vbuf[pl.ds(b, 2)].reshape(2 * KVD, SMAX)
            mix = lax.dot_general(prob, vv, (((1,), (1,)), ((), ())), preferred_element_type=F32)
            for j in range(2):
                m = mix[8 * j:8 * j + 8, 128 * j:128 * j + 128]
                orow[pl.ds((b + j) * 8, 8), :] = jnp.where((row8 < 4) == (lane_o < HEAD), m, pltpu.roll(m, HEAD, 1))
        return carry

    lax.fori_loop(0, STEPS, step, 0)
    for slab_idx in range(4):
        lower = orow[pl.ds(slab_idx * 2, ROWS, stride=8), :]
        upper = orow[pl.ds(slab_idx * 2 + 1, ROWS, stride=8), :]
        out_ref[:, slab_idx * 128:(slab_idx + 1) * 128] = jnp.where(lane < HEAD, lower, upper).astype(BF16)
    for i in range(STEPS):
        store_k(i).wait()
        store_v(i).wait()


def attn_call(layer, seq_lens, freq, hidden, g_attn, w_q, w_k, w_v, k_cache, v_cache, outs=()):
    cache = jax.ShapeDtypeStruct(k_cache.shape, BF16)
    return pl.pallas_call(
        functools.partial(attn_kernel, layer, bool(outs)),
        out_shape=(jax.ShapeDtypeStruct((ROWS, QD), BF16), cache, cache),
        in_specs=[HBM] * (10 + len(outs)),
        out_specs=(VMEM, HBM, HBM),
        scratch_shapes=[
            pltpu.SMEM((1, ROWS), jnp.int32),
            pltpu.VMEM((1, ROWS), jnp.int32),
            pltpu.VMEM((1, 128), F32),
            pltpu.VMEM((ROWS, D), BF16),
            pltpu.VMEM(g_attn.shape, BF16),
            pltpu.VMEM((D, QD), BF16),
            pltpu.VMEM((D, KVD), BF16),
            pltpu.VMEM((D, KVD), BF16),
            pltpu.VMEM((ROWS, KVD, SMAX), BF16),
            pltpu.VMEM((ROWS, KVD, SMAX), BF16),
            pltpu.VMEM((KVD, ROWS), F32),
            pltpu.VMEM((KVD, ROWS), F32),
            pltpu.VMEM((ROWS * 8, 128), F32),
            pltpu.VMEM((ROWS * 8, 128), F32),
            pltpu.SemaphoreType.DMA((8,)),
            pltpu.SemaphoreType.DMA((STEPS,)),
            pltpu.SemaphoreType.DMA((STEPS,)),
            pltpu.SemaphoreType.DMA((2, STEPS)),
        ],
        input_output_aliases={10: 1, 11: 2} if outs else {},
        compiler_params=pltpu.CompilerParams(vmem_limit_bytes=50 * 2 ** 20),
        name=f"attn{layer}",
    )(seq_lens, seq_lens, freq, hidden, g_attn, w_q, w_k, w_v, k_cache, v_cache, *outs)


def mlp_kernel(layer, attn_ref, h_hbm, g_hbm, wo_hbm, wg_hbm, wu_hbm, wd_hbm, out_ref,
               h_ref, g_ref, wo, wg, wu, wd, send1, recv1, pair, recv2, hbuf, act,
               hsem, wsem, s1_send, s1_recv, s2_send, s2_recv, s3_send, s3_recv):
    me = lax.axis_index("tp")
    core = lax.rem(me, 2)
    sibling = me + 1 - 2 * core
    peer = lax.rem(me + 2, 4)

    def load(kind, j):
        src = (wo_hbm, wg_hbm, wu_hbm, wd_hbm)[kind].at[layer, :, pl.ds(j * CW, CW)]
        return pltpu.make_async_copy(src, (wo, wg, wu, wd)[kind].at[j], wsem.at[kind, j])

    for j in range(NCH):
        load(0, j).start()
    load_h = pltpu.make_async_copy(h_hbm, h_ref, hsem.at[0])
    load_g = pltpu.make_async_copy(g_hbm, g_ref, hsem.at[1])
    load_h.start()
    load_g.start()

    barrier = pltpu.get_barrier_semaphore()
    for other in (sibling, peer):
        pl.semaphore_signal(barrier, inc=1, device_id={"tp": other}, device_id_type=MESH)

    def remote(src, dst, ss, rs, to):
        return pltpu.make_async_remote_copy(src_ref=src, dst_ref=dst, send_sem=ss, recv_sem=rs,
                                            device_id={"tp": to}, device_id_type=MESH)

    def cols(j):
        return pl.ds(pl.multiple_of(j * CW, CW), CW)

    def copy1(r, j):
        return remote(send1.at[r, j], recv1.at[r, j], s1_send.at[r, j], s1_recv.at[r, j], sibling)

    def copy2(r, j):
        return remote(pair.at[r, j], recv2.at[r, j], s2_send.at[r, j], s2_recv.at[r, j], peer)

    def copy3(r, j):
        mine = hbuf.at[r, core * 2 + j]
        return remote(mine, mine, s3_send.at[r, j], s3_recv.at[r, j], sibling)

    def copy3_in(r, j):
        theirs = hbuf.at[r, 2 - core * 2 + j]
        return remote(theirs, theirs, s3_send.at[r, j], s3_recv.at[r, j], sibling)

    def all_reduce(r, product, residual):
        def to_sibling(j):
            send1[r, j] = product(2 - core * 2 + j).astype(BF16)
            copy1(r, j).start()

        def to_peer(j, own):
            copy1(r, j).wait_recv()
            pair[r, j] = (own + recv1[r, j].astype(F32)).astype(BF16)
            copy2(r, j).start()

        to_sibling(0)
        own0 = product(core * 2)
        to_sibling(1)
        to_peer(0, own0)
        to_peer(1, product(core * 2 + 1))
        for j in range(2):
            copy2(r, j).wait_recv()
            total = pair[r, j].astype(F32) + recv2[r, j].astype(F32)
            hbuf[r, core * 2 + j] = (residual(core * 2 + j).astype(F32) + total).astype(BF16)
            copy3(r, j).start()
        for j in range(2):
            copy3_in(r, j).wait_recv()
        for j in range(2):
            copy1(r, j).wait_send()
            copy2(r, j).wait_send()
            copy3(r, j).wait_send()

    for j in range(NCH):
        load(0, j).wait()
    for j in range(NCH):
        load(1, j).start()
        load(2, j).start()
    for j in range(NCH):
        load(3, j).start()
    load_h.wait()
    load_g.wait()
    attn = attn_ref[...]
    pl.semaphore_wait(barrier, 2)
    all_reduce(0, lambda j: jnp.dot(attn, wo[j], preferred_element_type=F32), lambda j: h_ref[:, cols(j)])

    hidden = jnp.concatenate([hbuf[0, j] for j in range(NCH)], axis=1)
    normed = norm_rows(hidden.astype(F32), g_ref[layer:layer + 1, :])
    for j in range(NCH):
        load(1, j).wait()
        gate = jnp.dot(normed, wg[j], preferred_element_type=F32)
        load(2, j).wait()
        up = jnp.dot(normed, wu[j], preferred_element_type=F32)
        act[:, j * CW:(j + 1) * CW] = (gate * jax.nn.sigmoid(gate) * up).astype(BF16)
    for j in range(NCH):
        load(3, j).wait()
    all_reduce(1, lambda j: jnp.dot(act[...], wd[j], preferred_element_type=F32), lambda j: hbuf[0, j])
    for j in range(NCH):
        out_ref[:, j * CW:(j + 1) * CW] = hbuf[1, j]


def mlp_call(layer, attn, hidden, g_mlp, w_o, w_gate, w_up, w_down):
    chunk = pltpu.VMEM((2, 2, ROWS, CW), BF16)
    return pl.pallas_call(
        functools.partial(mlp_kernel, layer),
        out_shape=jax.ShapeDtypeStruct((ROWS, D), BF16),
        in_specs=[VMEM] + [HBM] * 6,
        out_specs=VMEM,
        scratch_shapes=[
            pltpu.VMEM((ROWS, D), BF16),
            pltpu.VMEM(g_mlp.shape, BF16),
            pltpu.VMEM((NCH, QD, CW), BF16),
            pltpu.VMEM((NCH, D, CW), BF16),
            pltpu.VMEM((NCH, D, CW), BF16),
            pltpu.VMEM((NCH, FF, CW), BF16),
            chunk, chunk, chunk, chunk,
            pltpu.VMEM((2, NCH, ROWS, CW), BF16),
            pltpu.VMEM((ROWS, FF), BF16),
            pltpu.SemaphoreType.DMA((2,)),
            pltpu.SemaphoreType.DMA((4, NCH)),
        ] + [pltpu.SemaphoreType.DMA((2, 2))] * 6,
        compiler_params=pltpu.CompilerParams(vmem_limit_bytes=50 * 2 ** 20, collective_id=layer, has_side_effects=True),
        name=f"mlp{layer}",
    )(attn, hidden, g_mlp, w_o, w_gate, w_up, w_down)


def solution(mesh):
    cache_spec = P(None, "dp", None, "tp", None)
    col_spec = P(None, None, "tp")
    row_spec = P(None, "tp", None)
    in_specs = (P("dp", None), P("dp"), cache_spec, cache_spec, P(None, None), col_spec, col_spec, col_spec,
                row_spec, P(None, None), col_spec, col_spec, row_spec)
    out_specs = (P("dp", None), cache_spec, cache_spec)

    def local_step(hidden, seq_lens, k_cache, v_cache, g_attn, w_q, w_k, w_v, w_o, g_mlp, w_gate, w_up, w_down):
        layers = k_cache.shape[0]
        kt = k_cache.transpose(0, 1, 3, 4, 2).reshape(layers, ROWS, KVD, SMAX)
        vt = v_cache.transpose(0, 1, 3, 4, 2).reshape(layers, ROWS, KVD, SMAX)
        freq = jnp.asarray(np.tile(rope_freqs(HEAD), 4)[None, :])
        seq_row = seq_lens.reshape(1, ROWS)
        hidden, g_attn, w_q, w_k, w_v, w_o, g_mlp, w_gate, w_up, w_down, kt, vt, freq, seq_row = (
            pltpu.with_memory_space_constraint(x, pltpu.HBM)
            for x in (hidden, g_attn, w_q, w_k, w_v, w_o, g_mlp, w_gate, w_up, w_down, kt, vt, freq, seq_row))
        outs = ()
        for layer in range(layers):
            attn, *outs = attn_call(layer, seq_row, freq, hidden, g_attn, w_q, w_k, w_v, kt, vt, outs)
            hidden = mlp_call(layer, attn, hidden, g_mlp, w_o, w_gate, w_up, w_down)

        def back(cache):
            return cache.reshape(layers, ROWS, 2, HEAD, SMAX).transpose(0, 1, 4, 2, 3)

        return hidden, back(outs[0]), back(outs[1])

    return jax.shard_map(local_step, mesh=mesh, in_specs=in_specs, out_specs=out_specs, check_vma=False)
```

```python
import functools

import jax
import jax.numpy as jnp
import numpy as np
from jax import lax
from jax.experimental import pallas as pl
from jax.experimental.pallas import tpu as pltpu
from jax.sharding import PartitionSpec as P

NORM_EPS = 1e-5
ROPE_THETA = 500000.0
ROPE_FACTOR = 8.0
LOW_FACTOR = 1.0
HIGH_FACTOR = 4.0
ORIG_CONTEXT = 8192.0

ROWS = 128
D = 2048
SMAX = 256
HEAD = 64
KVD = 128
QD = 512
FF = 2048
SEQS = 16
STEPS = ROWS // SEQS
CW = 512
NCH = D // CW
HALF = D // 2
RC = 32
NRC = ROWS // RC
F32 = jnp.float32
BF16 = jnp.bfloat16
MESH = pl.DeviceIdType.MESH
VMEM = pl.BlockSpec(memory_space=pltpu.VMEM)
HBM = pl.BlockSpec(memory_space=pltpu.HBM)


def rope_freqs(head_dim):
    freq_expo = np.arange(0, head_dim, 2).astype(np.float32) / np.float32(head_dim)
    inv_freq = 1.0 / (ROPE_THETA ** freq_expo.astype(np.float64))
    wavelen = 2.0 * np.pi / inv_freq
    smooth = (ORIG_CONTEXT / wavelen - LOW_FACTOR) / (HIGH_FACTOR - LOW_FACTOR)
    blended = (1.0 - smooth) * inv_freq / ROPE_FACTOR + smooth * inv_freq
    return np.where(wavelen > ORIG_CONTEXT / LOW_FACTOR, inv_freq / ROPE_FACTOR,
                    np.where(wavelen < ORIG_CONTEXT / HIGH_FACTOR, inv_freq, blended)).astype(np.float32)


def norm_rows(hidden_f, gain):
    inv_rms = lax.rsqrt(jnp.mean(hidden_f * hidden_f, axis=-1, keepdims=True) + NORM_EPS)
    return (hidden_f * inv_rms * gain.astype(F32)).astype(BF16)


def rope_slab(slab, cos, sin):
    lane = lax.broadcasted_iota(jnp.int32, slab.shape, 1)
    other = jnp.where(lane % HEAD < HEAD // 2, pltpu.roll(slab, 128 - HEAD // 2, 1), pltpu.roll(slab, HEAD // 2, 1))
    return slab * cos + other * sin


def layer_kernel(layer, seq_hbm, seqv_hbm, freq_hbm, h_hbm, ga_hbm, gm_hbm, wq_hbm, wk_hbm, wv_hbm, wo_hbm, wg_hbm, wu_hbm,
                 wd_hbm, k_hbm, v_hbm, out_ref, kbuf, vbuf, seq_ref, seqv, freq, h_ref, ga, gm, wq, wk, wv, wo, wg, wu, wd,
                 knew, vnew, qrow, orow, own1, send1, recv1, pair1, peer1, mid, send2, recv2, pair2, peer2, last, act,
                 sem, ksem, vsem, osem, wsem, sems1, sems2):
    me = lax.axis_index("tp")
    core = lax.rem(me, 2)
    sibling = me + 1 - 2 * core
    peer = lax.rem(me + 2, 4)

    barrier = pltpu.get_barrier_semaphore()
    for other in (sibling, peer):
        pl.semaphore_signal(barrier, inc=1, device_id={"tp": other}, device_id_type=MESH)

    def small(i):
        src, dst = ((seqv_hbm, seqv), (freq_hbm, freq), (h_hbm, h_ref), (ga_hbm, ga), (wk_hbm.at[layer], wk),
                    (wv_hbm.at[layer], wv), (wq_hbm.at[layer], wq), (seq_hbm, seq_ref), (gm_hbm, gm))[i]
        return pltpu.make_async_copy(src, dst, sem.at[i])

    def load_k(i):
        return pltpu.make_async_copy(k_hbm.at[layer, pl.ds(i * SEQS, SEQS)], kbuf.at[pl.ds(i * SEQS, SEQS)], ksem.at[i])

    def load_v(i):
        return pltpu.make_async_copy(v_hbm.at[layer, pl.ds(i * SEQS, SEQS)], vbuf.at[pl.ds(i * SEQS, SEQS)], vsem.at[i])

    def load_o(j):
        return pltpu.make_async_copy(wo_hbm.at[layer, :, pl.ds(j * HALF, HALF)], wo.at[j], osem.at[j])

    def load(kind, j):
        src = (wg_hbm, wu_hbm, wd_hbm)[kind].at[layer, :, pl.ds(j * CW, CW)]
        return pltpu.make_async_copy(src, (wg, wu, wd)[kind].at[j], wsem.at[kind, j])

    def remote(src, dst, sems, i, j, to):
        return pltpu.make_async_remote_copy(src_ref=src, dst_ref=dst, send_sem=sems.at[2 * i, j], recv_sem=sems.at[2 * i + 1, j],
                                            device_id={"tp": to}, device_id_type=MESH)

    for i in range(9):
        small(i).start()
    load_k(0).start()
    load_v(0).start()

    small(0).wait()
    small(1).wait()
    angle = jnp.broadcast_to(seqv[...].astype(F32), (ROWS, 128)).T * freq[...]
    cos = jnp.cos(angle)
    sin = jnp.sin(angle)
    lane = lax.broadcasted_iota(jnp.int32, (ROWS, 128), 1)
    sin = jnp.where(lane % HEAD < HEAD // 2, -sin, sin)
    small(2).wait()
    small(3).wait()
    normed = norm_rows(h_ref[...].astype(F32), ga[layer:layer + 1, :])
    small(4).wait()
    small(5).wait()
    small(6).wait()
    for i in range(1, STEPS):
        load_k(i).start()
        load_v(i).start()
        if i == 2:
            load_o(0).start()
            load_o(1).start()
    knew[...] = rope_slab(jnp.dot(normed, wk[...], preferred_element_type=F32), cos, sin).astype(BF16).astype(F32).T
    vnew[...] = jnp.dot(normed, wv[...], preferred_element_type=F32).astype(BF16).astype(F32).T
    for slab_idx in range(4):
        slab = jnp.dot(normed, wq[:, slab_idx * 128:(slab_idx + 1) * 128], preferred_element_type=F32)
        slab = rope_slab(slab, cos, sin).astype(BF16).astype(F32)
        turned = pltpu.roll(slab, HEAD, 1)
        for half in range(2):
            hg = slab_idx * 2 + half
            kv = hg // 4
            qrow[pl.ds(hg, ROWS, stride=8), :] = jnp.where(lane // HEAD == kv, slab if kv == half else turned, 0.0)
    small(7).wait()
    small(8).wait()
    pl.semaphore_wait(barrier, 2)

    def attend(i):
        load_k(i).wait()
        load_v(i).wait()
        lane16 = lax.broadcasted_iota(jnp.int16, (KVD, SMAX), 1)
        lane8 = lax.broadcasted_iota(jnp.int32, (8, SMAX), 1)
        row16 = lax.broadcasted_iota(jnp.int32, (16, 128), 0)
        row8 = lax.broadcasted_iota(jnp.int32, (8, 128), 0)
        lane_o = lax.broadcasted_iota(jnp.int32, (8, 128), 1)
        shift = lax.rem(ROWS - i * SEQS, ROWS)

        def insert(buf, new_ref):
            new = pltpu.roll(new_ref[...], shift, 1)
            for j in range(SEQS):
                b = i * SEQS + j
                column = jnp.broadcast_to(new[:, j:j + 1], (KVD, 128)).astype(BF16)
                here = lane16 == seq_ref[0, b].astype(jnp.int16)
                buf[b] = jnp.where(here, jnp.concatenate([column, column], axis=1), buf[b])

        insert(kbuf, knew)
        insert(vbuf, vnew)
        scores = []
        for p in range(SEQS // 2):
            b = i * SEQS + 2 * p
            q2 = qrow[pl.ds(b * 8, 16), :]
            qb = jnp.concatenate([jnp.where(row16 < 8, q2, 0.0), jnp.where(row16 >= 8, q2, 0.0)], axis=1).astype(BF16)
            kk = kbuf[pl.ds(b, 2)].reshape(2 * KVD, SMAX)
            scores.append(jnp.dot(qb, kk, preferred_element_type=F32) * (HEAD ** -0.5))
        for p in range(SEQS // 2):
            b = i * SEQS + 2 * p
            halves = []
            for j in range(2):
                s = jnp.where(lane8 <= seq_ref[0, b + j], scores[p][8 * j:8 * j + 8], -1e30)
                e = jnp.exp(s - jnp.max(s, axis=-1, keepdims=True))
                halves.append(e / jnp.sum(e, axis=-1, keepdims=True))
            prob = jnp.concatenate(halves, axis=0).astype(BF16)
            vv = vbuf[pl.ds(b, 2)].reshape(2 * KVD, SMAX)
            mix = lax.dot_general(prob, vv, (((1,), (1,)), ((), ())), preferred_element_type=F32)
            for j in range(2):
                m = mix[8 * j:8 * j + 8, 128 * j:128 * j + 128]
                orow[pl.ds((b + j) * 8, 8), :] = jnp.where((row8 < 4) == (lane_o < HEAD), m, pltpu.roll(m, HEAD, 1))

    def rows(rc):
        return pl.ds(pl.multiple_of(rc * RC, RC), RC)

    def copy1(rc):
        return remote(send1.at[rc], recv1.at[rc], sems1, 0, rc, sibling)

    def copy1_peer(rc):
        return remote(pair1.at[rc], peer1.at[rc], sems1, 1, rc, peer)

    def copy1_out(rc, half):
        return remote(mid.at[half, rows(rc)], mid.at[half, rows(rc)], sems1, 2, rc, sibling)

    def to_peer1(rc):
        copy1(rc).wait_recv()
        pair1[rc] = (own1[rc] + recv1[rc].astype(F32)).astype(BF16)
        copy1_peer(rc).start()

    def row_chunk(rc, carry):
        def step(i, c):
            attend(rc * (RC // SEQS) + i)
            return c

        lax.fori_loop(0, RC // SEQS, step, 0)
        parts = []
        lane_r = lax.broadcasted_iota(jnp.int32, (RC, 128), 1)
        for slab_idx in range(4):
            lower = orow[pl.ds(rc * RC * 8 + slab_idx * 2, RC, stride=8), :]
            upper = orow[pl.ds(rc * RC * 8 + slab_idx * 2 + 1, RC, stride=8), :]
            parts.append(jnp.where(lane_r < HEAD, lower, upper).astype(BF16))
        attn = jnp.concatenate(parts, axis=1)

        @pl.when(rc == 0)
        def _():
            load_o(0).wait()
            load_o(1).wait()

        send1[rc] = jnp.dot(attn, wo[1 - core], preferred_element_type=F32).astype(BF16)
        copy1(rc).start()
        own1[rc] = jnp.dot(attn, wo[core], preferred_element_type=F32)

        @pl.when(rc > 0)
        def _():
            to_peer1(rc - 1)

        @pl.when(rc == 1)
        def _():
            for j in range(NCH):
                load(0, j).start()
                load(1, j).start()

        @pl.when(rc == 2)
        def _():
            for j in range(NCH):
                load(2, j).start()

        return carry

    lax.fori_loop(0, NRC, row_chunk, 0)
    to_peer1(NRC - 1)
    for rc in range(NRC):
        copy1_peer(rc).wait_recv()
        total = pair1[rc].astype(F32) + peer1[rc].astype(F32)
        residual = h_ref[rc * RC:(rc + 1) * RC, pl.ds(pl.multiple_of(core * HALF, HALF), HALF)]
        mid[core, rc * RC:(rc + 1) * RC] = (residual.astype(F32) + total).astype(BF16)
        copy1_out(rc, core).start()
    for rc in range(NRC):
        copy1_out(rc, 1 - core).wait_recv()

    hidden = jnp.concatenate([mid[0], mid[1]], axis=1)
    normed = norm_rows(hidden.astype(F32), gm[layer:layer + 1, :])
    for j in range(NCH):
        load(0, j).wait()
        gate = jnp.dot(normed, wg[j], preferred_element_type=F32)
        load(1, j).wait()
        up = jnp.dot(normed, wu[j], preferred_element_type=F32)
        act[:, j * CW:(j + 1) * CW] = (gate * jax.nn.sigmoid(gate) * up).astype(BF16)
    for j in range(NCH):
        load(2, j).wait()

    def copy2(j):
        return remote(send2.at[j], recv2.at[j], sems2, 0, j, sibling)

    def copy2_peer(j):
        return remote(pair2.at[j], peer2.at[j], sems2, 1, j, peer)

    def copy2_out(j, half):
        return remote(last.at[half * 2 + j], last.at[half * 2 + j], sems2, 2, j, sibling)

    def down(j):
        return jnp.dot(act[...], wd[j], preferred_element_type=F32)

    def to_sibling2(j):
        send2[j] = down(2 - core * 2 + j).astype(BF16)
        copy2(j).start()

    def to_peer2(j, own):
        copy2(j).wait_recv()
        pair2[j] = (own + recv2[j].astype(F32)).astype(BF16)
        copy2_peer(j).start()

    to_sibling2(0)
    own = down(core * 2)
    to_sibling2(1)
    to_peer2(0, own)
    to_peer2(1, down(core * 2 + 1))
    for j in range(2):
        copy2_peer(j).wait_recv()
        total = pair2[j].astype(F32) + peer2[j].astype(F32)
        last[core * 2 + j] = (mid[core, :, j * CW:(j + 1) * CW].astype(F32) + total).astype(BF16)
        copy2_out(j, core).start()
    for j in range(2):
        copy2_out(j, 1 - core).wait_recv()
    for j in range(NCH):
        out_ref[:, j * CW:(j + 1) * CW] = last[j]
    for rc in range(NRC):
        copy1(rc).wait_send()
        copy1_peer(rc).wait_send()
        copy1_out(rc, core).wait_send()
    for j in range(2):
        copy2(j).wait_send()
        copy2_peer(j).wait_send()
        copy2_out(j, core).wait_send()


def layer_call(layer, seq_lens, freq, hidden, g_attn, g_mlp, w_q, w_k, w_v, w_o, w_gate, w_up, w_down, k_cache, v_cache):
    tile = pltpu.VMEM((ROWS, KVD, SMAX), BF16)
    chunk1 = pltpu.VMEM((NRC, RC, HALF), BF16)
    chunk2 = pltpu.VMEM((2, ROWS, CW), BF16)
    return pl.pallas_call(
        functools.partial(layer_kernel, layer),
        out_shape=(jax.ShapeDtypeStruct((ROWS, D), BF16), tile, tile),
        in_specs=[HBM] * 15,
        out_specs=(VMEM, VMEM, VMEM),
        scratch_shapes=[
            pltpu.SMEM((1, ROWS), jnp.int32),
            pltpu.VMEM((1, ROWS), jnp.int32),
            pltpu.VMEM((1, 128), F32),
            pltpu.VMEM((ROWS, D), BF16),
            pltpu.VMEM(g_attn.shape, BF16),
            pltpu.VMEM(g_mlp.shape, BF16),
            pltpu.VMEM((D, QD), BF16),
            pltpu.VMEM((D, KVD), BF16),
            pltpu.VMEM((D, KVD), BF16),
            pltpu.VMEM((2, QD, HALF), BF16),
            pltpu.VMEM((NCH, D, CW), BF16),
            pltpu.VMEM((NCH, D, CW), BF16),
            pltpu.VMEM((NCH, FF, CW), BF16),
            pltpu.VMEM((KVD, ROWS), F32),
            pltpu.VMEM((KVD, ROWS), F32),
            pltpu.VMEM((ROWS * 8, 128), F32),
            pltpu.VMEM((ROWS * 8, 128), F32),
            pltpu.VMEM((NRC, RC, HALF), F32),
            chunk1, chunk1, chunk1, chunk1,
            pltpu.VMEM((2, ROWS, HALF), BF16),
            chunk2, chunk2, chunk2, chunk2,
            pltpu.VMEM((NCH, ROWS, CW), BF16),
            pltpu.VMEM((ROWS, FF), BF16),
            pltpu.SemaphoreType.DMA((9,)),
            pltpu.SemaphoreType.DMA((STEPS,)),
            pltpu.SemaphoreType.DMA((STEPS,)),
            pltpu.SemaphoreType.DMA((2,)),
            pltpu.SemaphoreType.DMA((3, NCH)),
            pltpu.SemaphoreType.DMA((6, NRC)),
            pltpu.SemaphoreType.DMA((6, 2)),
        ],
        compiler_params=pltpu.CompilerParams(vmem_limit_bytes=44 * 2 ** 20, collective_id=layer, has_side_effects=True),
        name=f"layer{layer}",
    )(seq_lens, seq_lens, freq, hidden, g_attn, g_mlp, w_q, w_k, w_v, w_o, w_gate, w_up, w_down, k_cache, v_cache)


def write_kernel(layer, aliased, *refs):
    k_ref, v_ref = refs[:2]
    ko_hbm, vo_hbm, sem = refs[4 if aliased else 2:]

    def store(n, i):
        src, dst = ((k_ref, ko_hbm), (v_ref, vo_hbm))[n]
        part = pl.ds(i * SEQS, SEQS)
        return pltpu.make_async_copy(src.at[part], dst.at[layer, part], sem.at[n, i])

    for i in range(STEPS):
        store(0, i).start()
        store(1, i).start()
    for i in range(STEPS):
        store(0, i).wait()
        store(1, i).wait()


def write_call(layer, layers, k_tile, v_tile, outs):
    cache = jax.ShapeDtypeStruct((layers, ROWS, KVD, SMAX), BF16)
    k_tile, v_tile = (pltpu.with_memory_space_constraint(x, pltpu.VMEM) for x in (k_tile, v_tile))
    return pl.pallas_call(
        functools.partial(write_kernel, layer, bool(outs)),
        out_shape=(cache, cache),
        in_specs=[VMEM, VMEM] + [HBM] * len(outs),
        out_specs=(HBM, HBM),
        scratch_shapes=[pltpu.SemaphoreType.DMA((2, STEPS))],
        input_output_aliases={2: 0, 3: 1} if outs else {},
        compiler_params=pltpu.CompilerParams(vmem_limit_bytes=2 ** 20),
        name=f"write{layer}",
    )(k_tile, v_tile, *outs)


def solution(mesh):
    cache_spec = P(None, "dp", None, "tp", None)
    col_spec = P(None, None, "tp")
    row_spec = P(None, "tp", None)
    in_specs = (P("dp", None), P("dp"), cache_spec, cache_spec, P(None, None), col_spec, col_spec, col_spec,
                row_spec, P(None, None), col_spec, col_spec, row_spec)
    out_specs = (P("dp", None), cache_spec, cache_spec)

    def local_step(hidden, seq_lens, k_cache, v_cache, g_attn, w_q, w_k, w_v, w_o, g_mlp, w_gate, w_up, w_down):
        layers = k_cache.shape[0]
        kt = k_cache.transpose(0, 1, 3, 4, 2).reshape(layers, ROWS, KVD, SMAX)
        vt = v_cache.transpose(0, 1, 3, 4, 2).reshape(layers, ROWS, KVD, SMAX)
        freq = jnp.asarray(np.tile(rope_freqs(HEAD), 4)[None, :])
        seq_row = seq_lens.reshape(1, ROWS)
        hidden, g_attn, w_q, w_k, w_v, w_o, g_mlp, w_gate, w_up, w_down, kt, vt, freq, seq_row = (
            pltpu.with_memory_space_constraint(x, pltpu.HBM)
            for x in (hidden, g_attn, w_q, w_k, w_v, w_o, g_mlp, w_gate, w_up, w_down, kt, vt, freq, seq_row))
        outs = ()
        for layer in range(layers):
            hidden, k_tile, v_tile = layer_call(layer, seq_row, freq, hidden, g_attn, g_mlp, w_q, w_k, w_v, w_o, w_gate, w_up,
                                                w_down, kt, vt)
            outs = write_call(layer, layers, k_tile, v_tile, outs)
            hidden, outs = lax.optimization_barrier((hidden, outs))

        def back(cache):
            return cache.reshape(layers, ROWS, 2, HEAD, SMAX).transpose(0, 1, 4, 2, 3)

        return hidden, back(outs[0]), back(outs[1])

    return jax.shard_map(local_step, mesh=mesh, in_specs=in_specs, out_specs=out_specs, check_vma=False)
```

```python
import functools

import jax
import jax.numpy as jnp
import numpy as np
from jax import lax
from jax.experimental import pallas as pl
from jax.experimental.pallas import tpu as pltpu
from jax.sharding import PartitionSpec as P

NORM_EPS = 1e-5
ROPE_THETA = 500000.0
ROPE_FACTOR = 8.0
LOW_FACTOR = 1.0
HIGH_FACTOR = 4.0
ORIG_CONTEXT = 8192.0

ROWS = 128
D = 2048
SMAX = 256
HEAD = 64
KVD = 128
QD = 512
FF = 2048
SEQS = 16
STEPS = ROWS // SEQS
CW = 512
NCH = D // CW
HALF = D // 2
RC = 32
NRC = ROWS // RC
AHEAD = 3
F32 = jnp.float32
BF16 = jnp.bfloat16
MESH = pl.DeviceIdType.MESH
VMEM = pl.BlockSpec(memory_space=pltpu.VMEM)
HBM = pl.BlockSpec(memory_space=pltpu.HBM)


def rope_freqs(head_dim):
    freq_expo = np.arange(0, head_dim, 2).astype(np.float32) / np.float32(head_dim)
    inv_freq = 1.0 / (ROPE_THETA ** freq_expo.astype(np.float64))
    wavelen = 2.0 * np.pi / inv_freq
    smooth = (ORIG_CONTEXT / wavelen - LOW_FACTOR) / (HIGH_FACTOR - LOW_FACTOR)
    blended = (1.0 - smooth) * inv_freq / ROPE_FACTOR + smooth * inv_freq
    return np.where(wavelen > ORIG_CONTEXT / LOW_FACTOR, inv_freq / ROPE_FACTOR,
                    np.where(wavelen < ORIG_CONTEXT / HIGH_FACTOR, inv_freq, blended)).astype(np.float32)


def norm_rows(hidden_f, gain):
    inv_rms = lax.rsqrt(jnp.mean(hidden_f * hidden_f, axis=-1, keepdims=True) + NORM_EPS)
    return (hidden_f * inv_rms * gain.astype(F32)).astype(BF16)


def rope_slab(slab, cos, sin):
    lane = lax.broadcasted_iota(jnp.int32, slab.shape, 1)
    other = jnp.where(lane % HEAD < HEAD // 2, pltpu.roll(slab, 128 - HEAD // 2, 1), pltpu.roll(slab, HEAD // 2, 1))
    return slab * cos + other * sin


def layer_kernel(layer, seq_hbm, seqv_hbm, freq_hbm, h_hbm, ga_hbm, gm_hbm, wq_hbm, wk_hbm, wv_hbm, wo_hbm, wg_hbm, wu_hbm,
                 wd_hbm, k_hbm, v_hbm, out_ref, kbuf, vbuf, seq_ref, seqv, freq, h_ref, ga, gm, wq, wk, wv, wo, wg, wu, wd,
                 knew, vnew, qrow, orow, own1, send1, recv1, pair1, peer1, mid, send2, recv2, pair2, peer2, last, act,
                 sem, ksem, vsem, osem, wsem, sems1, sems2):
    me = lax.axis_index("tp")
    core = lax.rem(me, 2)
    sibling = me + 1 - 2 * core
    peer = lax.rem(me + 2, 4)

    barrier = pltpu.get_barrier_semaphore()
    for other in (sibling, peer):
        pl.semaphore_signal(barrier, inc=1, device_id={"tp": other}, device_id_type=MESH)

    def small(i):
        src, dst = ((seqv_hbm, seqv), (freq_hbm, freq), (h_hbm, h_ref), (ga_hbm, ga), (wk_hbm.at[layer], wk),
                    (wv_hbm.at[layer], wv), (wq_hbm.at[layer], wq), (seq_hbm, seq_ref), (gm_hbm, gm))[i]
        return pltpu.make_async_copy(src, dst, sem.at[i])

    def load_k(i):
        return pltpu.make_async_copy(k_hbm.at[layer, pl.ds(i * SEQS, SEQS)], kbuf.at[pl.ds(i * SEQS, SEQS)], ksem.at[i])

    def load_v(i):
        return pltpu.make_async_copy(v_hbm.at[layer, pl.ds(i * SEQS, SEQS)], vbuf.at[pl.ds(i * SEQS, SEQS)], vsem.at[i])

    def load_o(j):
        return pltpu.make_async_copy(wo_hbm.at[layer, :, pl.ds(j * HALF, HALF)], wo.at[j], osem.at[j])

    def load(kind, j):
        src = (wg_hbm, wu_hbm, wd_hbm)[kind].at[layer, :, pl.ds(j * CW, CW)]
        return pltpu.make_async_copy(src, (wg, wu, wd)[kind].at[j], wsem.at[kind, j])

    def remote(src, dst, sems, i, j, to):
        return pltpu.make_async_remote_copy(src_ref=src, dst_ref=dst, send_sem=sems.at[2 * i, j], recv_sem=sems.at[2 * i + 1, j],
                                            device_id={"tp": to}, device_id_type=MESH)

    for i in range(9):
        small(i).start()
    for i in range(AHEAD):
        load_k(i).start()
        load_v(i).start()

    small(0).wait()
    small(1).wait()
    angle = jnp.broadcast_to(seqv[...].astype(F32), (ROWS, 128)).T * freq[...]
    cos = jnp.cos(angle)
    sin = jnp.sin(angle)
    lane = lax.broadcasted_iota(jnp.int32, (ROWS, 128), 1)
    sin = jnp.where(lane % HEAD < HEAD // 2, -sin, sin)
    small(2).wait()
    small(3).wait()
    normed = norm_rows(h_ref[...].astype(F32), ga[layer:layer + 1, :])
    small(4).wait()
    small(5).wait()
    small(6).wait()
    knew[...] = rope_slab(jnp.dot(normed, wk[...], preferred_element_type=F32), cos, sin).astype(BF16).astype(F32).T
    vnew[...] = jnp.dot(normed, wv[...], preferred_element_type=F32).astype(BF16).astype(F32).T
    for slab_idx in range(4):
        slab = jnp.dot(normed, wq[:, slab_idx * 128:(slab_idx + 1) * 128], preferred_element_type=F32)
        slab = rope_slab(slab, cos, sin).astype(BF16).astype(F32)
        turned = pltpu.roll(slab, HEAD, 1)
        for half in range(2):
            hg = slab_idx * 2 + half
            kv = hg // 4
            qrow[pl.ds(hg, ROWS, stride=8), :] = jnp.where(lane // HEAD == kv, slab if kv == half else turned, 0.0)
    small(7).wait()
    small(8).wait()
    pl.semaphore_wait(barrier, 2)

    def attend(i):
        load_k(i).wait()
        load_v(i).wait()

        @pl.when(i + AHEAD < STEPS)
        def _():
            load_k(i + AHEAD).start()
            load_v(i + AHEAD).start()

        @pl.when(i == 0)
        def _():
            load_o(0).start()
            load_o(1).start()

        lane16 = lax.broadcasted_iota(jnp.int16, (KVD, SMAX), 1)
        lane8 = lax.broadcasted_iota(jnp.int32, (8, SMAX), 1)
        row16 = lax.broadcasted_iota(jnp.int32, (16, 128), 0)
        row8 = lax.broadcasted_iota(jnp.int32, (8, 128), 0)
        lane_o = lax.broadcasted_iota(jnp.int32, (8, 128), 1)
        shift = lax.rem(ROWS - i * SEQS, ROWS)

        def insert(buf, new_ref):
            new = pltpu.roll(new_ref[...], shift, 1)
            for j in range(SEQS):
                b = i * SEQS + j
                column = jnp.broadcast_to(new[:, j:j + 1], (KVD, 128)).astype(BF16)
                here = lane16 == seq_ref[0, b].astype(jnp.int16)
                buf[b] = jnp.where(here, jnp.concatenate([column, column], axis=1), buf[b])

        insert(kbuf, knew)
        insert(vbuf, vnew)
        scores = []
        for p in range(SEQS // 2):
            b = i * SEQS + 2 * p
            q2 = qrow[pl.ds(b * 8, 16), :]
            qb = jnp.concatenate([jnp.where(row16 < 8, q2, 0.0), jnp.where(row16 >= 8, q2, 0.0)], axis=1).astype(BF16)
            kk = kbuf[pl.ds(b, 2)].reshape(2 * KVD, SMAX)
            scores.append(jnp.dot(qb, kk, preferred_element_type=F32) * (HEAD ** -0.5))
        for p in range(SEQS // 2):
            b = i * SEQS + 2 * p
            halves = []
            for j in range(2):
                s = jnp.where(lane8 <= seq_ref[0, b + j], scores[p][8 * j:8 * j + 8], -1e30)
                e = jnp.exp(s - jnp.max(s, axis=-1, keepdims=True))
                halves.append(e / jnp.sum(e, axis=-1, keepdims=True))
            prob = jnp.concatenate(halves, axis=0).astype(BF16)
            vv = vbuf[pl.ds(b, 2)].reshape(2 * KVD, SMAX)
            mix = lax.dot_general(prob, vv, (((1,), (1,)), ((), ())), preferred_element_type=F32)
            for j in range(2):
                m = mix[8 * j:8 * j + 8, 128 * j:128 * j + 128]
                orow[pl.ds((b + j) * 8, 8), :] = jnp.where((row8 < 4) == (lane_o < HEAD), m, pltpu.roll(m, HEAD, 1))

    def rows(rc):
        return pl.ds(pl.multiple_of(rc * RC, RC), RC)

    def copy1(rc):
        return remote(send1.at[rc], recv1.at[rc], sems1, 0, rc, sibling)

    def copy1_peer(rc):
        return remote(pair1.at[rc], peer1.at[rc], sems1, 1, rc, peer)

    def copy1_out(rc, half):
        return remote(mid.at[half, rows(rc)], mid.at[half, rows(rc)], sems1, 2, rc, sibling)

    def to_peer1(rc):
        copy1(rc).wait_recv()
        pair1[rc] = (own1[rc] + recv1[rc].astype(F32)).astype(BF16)
        copy1_peer(rc).start()

    def row_chunk(rc, carry):
        def step(i, c):
            attend(rc * (RC // SEQS) + i)
            return c

        lax.fori_loop(0, RC // SEQS, step, 0)
        parts = []
        lane_r = lax.broadcasted_iota(jnp.int32, (RC, 128), 1)
        for slab_idx in range(4):
            lower = orow[pl.ds(rc * RC * 8 + slab_idx * 2, RC, stride=8), :]
            upper = orow[pl.ds(rc * RC * 8 + slab_idx * 2 + 1, RC, stride=8), :]
            parts.append(jnp.where(lane_r < HEAD, lower, upper).astype(BF16))
        attn = jnp.concatenate(parts, axis=1)

        @pl.when(rc == 0)
        def _():
            load_o(0).wait()
            load_o(1).wait()

        send1[rc] = jnp.dot(attn, wo[1 - core], preferred_element_type=F32).astype(BF16)
        copy1(rc).start()
        own1[rc] = jnp.dot(attn, wo[core], preferred_element_type=F32)

        @pl.when(rc > 0)
        def _():
            to_peer1(rc - 1)

        return carry

    lax.fori_loop(0, NRC, row_chunk, 0)
    load(0, 0).start()
    load(1, 0).start()
    to_peer1(NRC - 1)
    load(0, 1).start()
    load(1, 1).start()
    for rc in range(NRC):
        copy1_peer(rc).wait_recv()
        total = pair1[rc].astype(F32) + peer1[rc].astype(F32)
        residual = h_ref[rc * RC:(rc + 1) * RC, pl.ds(pl.multiple_of(core * HALF, HALF), HALF)]
        mid[core, rc * RC:(rc + 1) * RC] = (residual.astype(F32) + total).astype(BF16)
        copy1_out(rc, core).start()
        if rc < 2:
            load(0, rc + 2).start()
            load(1, rc + 2).start()
    for j in range(NCH):
        load(2, j).start()
    for rc in range(NRC):
        copy1_out(rc, 1 - core).wait_recv()

    hidden = jnp.concatenate([mid[0], mid[1]], axis=1)
    normed = norm_rows(hidden.astype(F32), gm[layer:layer + 1, :])
    for j in range(NCH):
        load(0, j).wait()
        gate = jnp.dot(normed, wg[j], preferred_element_type=F32)
        load(1, j).wait()
        up = jnp.dot(normed, wu[j], preferred_element_type=F32)
        act[:, j * CW:(j + 1) * CW] = (gate * jax.nn.sigmoid(gate) * up).astype(BF16)
    for j in range(NCH):
        load(2, j).wait()

    def copy2(j):
        return remote(send2.at[j], recv2.at[j], sems2, 0, j, sibling)

    def copy2_peer(j):
        return remote(pair2.at[j], peer2.at[j], sems2, 1, j, peer)

    def copy2_out(j, half):
        return remote(last.at[half * 2 + j], last.at[half * 2 + j], sems2, 2, j, sibling)

    def down(j):
        return jnp.dot(act[...], wd[j], preferred_element_type=F32)

    def to_sibling2(j):
        send2[j] = down(2 - core * 2 + j).astype(BF16)
        copy2(j).start()

    def to_peer2(j, own):
        copy2(j).wait_recv()
        pair2[j] = (own + recv2[j].astype(F32)).astype(BF16)
        copy2_peer(j).start()

    to_sibling2(0)
    own = down(core * 2)
    to_sibling2(1)
    to_peer2(0, own)
    to_peer2(1, down(core * 2 + 1))
    for j in range(2):
        copy2_peer(j).wait_recv()
        total = pair2[j].astype(F32) + peer2[j].astype(F32)
        last[core * 2 + j] = (mid[core, :, j * CW:(j + 1) * CW].astype(F32) + total).astype(BF16)
        copy2_out(j, core).start()
    for j in range(2):
        copy2_out(j, 1 - core).wait_recv()
    for j in range(NCH):
        out_ref[:, j * CW:(j + 1) * CW] = last[j]
    for rc in range(NRC):
        copy1(rc).wait_send()
        copy1_peer(rc).wait_send()
        copy1_out(rc, core).wait_send()
    for j in range(2):
        copy2(j).wait_send()
        copy2_peer(j).wait_send()
        copy2_out(j, core).wait_send()


def layer_call(layer, seq_lens, freq, hidden, g_attn, g_mlp, w_q, w_k, w_v, w_o, w_gate, w_up, w_down, k_cache, v_cache):
    tile = pltpu.VMEM((ROWS, KVD, SMAX), BF16)
    chunk1 = pltpu.VMEM((NRC, RC, HALF), BF16)
    chunk2 = pltpu.VMEM((2, ROWS, CW), BF16)
    return pl.pallas_call(
        functools.partial(layer_kernel, layer),
        out_shape=(jax.ShapeDtypeStruct((ROWS, D), BF16), tile, tile),
        in_specs=[HBM] * 15,
        out_specs=(VMEM, VMEM, VMEM),
        scratch_shapes=[
            pltpu.SMEM((1, ROWS), jnp.int32),
            pltpu.VMEM((1, ROWS), jnp.int32),
            pltpu.VMEM((1, 128), F32),
            pltpu.VMEM((ROWS, D), BF16),
            pltpu.VMEM(g_attn.shape, BF16),
            pltpu.VMEM(g_mlp.shape, BF16),
            pltpu.VMEM((D, QD), BF16),
            pltpu.VMEM((D, KVD), BF16),
            pltpu.VMEM((D, KVD), BF16),
            pltpu.VMEM((2, QD, HALF), BF16),
            pltpu.VMEM((NCH, D, CW), BF16),
            pltpu.VMEM((NCH, D, CW), BF16),
            pltpu.VMEM((NCH, FF, CW), BF16),
            pltpu.VMEM((KVD, ROWS), F32),
            pltpu.VMEM((KVD, ROWS), F32),
            pltpu.VMEM((ROWS * 8, 128), F32),
            pltpu.VMEM((ROWS * 8, 128), F32),
            pltpu.VMEM((NRC, RC, HALF), F32),
            chunk1, chunk1, chunk1, chunk1,
            pltpu.VMEM((2, ROWS, HALF), BF16),
            chunk2, chunk2, chunk2, chunk2,
            pltpu.VMEM((NCH, ROWS, CW), BF16),
            pltpu.VMEM((ROWS, FF), BF16),
            pltpu.SemaphoreType.DMA((9,)),
            pltpu.SemaphoreType.DMA((STEPS,)),
            pltpu.SemaphoreType.DMA((STEPS,)),
            pltpu.SemaphoreType.DMA((2,)),
            pltpu.SemaphoreType.DMA((3, NCH)),
            pltpu.SemaphoreType.DMA((6, NRC)),
            pltpu.SemaphoreType.DMA((6, 2)),
        ],
        compiler_params=pltpu.CompilerParams(vmem_limit_bytes=44 * 2 ** 20, collective_id=layer, has_side_effects=True),
        name=f"layer{layer}",
    )(seq_lens, seq_lens, freq, hidden, g_attn, g_mlp, w_q, w_k, w_v, w_o, w_gate, w_up, w_down, k_cache, v_cache)


def write_kernel(layer, aliased, *refs):
    k_ref, v_ref = refs[:2]
    ko_hbm, vo_hbm, sem = refs[4 if aliased else 2:]

    def store(n, i):
        src, dst = ((k_ref, ko_hbm), (v_ref, vo_hbm))[n]
        part = pl.ds(i * SEQS, SEQS)
        return pltpu.make_async_copy(src.at[part], dst.at[layer, part], sem.at[n, i])

    for i in range(STEPS):
        store(0, i).start()
        store(1, i).start()
    for i in range(STEPS):
        store(0, i).wait()
        store(1, i).wait()


def write_call(layer, layers, k_tile, v_tile, outs):
    cache = jax.ShapeDtypeStruct((layers, ROWS, KVD, SMAX), BF16)
    k_tile, v_tile = (pltpu.with_memory_space_constraint(x, pltpu.VMEM) for x in (k_tile, v_tile))
    return pl.pallas_call(
        functools.partial(write_kernel, layer, bool(outs)),
        out_shape=(cache, cache),
        in_specs=[VMEM, VMEM] + [HBM] * len(outs),
        out_specs=(HBM, HBM),
        scratch_shapes=[pltpu.SemaphoreType.DMA((2, STEPS))],
        input_output_aliases={2: 0, 3: 1} if outs else {},
        compiler_params=pltpu.CompilerParams(vmem_limit_bytes=2 ** 20),
        name=f"write{layer}",
    )(k_tile, v_tile, *outs)


def solution(mesh):
    cache_spec = P(None, "dp", None, "tp", None)
    col_spec = P(None, None, "tp")
    row_spec = P(None, "tp", None)
    in_specs = (P("dp", None), P("dp"), cache_spec, cache_spec, P(None, None), col_spec, col_spec, col_spec,
                row_spec, P(None, None), col_spec, col_spec, row_spec)
    out_specs = (P("dp", None), cache_spec, cache_spec)

    def local_step(hidden, seq_lens, k_cache, v_cache, g_attn, w_q, w_k, w_v, w_o, g_mlp, w_gate, w_up, w_down):
        layers = k_cache.shape[0]
        kt = k_cache.transpose(0, 1, 3, 4, 2).reshape(layers, ROWS, KVD, SMAX)
        vt = v_cache.transpose(0, 1, 3, 4, 2).reshape(layers, ROWS, KVD, SMAX)
        freq = jnp.asarray(np.tile(rope_freqs(HEAD), 4)[None, :])
        seq_row = seq_lens.reshape(1, ROWS)
        hidden, g_attn, w_q, w_k, w_v, w_o, g_mlp, w_gate, w_up, w_down, kt, vt, freq, seq_row = (
            pltpu.with_memory_space_constraint(x, pltpu.HBM)
            for x in (hidden, g_attn, w_q, w_k, w_v, w_o, g_mlp, w_gate, w_up, w_down, kt, vt, freq, seq_row))
        outs = ()
        for layer in range(layers):
            hidden, k_tile, v_tile = layer_call(layer, seq_row, freq, hidden, g_attn, g_mlp, w_q, w_k, w_v, w_o, w_gate, w_up,
                                                w_down, kt, vt)
            outs = write_call(layer, layers, k_tile, v_tile, outs)
            hidden, outs = lax.optimization_barrier((hidden, outs))

        def back(cache):
            return cache.reshape(layers, ROWS, 2, HEAD, SMAX).transpose(0, 1, 4, 2, 3)

        return hidden, back(outs[0]), back(outs[1])

    return jax.shard_map(local_step, mesh=mesh, in_specs=in_specs, out_specs=out_specs, check_vma=False)
```

```python
import functools

import jax
import jax.numpy as jnp
import numpy as np
from jax import lax
from jax.experimental import pallas as pl
from jax.experimental.pallas import tpu as pltpu
from jax.sharding import PartitionSpec as P

NORM_EPS = 1e-5
ROPE_THETA = 500000.0
ROPE_FACTOR = 8.0
LOW_FACTOR = 1.0
HIGH_FACTOR = 4.0
ORIG_CONTEXT = 8192.0

ROWS = 128
D = 2048
SMAX = 256
HEAD = 64
KVD = 128
QD = 512
FF = 2048
SEQS = 16
STEPS = ROWS // SEQS
CW = 512
NCH = D // CW
HALF = D // 2
RC = 32
NRC = ROWS // RC
AHEAD = 3
F32 = jnp.float32
BF16 = jnp.bfloat16
MESH = pl.DeviceIdType.MESH
VMEM = pl.BlockSpec(memory_space=pltpu.VMEM)
HBM = pl.BlockSpec(memory_space=pltpu.HBM)


def rope_freqs(head_dim):
    freq_expo = np.arange(0, head_dim, 2).astype(np.float32) / np.float32(head_dim)
    inv_freq = 1.0 / (ROPE_THETA ** freq_expo.astype(np.float64))
    wavelen = 2.0 * np.pi / inv_freq
    smooth = (ORIG_CONTEXT / wavelen - LOW_FACTOR) / (HIGH_FACTOR - LOW_FACTOR)
    blended = (1.0 - smooth) * inv_freq / ROPE_FACTOR + smooth * inv_freq
    return np.where(wavelen > ORIG_CONTEXT / LOW_FACTOR, inv_freq / ROPE_FACTOR,
                    np.where(wavelen < ORIG_CONTEXT / HIGH_FACTOR, inv_freq, blended)).astype(np.float32)


def norm_rows(hidden_f, gain):
    inv_rms = lax.rsqrt(jnp.mean(hidden_f * hidden_f, axis=-1, keepdims=True) + NORM_EPS)
    return (hidden_f * inv_rms * gain.astype(F32)).astype(BF16)


def rope_slab(slab, cos, sin):
    lane = lax.broadcasted_iota(jnp.int32, slab.shape, 1)
    other = jnp.where(lane % HEAD < HEAD // 2, pltpu.roll(slab, 128 - HEAD // 2, 1), pltpu.roll(slab, HEAD // 2, 1))
    return slab * cos + other * sin


def layer_kernel(layer, seq_hbm, seqv_hbm, freq_hbm, h_hbm, ga_hbm, gm_hbm, wq_hbm, wk_hbm, wv_hbm, wo_hbm, wg_hbm, wu_hbm,
                 wd_hbm, k_hbm, v_hbm, out_ref, kbuf, vbuf, seq_ref, seqv, freq, h_ref, ga, gm, wq, wk, wv, wo, wg, wu, wd,
                 knew, vnew, qrow, orow, own1, send1, recv1, pair1, peer1, mid, send2, recv2, pair2, peer2, last, act,
                 sem, ksem, vsem, osem, wsem, sems1, sems2):
    me = lax.axis_index("tp")
    core = lax.rem(me, 2)
    sibling = me + 1 - 2 * core
    peer = lax.rem(me + 2, 4)

    barrier = pltpu.get_barrier_semaphore()
    for other in (sibling, peer):
        pl.semaphore_signal(barrier, inc=1, device_id={"tp": other}, device_id_type=MESH)

    def small(i):
        src, dst = ((seqv_hbm, seqv), (freq_hbm, freq), (h_hbm, h_ref), (ga_hbm, ga), (wk_hbm.at[layer], wk),
                    (wv_hbm.at[layer], wv), (wq_hbm.at[layer], wq), (seq_hbm, seq_ref), (gm_hbm, gm))[i]
        return pltpu.make_async_copy(src, dst, sem.at[i])

    def load_k(i):
        return pltpu.make_async_copy(k_hbm.at[layer, pl.ds(i * SEQS, SEQS)], kbuf.at[pl.ds(i * SEQS, SEQS)], ksem.at[i])

    def load_v(i):
        return pltpu.make_async_copy(v_hbm.at[layer, pl.ds(i * SEQS, SEQS)], vbuf.at[pl.ds(i * SEQS, SEQS)], vsem.at[i])

    def load_o():
        return pltpu.make_async_copy(wo_hbm.at[layer], wo, osem.at[0])

    def load(kind, j):
        part = pl.ds(j * CW, CW)
        return pltpu.make_async_copy((wg_hbm, wu_hbm, wd_hbm)[kind].at[layer, part], (wg, wu, wd)[kind].at[part], wsem.at[kind, j])

    def half_cols(half):
        return pl.ds(pl.multiple_of(half * HALF, HALF), HALF)

    def remote(src, dst, sems, i, j, to):
        return pltpu.make_async_remote_copy(src_ref=src, dst_ref=dst, send_sem=sems.at[2 * i, j], recv_sem=sems.at[2 * i + 1, j],
                                            device_id={"tp": to}, device_id_type=MESH)

    for i in range(9):
        small(i).start()
    for i in range(AHEAD):
        load_k(i).start()
        load_v(i).start()

    small(0).wait()
    small(1).wait()
    angle = jnp.broadcast_to(seqv[...].astype(F32), (ROWS, 128)).T * freq[...]
    cos = jnp.cos(angle)
    sin = jnp.sin(angle)
    lane = lax.broadcasted_iota(jnp.int32, (ROWS, 128), 1)
    sin = jnp.where(lane % HEAD < HEAD // 2, -sin, sin)
    small(2).wait()
    small(3).wait()
    normed = norm_rows(h_ref[...].astype(F32), ga[layer:layer + 1, :])
    small(4).wait()
    small(5).wait()
    small(6).wait()
    knew[...] = rope_slab(jnp.dot(normed, wk[...], preferred_element_type=F32), cos, sin).astype(BF16).astype(F32).T
    vnew[...] = jnp.dot(normed, wv[...], preferred_element_type=F32).astype(BF16).astype(F32).T
    for slab_idx in range(4):
        slab = jnp.dot(normed, wq[:, slab_idx * 128:(slab_idx + 1) * 128], preferred_element_type=F32)
        slab = rope_slab(slab, cos, sin).astype(BF16).astype(F32)
        turned = pltpu.roll(slab, HEAD, 1)
        for half in range(2):
            hg = slab_idx * 2 + half
            kv = hg // 4
            qrow[pl.ds(hg, ROWS, stride=8), :] = jnp.where(lane // HEAD == kv, slab if kv == half else turned, 0.0)
    small(7).wait()
    small(8).wait()
    pl.semaphore_wait(barrier, 2)

    def attend(i):
        load_k(i).wait()
        load_v(i).wait()

        @pl.when(i + AHEAD < STEPS)
        def _():
            load_k(i + AHEAD).start()
            load_v(i + AHEAD).start()

        @pl.when(i == 0)
        def _():
            load_o().start()

        lane16 = lax.broadcasted_iota(jnp.int16, (KVD, SMAX), 1)
        lane8 = lax.broadcasted_iota(jnp.int32, (8, SMAX), 1)
        row16 = lax.broadcasted_iota(jnp.int32, (16, 128), 0)
        row8 = lax.broadcasted_iota(jnp.int32, (8, 128), 0)
        lane_o = lax.broadcasted_iota(jnp.int32, (8, 128), 1)
        shift = lax.rem(ROWS - i * SEQS, ROWS)

        def insert(buf, new_ref):
            new = pltpu.roll(new_ref[...], shift, 1)
            for j in range(SEQS):
                b = i * SEQS + j
                column = jnp.broadcast_to(new[:, j:j + 1], (KVD, 128)).astype(BF16)
                here = lane16 == seq_ref[0, b].astype(jnp.int16)
                buf[b] = jnp.where(here, jnp.concatenate([column, column], axis=1), buf[b])

        insert(kbuf, knew)
        insert(vbuf, vnew)
        scores = []
        for p in range(SEQS // 2):
            b = i * SEQS + 2 * p
            q2 = qrow[pl.ds(b * 8, 16), :]
            qb = jnp.concatenate([jnp.where(row16 < 8, q2, 0.0), jnp.where(row16 >= 8, q2, 0.0)], axis=1).astype(BF16)
            kk = kbuf[pl.ds(b, 2)].reshape(2 * KVD, SMAX)
            scores.append(jnp.dot(qb, kk, preferred_element_type=F32) * (HEAD ** -0.5))
        for p in range(SEQS // 2):
            b = i * SEQS + 2 * p
            halves = []
            for j in range(2):
                s = jnp.where(lane8 <= seq_ref[0, b + j], scores[p][8 * j:8 * j + 8], -1e30)
                e = jnp.exp(s - jnp.max(s, axis=-1, keepdims=True))
                halves.append(e / jnp.sum(e, axis=-1, keepdims=True))
            prob = jnp.concatenate(halves, axis=0).astype(BF16)
            vv = vbuf[pl.ds(b, 2)].reshape(2 * KVD, SMAX)
            mix = lax.dot_general(prob, vv, (((1,), (1,)), ((), ())), preferred_element_type=F32)
            for j in range(2):
                m = mix[8 * j:8 * j + 8, 128 * j:128 * j + 128]
                orow[pl.ds((b + j) * 8, 8), :] = jnp.where((row8 < 4) == (lane_o < HEAD), m, pltpu.roll(m, HEAD, 1))

    def rows(rc):
        return pl.ds(pl.multiple_of(rc * RC, RC), RC)

    def copy1(rc):
        return remote(send1.at[rc], recv1.at[rc], sems1, 0, rc, sibling)

    def copy1_peer(rc):
        return remote(pair1.at[rc], peer1.at[rc], sems1, 1, rc, peer)

    def copy1_out(rc, half):
        return remote(mid.at[half, rows(rc)], mid.at[half, rows(rc)], sems1, 2, rc, sibling)

    def to_peer1(rc):
        copy1(rc).wait_recv()
        pair1[rc] = (own1[rc] + recv1[rc].astype(F32)).astype(BF16)
        copy1_peer(rc).start()

    def row_chunk(rc, carry):
        def step(i, c):
            attend(rc * (RC // SEQS) + i)
            return c

        lax.fori_loop(0, RC // SEQS, step, 0)
        parts = []
        lane_r = lax.broadcasted_iota(jnp.int32, (RC, 128), 1)
        for slab_idx in range(4):
            lower = orow[pl.ds(rc * RC * 8 + slab_idx * 2, RC, stride=8), :]
            upper = orow[pl.ds(rc * RC * 8 + slab_idx * 2 + 1, RC, stride=8), :]
            parts.append(jnp.where(lane_r < HEAD, lower, upper).astype(BF16))
        attn = jnp.concatenate(parts, axis=1)

        @pl.when(rc == 0)
        def _():
            load_o().wait()

        send1[rc] = jnp.dot(attn, wo[:, half_cols(1 - core)], preferred_element_type=F32).astype(BF16)
        copy1(rc).start()
        own1[rc] = jnp.dot(attn, wo[:, half_cols(core)], preferred_element_type=F32)

        @pl.when(rc > 0)
        def _():
            to_peer1(rc - 1)

        return carry

    lax.fori_loop(0, NRC, row_chunk, 0)
    load(0, 0).start()
    load(1, 0).start()
    to_peer1(NRC - 1)
    load(0, 1).start()
    load(1, 1).start()
    for rc in range(NRC):
        copy1_peer(rc).wait_recv()
        total = pair1[rc].astype(F32) + peer1[rc].astype(F32)
        residual = h_ref[rc * RC:(rc + 1) * RC, half_cols(core)]
        mid[core, rc * RC:(rc + 1) * RC] = (residual.astype(F32) + total).astype(BF16)
        copy1_out(rc, core).start()
        if rc < 2:
            load(0, rc + 2).start()
            load(1, rc + 2).start()
    for j in range(NCH):
        load(2, j).start()
    for rc in range(NRC):
        copy1_out(rc, 1 - core).wait_recv()

    hidden = jnp.concatenate([mid[0], mid[1]], axis=1)
    normed = norm_rows(hidden.astype(F32), gm[layer:layer + 1, :])
    for j in range(NCH):
        load(0, j).wait()
        load(1, j).wait()
    for j in range(NCH):
        gate = jnp.dot(normed, wg[:, j * CW:(j + 1) * CW], preferred_element_type=F32)
        up = jnp.dot(normed, wu[:, j * CW:(j + 1) * CW], preferred_element_type=F32)
        act[:, j * CW:(j + 1) * CW] = (gate * jax.nn.sigmoid(gate) * up).astype(BF16)
    for j in range(NCH):
        load(2, j).wait()

    def copy2(j):
        return remote(send2.at[j], recv2.at[j], sems2, 0, j, sibling)

    def copy2_peer(j):
        return remote(pair2.at[j], peer2.at[j], sems2, 1, j, peer)

    def copy2_out(j, half):
        return remote(last.at[half * 2 + j], last.at[half * 2 + j], sems2, 2, j, sibling)

    def down(j):
        return jnp.dot(act[...], wd[:, pl.ds(pl.multiple_of(j * CW, CW), CW)], preferred_element_type=F32)

    def to_sibling2(j):
        send2[j] = down(2 - core * 2 + j).astype(BF16)
        copy2(j).start()

    def to_peer2(j, own):
        copy2(j).wait_recv()
        pair2[j] = (own + recv2[j].astype(F32)).astype(BF16)
        copy2_peer(j).start()

    to_sibling2(0)
    own = down(core * 2)
    to_sibling2(1)
    to_peer2(0, own)
    to_peer2(1, down(core * 2 + 1))
    for j in range(2):
        copy2_peer(j).wait_recv()
        total = pair2[j].astype(F32) + peer2[j].astype(F32)
        last[core * 2 + j] = (mid[core, :, j * CW:(j + 1) * CW].astype(F32) + total).astype(BF16)
        copy2_out(j, core).start()
    for j in range(2):
        copy2_out(j, 1 - core).wait_recv()
    for j in range(NCH):
        out_ref[:, j * CW:(j + 1) * CW] = last[j]
    for rc in range(NRC):
        copy1(rc).wait_send()
        copy1_peer(rc).wait_send()
        copy1_out(rc, core).wait_send()
    for j in range(2):
        copy2(j).wait_send()
        copy2_peer(j).wait_send()
        copy2_out(j, core).wait_send()


def layer_call(layer, seq_lens, freq, hidden, g_attn, g_mlp, w_q, w_k, w_v, w_o, w_gate, w_up, w_down, k_cache, v_cache):
    tile = pltpu.VMEM((ROWS, KVD, SMAX), BF16)
    chunk1 = pltpu.VMEM((NRC, RC, HALF), BF16)
    chunk2 = pltpu.VMEM((2, ROWS, CW), BF16)
    return pl.pallas_call(
        functools.partial(layer_kernel, layer),
        out_shape=(jax.ShapeDtypeStruct((ROWS, D), BF16), tile, tile),
        in_specs=[HBM] * 15,
        out_specs=(VMEM, VMEM, VMEM),
        scratch_shapes=[
            pltpu.SMEM((1, ROWS), jnp.int32),
            pltpu.VMEM((1, ROWS), jnp.int32),
            pltpu.VMEM((1, 128), F32),
            pltpu.VMEM((ROWS, D), BF16),
            pltpu.VMEM(g_attn.shape, BF16),
            pltpu.VMEM(g_mlp.shape, BF16),
            pltpu.VMEM((D, QD), BF16),
            pltpu.VMEM((D, KVD), BF16),
            pltpu.VMEM((D, KVD), BF16),
            pltpu.VMEM((QD, D), BF16),
            pltpu.VMEM((D, FF), BF16),
            pltpu.VMEM((D, FF), BF16),
            pltpu.VMEM((FF, D), BF16),
            pltpu.VMEM((KVD, ROWS), F32),
            pltpu.VMEM((KVD, ROWS), F32),
            pltpu.VMEM((ROWS * 8, 128), F32),
            pltpu.VMEM((ROWS * 8, 128), F32),
            pltpu.VMEM((NRC, RC, HALF), F32),
            chunk1, chunk1, chunk1, chunk1,
            pltpu.VMEM((2, ROWS, HALF), BF16),
            chunk2, chunk2, chunk2, chunk2,
            pltpu.VMEM((NCH, ROWS, CW), BF16),
            pltpu.VMEM((ROWS, FF), BF16),
            pltpu.SemaphoreType.DMA((9,)),
            pltpu.SemaphoreType.DMA((STEPS,)),
            pltpu.SemaphoreType.DMA((STEPS,)),
            pltpu.SemaphoreType.DMA((1,)),
            pltpu.SemaphoreType.DMA((3, NCH)),
            pltpu.SemaphoreType.DMA((6, NRC)),
            pltpu.SemaphoreType.DMA((6, 2)),
        ],
        compiler_params=pltpu.CompilerParams(vmem_limit_bytes=44 * 2 ** 20, collective_id=layer, has_side_effects=True),
        name=f"layer{layer}",
    )(seq_lens, seq_lens, freq, hidden, g_attn, g_mlp, w_q, w_k, w_v, w_o, w_gate, w_up, w_down, k_cache, v_cache)


def write_kernel(layer, aliased, *refs):
    k_ref, v_ref = refs[:2]
    ko_hbm, vo_hbm, sem = refs[4 if aliased else 2:]

    def store(n, i):
        src, dst = ((k_ref, ko_hbm), (v_ref, vo_hbm))[n]
        part = pl.ds(i * SEQS, SEQS)
        return pltpu.make_async_copy(src.at[part], dst.at[layer, part], sem.at[n, i])

    for i in range(STEPS):
        store(0, i).start()
        store(1, i).start()
    for i in range(STEPS):
        store(0, i).wait()
        store(1, i).wait()


def write_call(layer, layers, k_tile, v_tile, outs):
    cache = jax.ShapeDtypeStruct((layers, ROWS, KVD, SMAX), BF16)
    k_tile, v_tile = (pltpu.with_memory_space_constraint(x, pltpu.VMEM) for x in (k_tile, v_tile))
    return pl.pallas_call(
        functools.partial(write_kernel, layer, bool(outs)),
        out_shape=(cache, cache),
        in_specs=[VMEM, VMEM] + [HBM] * len(outs),
        out_specs=(HBM, HBM),
        scratch_shapes=[pltpu.SemaphoreType.DMA((2, STEPS))],
        input_output_aliases={2: 0, 3: 1} if outs else {},
        compiler_params=pltpu.CompilerParams(vmem_limit_bytes=2 ** 20),
        name=f"write{layer}",
    )(k_tile, v_tile, *outs)


def solution(mesh):
    cache_spec = P(None, "dp", None, "tp", None)
    col_spec = P(None, None, "tp")
    row_spec = P(None, "tp", None)
    in_specs = (P("dp", None), P("dp"), cache_spec, cache_spec, P(None, None), col_spec, col_spec, col_spec,
                row_spec, P(None, None), col_spec, col_spec, row_spec)
    out_specs = (P("dp", None), cache_spec, cache_spec)

    def local_step(hidden, seq_lens, k_cache, v_cache, g_attn, w_q, w_k, w_v, w_o, g_mlp, w_gate, w_up, w_down):
        layers = k_cache.shape[0]
        kt = k_cache.transpose(0, 1, 3, 4, 2).reshape(layers, ROWS, KVD, SMAX)
        vt = v_cache.transpose(0, 1, 3, 4, 2).reshape(layers, ROWS, KVD, SMAX)
        freq = jnp.asarray(np.tile(rope_freqs(HEAD), 4)[None, :])
        seq_row = seq_lens.reshape(1, ROWS)
        hidden, g_attn, w_q, w_k, w_v, w_o, g_mlp, w_gate, w_up, w_down, kt, vt, freq, seq_row = (
            pltpu.with_memory_space_constraint(x, pltpu.HBM)
            for x in (hidden, g_attn, w_q, w_k, w_v, w_o, g_mlp, w_gate, w_up, w_down, kt, vt, freq, seq_row))
        outs = ()
        for layer in range(layers):
            hidden, k_tile, v_tile = layer_call(layer, seq_row, freq, hidden, g_attn, g_mlp, w_q, w_k, w_v, w_o, w_gate, w_up,
                                                w_down, kt, vt)
            outs = write_call(layer, layers, k_tile, v_tile, outs)
            hidden, outs = lax.optimization_barrier((hidden, outs))

        def back(cache):
            return cache.reshape(layers, ROWS, 2, HEAD, SMAX).transpose(0, 1, 4, 2, 3)

        return hidden, back(outs[0]), back(outs[1])

    return jax.shard_map(local_step, mesh=mesh, in_specs=in_specs, out_specs=out_specs, check_vma=False)
```

```python
import functools

import jax
import jax.numpy as jnp
import numpy as np
from jax import lax
from jax.experimental import pallas as pl
from jax.experimental.pallas import tpu as pltpu
from jax.sharding import PartitionSpec as P

NORM_EPS = 1e-5
ROPE_THETA = 500000.0
ROPE_FACTOR = 8.0
LOW_FACTOR = 1.0
HIGH_FACTOR = 4.0
ORIG_CONTEXT = 8192.0

ROWS = 128
D = 2048
SMAX = 256
HEAD = 64
KVD = 128
QD = 512
FF = 2048
SEQS = 16
STEPS = ROWS // SEQS
CW = 512
NCH = D // CW
HALF = D // 2
RC = 32
NRC = ROWS // RC
AHEAD = 3
F32 = jnp.float32
BF16 = jnp.bfloat16
MESH = pl.DeviceIdType.MESH
VMEM = pl.BlockSpec(memory_space=pltpu.VMEM)
HBM = pl.BlockSpec(memory_space=pltpu.HBM)


def rope_freqs(head_dim):
    freq_expo = np.arange(0, head_dim, 2).astype(np.float32) / np.float32(head_dim)
    inv_freq = 1.0 / (ROPE_THETA ** freq_expo.astype(np.float64))
    wavelen = 2.0 * np.pi / inv_freq
    smooth = (ORIG_CONTEXT / wavelen - LOW_FACTOR) / (HIGH_FACTOR - LOW_FACTOR)
    blended = (1.0 - smooth) * inv_freq / ROPE_FACTOR + smooth * inv_freq
    return np.where(wavelen > ORIG_CONTEXT / LOW_FACTOR, inv_freq / ROPE_FACTOR,
                    np.where(wavelen < ORIG_CONTEXT / HIGH_FACTOR, inv_freq, blended)).astype(np.float32)


def norm_rows(hidden_f, gain):
    inv_rms = lax.rsqrt(jnp.mean(hidden_f * hidden_f, axis=-1, keepdims=True) + NORM_EPS)
    return (hidden_f * inv_rms * gain.astype(F32)).astype(BF16)


def rope_slab(slab, cos, sin):
    lane = lax.broadcasted_iota(jnp.int32, slab.shape, 1)
    other = jnp.where(lane % HEAD < HEAD // 2, pltpu.roll(slab, 128 - HEAD // 2, 1), pltpu.roll(slab, HEAD // 2, 1))
    return slab * cos + other * sin


def layer_kernel(layer, seq_hbm, seqv_hbm, freq_hbm, h_hbm, ga_hbm, gm_hbm, wq_hbm, wk_hbm, wv_hbm, wo_hbm, wg_hbm, wu_hbm,
                 wd_hbm, k_hbm, v_hbm, out_ref, kbuf, vbuf, seq_ref, seqv, freq, h_ref, ga, gm, wq, wk, wv, wo, wg, wu, wd,
                 knew, vnew, krow, vrow, qrow, orow, own1, send1, recv1, pair1, peer1, mid, send2, recv2, pair2, peer2, last, act,
                 sem, ksem, vsem, osem, wsem, sems1, sems2):
    me = lax.axis_index("tp")
    core = lax.rem(me, 2)
    sibling = me + 1 - 2 * core
    peer = lax.rem(me + 2, 4)

    barrier = pltpu.get_barrier_semaphore()
    for other in (sibling, peer):
        pl.semaphore_signal(barrier, inc=1, device_id={"tp": other}, device_id_type=MESH)

    def small(i):
        src, dst = ((seqv_hbm, seqv), (freq_hbm, freq), (h_hbm, h_ref), (ga_hbm, ga), (wk_hbm.at[layer], wk),
                    (wv_hbm.at[layer], wv), (wq_hbm.at[layer], wq), (seq_hbm, seq_ref), (gm_hbm, gm))[i]
        return pltpu.make_async_copy(src, dst, sem.at[i])

    def load_k(i):
        return pltpu.make_async_copy(k_hbm.at[layer, pl.ds(i * SEQS, SEQS)], kbuf.at[pl.ds(i * SEQS, SEQS)], ksem.at[i])

    def load_v(i):
        return pltpu.make_async_copy(v_hbm.at[layer, pl.ds(i * SEQS, SEQS)], vbuf.at[pl.ds(i * SEQS, SEQS)], vsem.at[i])

    def load_o():
        return pltpu.make_async_copy(wo_hbm.at[layer], wo, osem.at[0])

    def load(kind, j):
        part = pl.ds(j * CW, CW)
        return pltpu.make_async_copy((wg_hbm, wu_hbm, wd_hbm)[kind].at[layer, part], (wg, wu, wd)[kind].at[part], wsem.at[kind, j])

    def half_cols(half):
        return pl.ds(pl.multiple_of(half * HALF, HALF), HALF)

    def remote(src, dst, sems, i, j, to):
        return pltpu.make_async_remote_copy(src_ref=src, dst_ref=dst, send_sem=sems.at[2 * i, j], recv_sem=sems.at[2 * i + 1, j],
                                            device_id={"tp": to}, device_id_type=MESH)

    for i in range(9):
        small(i).start()
    small(0).wait()
    small(1).wait()
    angle = jnp.broadcast_to(seqv[...].astype(F32), (ROWS, 128)).T * freq[...]
    cos = jnp.cos(angle)
    sin = jnp.sin(angle)
    lane = lax.broadcasted_iota(jnp.int32, (ROWS, 128), 1)
    sin = jnp.where(lane % HEAD < HEAD // 2, -sin, sin)
    small(2).wait()
    small(3).wait()
    normed = norm_rows(h_ref[...].astype(F32), ga[layer:layer + 1, :])
    small(4).wait()
    small(5).wait()
    small(6).wait()
    for i in range(AHEAD):
        load_k(i).start()
        load_v(i).start()
    k_row = rope_slab(jnp.dot(normed, wk[...], preferred_element_type=F32), cos, sin).astype(BF16).astype(F32)
    v_row = jnp.dot(normed, wv[...], preferred_element_type=F32).astype(BF16).astype(F32)
    krow[...] = k_row
    vrow[...] = v_row
    knew[...] = k_row.T
    vnew[...] = v_row.T
    for slab_idx in range(4):
        slab = jnp.dot(normed, wq[:, slab_idx * 128:(slab_idx + 1) * 128], preferred_element_type=F32)
        slab = rope_slab(slab, cos, sin).astype(BF16).astype(F32)
        turned = pltpu.roll(slab, HEAD, 1)
        for half in range(2):
            hg = slab_idx * 2 + half
            kv = hg // 4
            qrow[pl.ds(hg, ROWS, stride=8), :] = jnp.where(lane // HEAD == kv, slab if kv == half else turned, 0.0)
    small(7).wait()
    small(8).wait()
    pl.semaphore_wait(barrier, 2)

    def attend(i):
        load_k(i).wait()
        load_v(i).wait()

        @pl.when(i + AHEAD < STEPS)
        def _():
            load_k(i + AHEAD).start()
            load_v(i + AHEAD).start()

        @pl.when(i == 0)
        def _():
            load_o().start()

        lane8 = lax.broadcasted_iota(jnp.int32, (8, SMAX), 1)
        row16 = lax.broadcasted_iota(jnp.int32, (16, 128), 0)
        row8 = lax.broadcasted_iota(jnp.int32, (8, 128), 0)
        lane_o = lax.broadcasted_iota(jnp.int32, (8, 128), 1)
        scale = HEAD ** -0.5
        scores = []
        fresh = []
        for p in range(SEQS // 2):
            b = i * SEQS + 2 * p
            q2 = qrow[pl.ds(b * 8, 16), :]
            qb = jnp.concatenate([jnp.where(row16 < 8, q2, 0.0), jnp.where(row16 >= 8, q2, 0.0)], axis=1).astype(BF16)
            kk = kbuf[pl.ds(b, 2)].reshape(2 * KVD, SMAX)
            scores.append(jnp.dot(qb, kk, preferred_element_type=F32) * scale)
            for j in range(2):
                fresh.append(jnp.sum(q2[8 * j:8 * j + 8] * krow[pl.ds(b + j, 1), :], axis=-1, keepdims=True) * scale)
        for p in range(SEQS // 2):
            b = i * SEQS + 2 * p
            halves = []
            added = []
            for j in range(2):
                s = jnp.where(lane8 < seq_ref[0, b + j], scores[p][8 * j:8 * j + 8], -1e30)
                s_new = fresh[2 * p + j]
                peak = jnp.maximum(jnp.max(s, axis=-1, keepdims=True), s_new)
                e = jnp.exp(s - peak)
                e_new = jnp.exp(s_new - peak)
                denom = jnp.sum(e, axis=-1, keepdims=True) + e_new
                halves.append(e / denom)
                added.append((e_new / denom).astype(BF16).astype(F32) * vrow[pl.ds(b + j, 1), :])
            prob = jnp.concatenate(halves, axis=0).astype(BF16)
            vv = vbuf[pl.ds(b, 2)].reshape(2 * KVD, SMAX)
            mix = lax.dot_general(prob, vv, (((1,), (1,)), ((), ())), preferred_element_type=F32)
            for j in range(2):
                m = mix[8 * j:8 * j + 8, 128 * j:128 * j + 128] + added[j]
                orow[pl.ds((b + j) * 8, 8), :] = jnp.where((row8 < 4) == (lane_o < HEAD), m, pltpu.roll(m, HEAD, 1))

    def insert(i, carry):
        lane16 = lax.broadcasted_iota(jnp.int16, (KVD, SMAX), 1)
        shift = lax.rem(ROWS - i * SEQS, ROWS)
        for buf, new_ref in ((kbuf, knew), (vbuf, vnew)):
            new = pltpu.roll(new_ref[...], shift, 1)
            for j in range(SEQS):
                b = i * SEQS + j
                column = jnp.broadcast_to(new[:, j:j + 1], (KVD, 128)).astype(BF16)
                here = lane16 == seq_ref[0, b].astype(jnp.int16)
                buf[b] = jnp.where(here, jnp.concatenate([column, column], axis=1), buf[b])
        return carry

    def rows(rc):
        return pl.ds(pl.multiple_of(rc * RC, RC), RC)

    def copy1(rc):
        return remote(send1.at[rc], recv1.at[rc], sems1, 0, rc, sibling)

    def copy1_peer(rc):
        return remote(pair1.at[rc], peer1.at[rc], sems1, 1, rc, peer)

    def copy1_out(rc, half):
        return remote(mid.at[half, rows(rc)], mid.at[half, rows(rc)], sems1, 2, rc, sibling)

    def to_peer1(rc):
        copy1(rc).wait_recv()
        pair1[rc] = (own1[rc] + recv1[rc].astype(F32)).astype(BF16)
        copy1_peer(rc).start()

    def row_chunk(rc, carry):
        def step(i, c):
            attend(rc * (RC // SEQS) + i)
            return c

        lax.fori_loop(0, RC // SEQS, step, 0)
        parts = []
        lane_r = lax.broadcasted_iota(jnp.int32, (RC, 128), 1)
        for slab_idx in range(4):
            lower = orow[pl.ds(rc * RC * 8 + slab_idx * 2, RC, stride=8), :]
            upper = orow[pl.ds(rc * RC * 8 + slab_idx * 2 + 1, RC, stride=8), :]
            parts.append(jnp.where(lane_r < HEAD, lower, upper).astype(BF16))
        attn = jnp.concatenate(parts, axis=1)

        @pl.when(rc == 0)
        def _():
            load_o().wait()

        send1[rc] = jnp.dot(attn, wo[:, half_cols(1 - core)], preferred_element_type=F32).astype(BF16)
        copy1(rc).start()
        own1[rc] = jnp.dot(attn, wo[:, half_cols(core)], preferred_element_type=F32)

        @pl.when(rc > 0)
        def _():
            to_peer1(rc - 1)

        @pl.when(rc >= NRC - 2)
        def _():
            load(0, rc - NRC + 2).start()
            load(1, rc - NRC + 2).start()

        return carry

    lax.fori_loop(0, NRC, row_chunk, 0)
    load(0, 2).start()
    load(1, 2).start()
    lax.fori_loop(0, STEPS // 2, insert, 0)
    to_peer1(NRC - 1)
    load(0, 3).start()
    load(1, 3).start()
    lax.fori_loop(STEPS // 2, STEPS, insert, 0)
    for rc in range(NRC):
        copy1_peer(rc).wait_recv()
        total = pair1[rc].astype(F32) + peer1[rc].astype(F32)
        residual = h_ref[rc * RC:(rc + 1) * RC, half_cols(core)]
        mid[core, rc * RC:(rc + 1) * RC] = (residual.astype(F32) + total).astype(BF16)
        copy1_out(rc, core).start()
        load(2, rc).start()
    for rc in range(NRC):
        copy1_out(rc, 1 - core).wait_recv()

    hidden = jnp.concatenate([mid[0], mid[1]], axis=1)
    normed = norm_rows(hidden.astype(F32), gm[layer:layer + 1, :])
    for j in range(NCH):
        load(0, j).wait()
        load(1, j).wait()
    for j in range(NCH):
        gate = jnp.dot(normed, wg[:, j * CW:(j + 1) * CW], preferred_element_type=F32)
        up = jnp.dot(normed, wu[:, j * CW:(j + 1) * CW], preferred_element_type=F32)
        act[:, j * CW:(j + 1) * CW] = (gate * jax.nn.sigmoid(gate) * up).astype(BF16)
    for j in range(NCH):
        load(2, j).wait()

    def copy2(j):
        return remote(send2.at[j], recv2.at[j], sems2, 0, j, sibling)

    def copy2_peer(j):
        return remote(pair2.at[j], peer2.at[j], sems2, 1, j, peer)

    def copy2_out(j, half):
        return remote(last.at[half * 2 + j], last.at[half * 2 + j], sems2, 2, j, sibling)

    def down(j):
        return jnp.dot(act[...], wd[:, pl.ds(pl.multiple_of(j * CW, CW), CW)], preferred_element_type=F32)

    def to_sibling2(j):
        send2[j] = down(2 - core * 2 + j).astype(BF16)
        copy2(j).start()

    def to_peer2(j, own):
        copy2(j).wait_recv()
        pair2[j] = (own + recv2[j].astype(F32)).astype(BF16)
        copy2_peer(j).start()

    to_sibling2(0)
    own = down(core * 2)
    to_sibling2(1)
    to_peer2(0, own)
    to_peer2(1, down(core * 2 + 1))
    for j in range(2):
        copy2_peer(j).wait_recv()
        total = pair2[j].astype(F32) + peer2[j].astype(F32)
        last[core * 2 + j] = (mid[core, :, j * CW:(j + 1) * CW].astype(F32) + total).astype(BF16)
        copy2_out(j, core).start()
    for j in range(2):
        copy2_out(j, 1 - core).wait_recv()
    for j in range(NCH):
        out_ref[:, j * CW:(j + 1) * CW] = last[j]
    for rc in range(NRC):
        copy1(rc).wait_send()
        copy1_peer(rc).wait_send()
        copy1_out(rc, core).wait_send()
    for j in range(2):
        copy2(j).wait_send()
        copy2_peer(j).wait_send()
        copy2_out(j, core).wait_send()


def layer_call(layer, seq_lens, freq, hidden, g_attn, g_mlp, w_q, w_k, w_v, w_o, w_gate, w_up, w_down, k_cache, v_cache):
    tile = pltpu.VMEM((ROWS, KVD, SMAX), BF16)
    chunk1 = pltpu.VMEM((NRC, RC, HALF), BF16)
    chunk2 = pltpu.VMEM((2, ROWS, CW), BF16)
    return pl.pallas_call(
        functools.partial(layer_kernel, layer),
        out_shape=(jax.ShapeDtypeStruct((ROWS, D), BF16), tile, tile),
        in_specs=[HBM] * 15,
        out_specs=(VMEM, VMEM, VMEM),
        scratch_shapes=[
            pltpu.SMEM((1, ROWS), jnp.int32),
            pltpu.VMEM((1, ROWS), jnp.int32),
            pltpu.VMEM((1, 128), F32),
            pltpu.VMEM((ROWS, D), BF16),
            pltpu.VMEM(g_attn.shape, BF16),
            pltpu.VMEM(g_mlp.shape, BF16),
            pltpu.VMEM((D, QD), BF16),
            pltpu.VMEM((D, KVD), BF16),
            pltpu.VMEM((D, KVD), BF16),
            pltpu.VMEM((QD, D), BF16),
            pltpu.VMEM((D, FF), BF16),
            pltpu.VMEM((D, FF), BF16),
            pltpu.VMEM((FF, D), BF16),
            pltpu.VMEM((KVD, ROWS), F32),
            pltpu.VMEM((KVD, ROWS), F32),
            pltpu.VMEM((ROWS, KVD), F32),
            pltpu.VMEM((ROWS, KVD), F32),
            pltpu.VMEM((ROWS * 8, 128), F32),
            pltpu.VMEM((ROWS * 8, 128), F32),
            pltpu.VMEM((NRC, RC, HALF), F32),
            chunk1, chunk1, chunk1, chunk1,
            pltpu.VMEM((2, ROWS, HALF), BF16),
            chunk2, chunk2, chunk2, chunk2,
            pltpu.VMEM((NCH, ROWS, CW), BF16),
            pltpu.VMEM((ROWS, FF), BF16),
            pltpu.SemaphoreType.DMA((9,)),
            pltpu.SemaphoreType.DMA((STEPS,)),
            pltpu.SemaphoreType.DMA((STEPS,)),
            pltpu.SemaphoreType.DMA((1,)),
            pltpu.SemaphoreType.DMA((3, NCH)),
            pltpu.SemaphoreType.DMA((6, NRC)),
            pltpu.SemaphoreType.DMA((6, 2)),
        ],
        compiler_params=pltpu.CompilerParams(vmem_limit_bytes=44 * 2 ** 20, collective_id=layer, has_side_effects=True),
        name=f"layer{layer}",
    )(seq_lens, seq_lens, freq, hidden, g_attn, g_mlp, w_q, w_k, w_v, w_o, w_gate, w_up, w_down, k_cache, v_cache)


def write_kernel(layer, aliased, *refs):
    k_ref, v_ref = refs[:2]
    ko_hbm, vo_hbm, sem = refs[4 if aliased else 2:]

    def store(n, i):
        src, dst = ((k_ref, ko_hbm), (v_ref, vo_hbm))[n]
        part = pl.ds(i * SEQS, SEQS)
        return pltpu.make_async_copy(src.at[part], dst.at[layer, part], sem.at[n, i])

    for i in range(STEPS):
        store(0, i).start()
        store(1, i).start()
    for i in range(STEPS):
        store(0, i).wait()
        store(1, i).wait()


def write_call(layer, layers, k_tile, v_tile, outs):
    cache = jax.ShapeDtypeStruct((layers, ROWS, KVD, SMAX), BF16)
    k_tile, v_tile = (pltpu.with_memory_space_constraint(x, pltpu.VMEM) for x in (k_tile, v_tile))
    return pl.pallas_call(
        functools.partial(write_kernel, layer, bool(outs)),
        out_shape=(cache, cache),
        in_specs=[VMEM, VMEM] + [HBM] * len(outs),
        out_specs=(HBM, HBM),
        scratch_shapes=[pltpu.SemaphoreType.DMA((2, STEPS))],
        input_output_aliases={2: 0, 3: 1} if outs else {},
        compiler_params=pltpu.CompilerParams(vmem_limit_bytes=2 ** 20),
        name=f"write{layer}",
    )(k_tile, v_tile, *outs)


def solution(mesh):
    cache_spec = P(None, "dp", None, "tp", None)
    col_spec = P(None, None, "tp")
    row_spec = P(None, "tp", None)
    in_specs = (P("dp", None), P("dp"), cache_spec, cache_spec, P(None, None), col_spec, col_spec, col_spec,
                row_spec, P(None, None), col_spec, col_spec, row_spec)
    out_specs = (P("dp", None), cache_spec, cache_spec)

    def local_step(hidden, seq_lens, k_cache, v_cache, g_attn, w_q, w_k, w_v, w_o, g_mlp, w_gate, w_up, w_down):
        layers = k_cache.shape[0]
        kt = k_cache.transpose(0, 1, 3, 4, 2).reshape(layers, ROWS, KVD, SMAX)
        vt = v_cache.transpose(0, 1, 3, 4, 2).reshape(layers, ROWS, KVD, SMAX)
        freq = jnp.asarray(np.tile(rope_freqs(HEAD), 4)[None, :])
        seq_row = seq_lens.reshape(1, ROWS)
        hidden, g_attn, w_q, w_k, w_v, w_o, g_mlp, w_gate, w_up, w_down, kt, vt, freq, seq_row = (
            pltpu.with_memory_space_constraint(x, pltpu.HBM)
            for x in (hidden, g_attn, w_q, w_k, w_v, w_o, g_mlp, w_gate, w_up, w_down, kt, vt, freq, seq_row))
        outs = ()
        for layer in range(layers):
            hidden, k_tile, v_tile = layer_call(layer, seq_row, freq, hidden, g_attn, g_mlp, w_q, w_k, w_v, w_o, w_gate, w_up,
                                                w_down, kt, vt)
            outs = write_call(layer, layers, k_tile, v_tile, outs)
            hidden, outs = lax.optimization_barrier((hidden, outs))

        def back(cache):
            return cache.reshape(layers, ROWS, 2, HEAD, SMAX).transpose(0, 1, 4, 2, 3)

        return hidden, back(outs[0]), back(outs[1])

    return jax.shard_map(local_step, mesh=mesh, in_specs=in_specs, out_specs=out_specs, check_vma=False)
```

```python
import functools

import jax
import jax.numpy as jnp
import numpy as np
from jax import lax
from jax.experimental import pallas as pl
from jax.experimental.pallas import tpu as pltpu
from jax.sharding import PartitionSpec as P

NORM_EPS = 1e-5
ROPE_THETA = 500000.0
ROPE_FACTOR = 8.0
LOW_FACTOR = 1.0
HIGH_FACTOR = 4.0
ORIG_CONTEXT = 8192.0

ROWS = 128
D = 2048
SMAX = 256
HEAD = 64
KVD = 128
QD = 512
FF = 2048
SEQS = 16
STEPS = ROWS // SEQS
CW = 512
NCH = D // CW
HALF = D // 2
RC = 32
NRC = ROWS // RC
AHEAD = 3
F32 = jnp.float32
BF16 = jnp.bfloat16
MESH = pl.DeviceIdType.MESH
VMEM = pl.BlockSpec(memory_space=pltpu.VMEM)
HBM = pl.BlockSpec(memory_space=pltpu.HBM)


def rope_freqs(head_dim):
    freq_expo = np.arange(0, head_dim, 2).astype(np.float32) / np.float32(head_dim)
    inv_freq = 1.0 / (ROPE_THETA ** freq_expo.astype(np.float64))
    wavelen = 2.0 * np.pi / inv_freq
    smooth = (ORIG_CONTEXT / wavelen - LOW_FACTOR) / (HIGH_FACTOR - LOW_FACTOR)
    blended = (1.0 - smooth) * inv_freq / ROPE_FACTOR + smooth * inv_freq
    return np.where(wavelen > ORIG_CONTEXT / LOW_FACTOR, inv_freq / ROPE_FACTOR,
                    np.where(wavelen < ORIG_CONTEXT / HIGH_FACTOR, inv_freq, blended)).astype(np.float32)


def norm_rows(hidden_f, gain):
    inv_rms = lax.rsqrt(jnp.mean(hidden_f * hidden_f, axis=-1, keepdims=True) + NORM_EPS)
    return (hidden_f * inv_rms * gain.astype(F32)).astype(BF16)


def rope_slab(slab, cos, sin):
    lane = lax.broadcasted_iota(jnp.int32, slab.shape, 1)
    other = jnp.where(lane % HEAD < HEAD // 2, pltpu.roll(slab, 128 - HEAD // 2, 1), pltpu.roll(slab, HEAD // 2, 1))
    return slab * cos + other * sin


def layer_kernel(layer, seq_hbm, seqv_hbm, freq_hbm, h_hbm, ga_hbm, gm_hbm, wq_hbm, wk_hbm, wv_hbm, wo_hbm, wg_hbm, wu_hbm,
                 wd_hbm, k_hbm, v_hbm, out_ref, kbuf, vbuf, seq_ref, seqv, freq, h_ref, ga, gm, wq, wk, wv, wo, wg, wu, wd,
                 knew, vnew, krow, vrow, qrow, orow, own1, send1, recv1, pair1, peer1, mid, send2, recv2, pair2, peer2, last, act,
                 sem, ksem, vsem, osem, wsem, sems1, sems2):
    me = lax.axis_index("tp")
    core = lax.rem(me, 2)
    sibling = me + 1 - 2 * core
    peer = lax.rem(me + 2, 4)

    barrier = pltpu.get_barrier_semaphore()
    for other in (sibling, peer):
        pl.semaphore_signal(barrier, inc=1, device_id={"tp": other}, device_id_type=MESH)

    def small(i):
        src, dst = ((seqv_hbm, seqv), (freq_hbm, freq), (h_hbm, h_ref), (ga_hbm, ga), (wk_hbm.at[layer], wk),
                    (wv_hbm.at[layer], wv), (wq_hbm.at[layer], wq), (seq_hbm, seq_ref), (gm_hbm, gm))[i]
        return pltpu.make_async_copy(src, dst, sem.at[i])

    def load_k(i):
        return pltpu.make_async_copy(k_hbm.at[layer, pl.ds(i * SEQS, SEQS)], kbuf.at[pl.ds(i * SEQS, SEQS)], ksem.at[i])

    def load_v(i):
        return pltpu.make_async_copy(v_hbm.at[layer, pl.ds(i * SEQS, SEQS)], vbuf.at[pl.ds(i * SEQS, SEQS)], vsem.at[i])

    def load_o():
        return pltpu.make_async_copy(wo_hbm.at[layer], wo, osem.at[0])

    def load(kind, j):
        part = pl.ds(j * CW, CW)
        return pltpu.make_async_copy((wg_hbm, wu_hbm, wd_hbm)[kind].at[layer, part], (wg, wu, wd)[kind].at[part], wsem.at[kind, j])

    def half_cols(half):
        return pl.ds(pl.multiple_of(half * HALF, HALF), HALF)

    def remote(src, dst, sems, i, j, to):
        return pltpu.make_async_remote_copy(src_ref=src, dst_ref=dst, send_sem=sems.at[2 * i, j], recv_sem=sems.at[2 * i + 1, j],
                                            device_id={"tp": to}, device_id_type=MESH)

    for i in range(9):
        small(i).start()
    load_k(0).start()
    load_v(0).start()
    small(0).wait()
    small(1).wait()
    angle = jnp.broadcast_to(seqv[...].astype(F32), (ROWS, 128)).T * freq[...]
    cos = jnp.cos(angle)
    sin = jnp.sin(angle)
    lane = lax.broadcasted_iota(jnp.int32, (ROWS, 128), 1)
    sin = jnp.where(lane % HEAD < HEAD // 2, -sin, sin)
    small(2).wait()
    small(3).wait()
    normed = norm_rows(h_ref[...].astype(F32), ga[layer:layer + 1, :])
    small(4).wait()
    small(5).wait()
    for i in range(1, AHEAD):
        load_k(i).start()
        load_v(i).start()
    k_row = rope_slab(jnp.dot(normed, wk[...], preferred_element_type=F32), cos, sin).astype(BF16).astype(F32)
    v_row = jnp.dot(normed, wv[...], preferred_element_type=F32).astype(BF16).astype(F32)
    krow[...] = k_row
    vrow[...] = v_row
    knew[...] = k_row.T
    vnew[...] = v_row.T
    small(6).wait()
    for slab_idx in range(4):
        slab = jnp.dot(normed, wq[:, slab_idx * 128:(slab_idx + 1) * 128], preferred_element_type=F32)
        slab = rope_slab(slab, cos, sin).astype(BF16).astype(F32)
        turned = pltpu.roll(slab, HEAD, 1)
        for half in range(2):
            hg = slab_idx * 2 + half
            kv = hg // 4
            qrow[pl.ds(hg, ROWS, stride=8), :] = jnp.where(lane // HEAD == kv, slab if kv == half else turned, 0.0)
    small(7).wait()
    small(8).wait()
    pl.semaphore_wait(barrier, 2)

    def attend(i):
        load_k(i).wait()
        load_v(i).wait()

        @pl.when(i + AHEAD < STEPS)
        def _():
            load_k(i + AHEAD).start()
            load_v(i + AHEAD).start()

        @pl.when(i == 0)
        def _():
            load_o().start()

        lane8 = lax.broadcasted_iota(jnp.int32, (8, SMAX), 1)
        row16 = lax.broadcasted_iota(jnp.int32, (16, 128), 0)
        row8 = lax.broadcasted_iota(jnp.int32, (8, 128), 0)
        lane_o = lax.broadcasted_iota(jnp.int32, (8, 128), 1)
        scale = HEAD ** -0.5
        scores = []
        fresh = []
        for p in range(SEQS // 2):
            b = i * SEQS + 2 * p
            q2 = qrow[pl.ds(b * 8, 16), :]
            qb = jnp.concatenate([jnp.where(row16 < 8, q2, 0.0), jnp.where(row16 >= 8, q2, 0.0)], axis=1).astype(BF16)
            kk = kbuf[pl.ds(b, 2)].reshape(2 * KVD, SMAX)
            scores.append(jnp.dot(qb, kk, preferred_element_type=F32) * scale)
            for j in range(2):
                fresh.append(jnp.sum(q2[8 * j:8 * j + 8] * krow[pl.ds(b + j, 1), :], axis=-1, keepdims=True) * scale)
        for p in range(SEQS // 2):
            b = i * SEQS + 2 * p
            halves = []
            added = []
            for j in range(2):
                s = jnp.where(lane8 < seq_ref[0, b + j], scores[p][8 * j:8 * j + 8], -1e30)
                s_new = fresh[2 * p + j]
                peak = jnp.maximum(jnp.max(s, axis=-1, keepdims=True), s_new)
                e = jnp.exp(s - peak)
                e_new = jnp.exp(s_new - peak)
                denom = jnp.sum(e, axis=-1, keepdims=True) + e_new
                halves.append(e / denom)
                added.append((e_new / denom).astype(BF16).astype(F32) * vrow[pl.ds(b + j, 1), :])
            prob = jnp.concatenate(halves, axis=0).astype(BF16)
            vv = vbuf[pl.ds(b, 2)].reshape(2 * KVD, SMAX)
            mix = lax.dot_general(prob, vv, (((1,), (1,)), ((), ())), preferred_element_type=F32)
            for j in range(2):
                m = mix[8 * j:8 * j + 8, 128 * j:128 * j + 128] + added[j]
                orow[pl.ds((b + j) * 8, 8), :] = jnp.where((row8 < 4) == (lane_o < HEAD), m, pltpu.roll(m, HEAD, 1))

    def insert(i, carry):
        lane16 = lax.broadcasted_iota(jnp.int16, (KVD, SMAX), 1)
        shift = lax.rem(ROWS - i * SEQS, ROWS)
        for buf, new_ref in ((kbuf, knew), (vbuf, vnew)):
            new = pltpu.roll(new_ref[...], shift, 1)
            for j in range(SEQS):
                b = i * SEQS + j
                column = jnp.broadcast_to(new[:, j:j + 1], (KVD, 128)).astype(BF16)
                here = lane16 == seq_ref[0, b].astype(jnp.int16)
                buf[b] = jnp.where(here, jnp.concatenate([column, column], axis=1), buf[b])
        return carry

    def rows(rc):
        return pl.ds(pl.multiple_of(rc * RC, RC), RC)

    def copy1(rc):
        return remote(send1.at[rc], recv1.at[rc], sems1, 0, rc, sibling)

    def copy1_peer(rc):
        return remote(pair1.at[rc], peer1.at[rc], sems1, 1, rc, peer)

    def copy1_out(rc, half):
        return remote(mid.at[half, rows(rc)], mid.at[half, rows(rc)], sems1, 2, rc, sibling)

    def to_peer1(rc):
        copy1(rc).wait_recv()
        pair1[rc] = (own1[rc] + recv1[rc].astype(F32)).astype(BF16)
        copy1_peer(rc).start()

    def row_chunk(rc, carry):
        def step(i, c):
            attend(rc * (RC // SEQS) + i)
            return c

        lax.fori_loop(0, RC // SEQS, step, 0)
        parts = []
        lane_r = lax.broadcasted_iota(jnp.int32, (RC, 128), 1)
        for slab_idx in range(4):
            lower = orow[pl.ds(rc * RC * 8 + slab_idx * 2, RC, stride=8), :]
            upper = orow[pl.ds(rc * RC * 8 + slab_idx * 2 + 1, RC, stride=8), :]
            parts.append(jnp.where(lane_r < HEAD, lower, upper).astype(BF16))
        attn = jnp.concatenate(parts, axis=1)

        @pl.when(rc == 0)
        def _():
            load_o().wait()

        send1[rc] = jnp.dot(attn, wo[:, half_cols(1 - core)], preferred_element_type=F32).astype(BF16)
        copy1(rc).start()
        own1[rc] = jnp.dot(attn, wo[:, half_cols(core)], preferred_element_type=F32)

        @pl.when(rc > 0)
        def _():
            to_peer1(rc - 1)

        @pl.when(rc == NRC - 2)
        def _():
            for j in range(NCH):
                load(0, j).start()
                load(1, j).start()

        return carry

    lax.fori_loop(0, NRC, row_chunk, 0)
    for j in range(NCH):
        load(2, j).start()
    lax.fori_loop(0, 1, insert, 0)
    to_peer1(NRC - 1)
    lax.fori_loop(1, STEPS, insert, 0)
    for rc in range(NRC):
        copy1_peer(rc).wait_recv()
        total = pair1[rc].astype(F32) + peer1[rc].astype(F32)
        residual = h_ref[rc * RC:(rc + 1) * RC, half_cols(core)]
        mid[core, rc * RC:(rc + 1) * RC] = (residual.astype(F32) + total).astype(BF16)
        copy1_out(rc, core).start()
    for rc in range(NRC):
        copy1_out(rc, 1 - core).wait_recv()

    hidden = jnp.concatenate([mid[0], mid[1]], axis=1)
    normed = norm_rows(hidden.astype(F32), gm[layer:layer + 1, :])
    for j in range(NCH):
        load(0, j).wait()
        load(1, j).wait()
    for j in range(NCH):
        gate = jnp.dot(normed, wg[:, j * CW:(j + 1) * CW], preferred_element_type=F32)
        up = jnp.dot(normed, wu[:, j * CW:(j + 1) * CW], preferred_element_type=F32)
        act[:, j * CW:(j + 1) * CW] = (gate * jax.nn.sigmoid(gate) * up).astype(BF16)
    for j in range(NCH):
        load(2, j).wait()

    def copy2(j):
        return remote(send2.at[j], recv2.at[j], sems2, 0, j, sibling)

    def copy2_peer(j):
        return remote(pair2.at[j], peer2.at[j], sems2, 1, j, peer)

    def copy2_out(j, half):
        return remote(last.at[half * 2 + j], last.at[half * 2 + j], sems2, 2, j, sibling)

    def down(j):
        return jnp.dot(act[...], wd[:, pl.ds(pl.multiple_of(j * CW, CW), CW)], preferred_element_type=F32)

    def to_sibling2(j):
        send2[j] = down(2 - core * 2 + j).astype(BF16)
        copy2(j).start()

    def to_peer2(j, own):
        copy2(j).wait_recv()
        pair2[j] = (own + recv2[j].astype(F32)).astype(BF16)
        copy2_peer(j).start()

    to_sibling2(0)
    own = down(core * 2)
    to_sibling2(1)
    to_peer2(0, own)
    to_peer2(1, down(core * 2 + 1))
    for j in range(2):
        copy2_peer(j).wait_recv()
        total = pair2[j].astype(F32) + peer2[j].astype(F32)
        last[core * 2 + j] = (mid[core, :, j * CW:(j + 1) * CW].astype(F32) + total).astype(BF16)
        copy2_out(j, core).start()
    for j in range(2):
        copy2_out(j, 1 - core).wait_recv()
    for j in range(NCH):
        out_ref[:, j * CW:(j + 1) * CW] = last[j]
    for rc in range(NRC):
        copy1(rc).wait_send()
        copy1_peer(rc).wait_send()
        copy1_out(rc, core).wait_send()
    for j in range(2):
        copy2(j).wait_send()
        copy2_peer(j).wait_send()
        copy2_out(j, core).wait_send()


def layer_call(layer, last, seq_lens, freq, hidden, g_attn, g_mlp, w_q, w_k, w_v, w_o, w_gate, w_up, w_down, k_cache, v_cache):
    tile = pltpu.VMEM((ROWS, KVD, SMAX), BF16)
    chunk1 = pltpu.VMEM((NRC, RC, HALF), BF16)
    chunk2 = pltpu.VMEM((2, ROWS, CW), BF16)
    return pl.pallas_call(
        functools.partial(layer_kernel, layer),
        out_shape=(pltpu.VMEM((ROWS, D), BF16) if last else jax.ShapeDtypeStruct((ROWS, D), BF16), tile, tile),
        in_specs=[HBM] * 15,
        out_specs=(VMEM, VMEM, VMEM),
        scratch_shapes=[
            pltpu.SMEM((1, ROWS), jnp.int32),
            pltpu.VMEM((1, ROWS), jnp.int32),
            pltpu.VMEM((1, 128), F32),
            pltpu.VMEM((ROWS, D), BF16),
            pltpu.VMEM(g_attn.shape, BF16),
            pltpu.VMEM(g_mlp.shape, BF16),
            pltpu.VMEM((D, QD), BF16),
            pltpu.VMEM((D, KVD), BF16),
            pltpu.VMEM((D, KVD), BF16),
            pltpu.VMEM((QD, D), BF16),
            pltpu.VMEM((D, FF), BF16),
            pltpu.VMEM((D, FF), BF16),
            pltpu.VMEM((FF, D), BF16),
            pltpu.VMEM((KVD, ROWS), F32),
            pltpu.VMEM((KVD, ROWS), F32),
            pltpu.VMEM((ROWS, KVD), F32),
            pltpu.VMEM((ROWS, KVD), F32),
            pltpu.VMEM((ROWS * 8, 128), F32),
            pltpu.VMEM((ROWS * 8, 128), F32),
            pltpu.VMEM((NRC, RC, HALF), F32),
            chunk1, chunk1, chunk1, chunk1,
            pltpu.VMEM((2, ROWS, HALF), BF16),
            chunk2, chunk2, chunk2, chunk2,
            pltpu.VMEM((NCH, ROWS, CW), BF16),
            pltpu.VMEM((ROWS, FF), BF16),
            pltpu.SemaphoreType.DMA((9,)),
            pltpu.SemaphoreType.DMA((STEPS,)),
            pltpu.SemaphoreType.DMA((STEPS,)),
            pltpu.SemaphoreType.DMA((1,)),
            pltpu.SemaphoreType.DMA((3, NCH)),
            pltpu.SemaphoreType.DMA((6, NRC)),
            pltpu.SemaphoreType.DMA((6, 2)),
        ],
        compiler_params=pltpu.CompilerParams(vmem_limit_bytes=44 * 2 ** 20, collective_id=layer, has_side_effects=True),
        name=f"layer{layer}",
    )(seq_lens, seq_lens, freq, hidden, g_attn, g_mlp, w_q, w_k, w_v, w_o, w_gate, w_up, w_down, k_cache, v_cache)


def write_kernel(layer, n_in, *refs):
    sources, results, sem = refs[:n_in], refs[-1 - n_in:-1], refs[-1]
    copies = []
    for n in range(2):
        for i in range(STEPS):
            part = pl.ds(i * SEQS, SEQS)
            copies.append(pltpu.make_async_copy(sources[n].at[part], results[n].at[layer, part], sem.at[n, i]))
    if n_in > 2:
        copies.append(pltpu.make_async_copy(sources[2], results[2], sem.at[2, 0]))
    for copy in copies:
        copy.start()
    for copy in copies:
        copy.wait()


def write_call(layer, layers, tiles, outs):
    cache = jax.ShapeDtypeStruct((layers, ROWS, KVD, SMAX), BF16)
    n_in = len(tiles)
    tiles = [pltpu.with_memory_space_constraint(x, pltpu.VMEM) for x in tiles]
    return pl.pallas_call(
        functools.partial(write_kernel, layer, n_in),
        out_shape=(cache, cache, jax.ShapeDtypeStruct((ROWS, D), BF16))[:n_in],
        in_specs=[VMEM] * n_in + [HBM] * len(outs),
        out_specs=(HBM,) * n_in,
        scratch_shapes=[pltpu.SemaphoreType.DMA((3, STEPS))],
        input_output_aliases={n_in: 0, n_in + 1: 1} if outs else {},
        compiler_params=pltpu.CompilerParams(vmem_limit_bytes=2 ** 20),
        name=f"write{layer}",
    )(*tiles, *outs)


def solution(mesh):
    cache_spec = P(None, "dp", None, "tp", None)
    col_spec = P(None, None, "tp")
    row_spec = P(None, "tp", None)
    in_specs = (P("dp", None), P("dp"), cache_spec, cache_spec, P(None, None), col_spec, col_spec, col_spec,
                row_spec, P(None, None), col_spec, col_spec, row_spec)
    out_specs = (P("dp", None), cache_spec, cache_spec)

    def local_step(hidden, seq_lens, k_cache, v_cache, g_attn, w_q, w_k, w_v, w_o, g_mlp, w_gate, w_up, w_down):
        layers = k_cache.shape[0]
        kt = k_cache.transpose(0, 1, 3, 4, 2).reshape(layers, ROWS, KVD, SMAX)
        vt = v_cache.transpose(0, 1, 3, 4, 2).reshape(layers, ROWS, KVD, SMAX)
        freq = jnp.asarray(np.tile(rope_freqs(HEAD), 4)[None, :])
        seq_row = seq_lens.reshape(1, ROWS)
        hidden, g_attn, w_q, w_k, w_v, w_o, g_mlp, w_gate, w_up, w_down, kt, vt, freq, seq_row = (
            pltpu.with_memory_space_constraint(x, pltpu.HBM)
            for x in (hidden, g_attn, w_q, w_k, w_v, w_o, g_mlp, w_gate, w_up, w_down, kt, vt, freq, seq_row))
        outs = ()
        for layer in range(layers):
            hidden, k_tile, v_tile = layer_call(layer, layer == layers - 1, seq_row, freq, hidden, g_attn, g_mlp, w_q, w_k, w_v, w_o, w_gate, w_up,
                                                w_down, kt, vt)
            if layer < layers - 1:
                outs = write_call(layer, layers, (k_tile, v_tile), outs)
                hidden, outs = lax.optimization_barrier((hidden, outs))
            else:
                *outs, hidden = write_call(layer, layers, (k_tile, v_tile, hidden), outs)

        def back(cache):
            return cache.reshape(layers, ROWS, 2, HEAD, SMAX).transpose(0, 1, 4, 2, 3)

        return hidden, back(outs[0]), back(outs[1])

    return jax.shard_map(local_step, mesh=mesh, in_specs=in_specs, out_specs=out_specs, check_vma=False)
```

```python
import functools

import jax
import jax.numpy as jnp
import numpy as np
from jax import lax
from jax.experimental import pallas as pl
from jax.experimental.pallas import tpu as pltpu
from jax.sharding import PartitionSpec as P

NORM_EPS = 1e-5
ROPE_THETA = 500000.0
ROPE_FACTOR = 8.0
LOW_FACTOR = 1.0
HIGH_FACTOR = 4.0
ORIG_CONTEXT = 8192.0

ROWS = 128
D = 2048
SMAX = 256
HEAD = 64
KVD = 128
QD = 512
FF = 2048
SEQS = 16
STEPS = ROWS // SEQS
CW = 512
NCH = D // CW
HALF = D // 2
RC = 32
NRC = ROWS // RC
AHEAD = 3
F32 = jnp.float32
BF16 = jnp.bfloat16
MESH = pl.DeviceIdType.MESH
VMEM = pl.BlockSpec(memory_space=pltpu.VMEM)
HBM = pl.BlockSpec(memory_space=pltpu.HBM)


def rope_freqs(head_dim):
    freq_expo = np.arange(0, head_dim, 2).astype(np.float32) / np.float32(head_dim)
    inv_freq = 1.0 / (ROPE_THETA ** freq_expo.astype(np.float64))
    wavelen = 2.0 * np.pi / inv_freq
    smooth = (ORIG_CONTEXT / wavelen - LOW_FACTOR) / (HIGH_FACTOR - LOW_FACTOR)
    blended = (1.0 - smooth) * inv_freq / ROPE_FACTOR + smooth * inv_freq
    return np.where(wavelen > ORIG_CONTEXT / LOW_FACTOR, inv_freq / ROPE_FACTOR,
                    np.where(wavelen < ORIG_CONTEXT / HIGH_FACTOR, inv_freq, blended)).astype(np.float32)


def norm_rows(hidden_f, gain):
    inv_rms = lax.rsqrt(jnp.mean(hidden_f * hidden_f, axis=-1, keepdims=True) + NORM_EPS)
    return (hidden_f * inv_rms * gain.astype(F32)).astype(BF16)


def rope_slab(slab, cos, sin):
    lane = lax.broadcasted_iota(jnp.int32, slab.shape, 1)
    other = jnp.where(lane % HEAD < HEAD // 2, pltpu.roll(slab, 128 - HEAD // 2, 1), pltpu.roll(slab, HEAD // 2, 1))
    return slab * cos + other * sin


def layer_kernel(layer, first, last, *refs):
    (seq_hbm, seqv_hbm, freq_hbm, h_in, ga_hbm, gm_hbm, wq_in, wk_in, wv_in, wo_hbm, wg_hbm, wu_hbm, wd_hbm, k_hbm, v_hbm) = refs[:15]
    refs = refs[15:]
    if not first:
        h_ref, wq, wk, wv = h_in, wq_in, wk_in, wv_in
    if not last:
        nq_hbm, nk_hbm, nv_hbm = (wq_in, wk_in, wv_in) if first else refs[:3]
        refs = refs if first else refs[3:]
    out_ref, kbuf, vbuf = refs[:3]
    refs = refs[3:]
    if not last:
        next_q, next_k, next_v = refs[:3]
        refs = refs[3:]
    if first:
        h_ref, wq, wk, wv = refs[:4]
        refs = refs[4:]
    (seq_ref, seqv, freq, ga, gm, wo, wg, wu, wd,
     knew, vnew, krow, vrow, qrow, orow, own1, send1, recv1, pair1, peer1, mid, send2, recv2, pair2, peer2, last2, act,
     sem, ksem, vsem, osem, wsem, nsem, sems1, sems2) = refs
    me = lax.axis_index("tp")
    core = lax.rem(me, 2)
    sibling = me + 1 - 2 * core
    peer = lax.rem(me + 2, 4)

    barrier = pltpu.get_barrier_semaphore()
    for other in (sibling, peer):
        pl.semaphore_signal(barrier, inc=1, device_id={"tp": other}, device_id_type=MESH)

    smalls = {0: (seqv_hbm, seqv), 1: (freq_hbm, freq), 3: (ga_hbm, ga), 7: (seq_hbm, seq_ref), 8: (gm_hbm, gm)}
    if first:
        smalls.update({2: (h_in, h_ref), 4: (wk_in.at[layer], wk), 5: (wv_in.at[layer], wv), 6: (wq_in.at[layer], wq)})

    class Small:
        def __init__(self, i):
            self.copy = pltpu.make_async_copy(*smalls[i], sem.at[i]) if i in smalls else None

        def start(self):
            if self.copy is not None:
                self.copy.start()

        def wait(self):
            if self.copy is not None:
                self.copy.wait()

    small = Small

    def load_next(i):
        src, dst = ((nq_hbm, next_q), (nk_hbm, next_k), (nv_hbm, next_v))[i]
        return pltpu.make_async_copy(src.at[layer + 1], dst, nsem.at[i])

    def load_k(i):
        return pltpu.make_async_copy(k_hbm.at[layer, pl.ds(i * SEQS, SEQS)], kbuf.at[pl.ds(i * SEQS, SEQS)], ksem.at[i])

    def load_v(i):
        return pltpu.make_async_copy(v_hbm.at[layer, pl.ds(i * SEQS, SEQS)], vbuf.at[pl.ds(i * SEQS, SEQS)], vsem.at[i])

    def load_o():
        return pltpu.make_async_copy(wo_hbm.at[layer], wo, osem.at[0])

    def load(kind, j):
        part = pl.ds(j * CW, CW)
        return pltpu.make_async_copy((wg_hbm, wu_hbm, wd_hbm)[kind].at[layer, part], (wg, wu, wd)[kind].at[part], wsem.at[kind, j])

    def half_cols(half):
        return pl.ds(pl.multiple_of(half * HALF, HALF), HALF)

    def remote(src, dst, sems, i, j, to):
        return pltpu.make_async_remote_copy(src_ref=src, dst_ref=dst, send_sem=sems.at[2 * i, j], recv_sem=sems.at[2 * i + 1, j],
                                            device_id={"tp": to}, device_id_type=MESH)

    for i in range(9):
        small(i).start()
    load_k(0).start()
    load_v(0).start()
    small(0).wait()
    small(1).wait()
    angle = jnp.broadcast_to(seqv[...].astype(F32), (ROWS, 128)).T * freq[...]
    cos = jnp.cos(angle)
    sin = jnp.sin(angle)
    lane = lax.broadcasted_iota(jnp.int32, (ROWS, 128), 1)
    sin = jnp.where(lane % HEAD < HEAD // 2, -sin, sin)
    small(2).wait()
    small(3).wait()
    normed = norm_rows(h_ref[...].astype(F32), ga[layer:layer + 1, :])
    small(4).wait()
    small(5).wait()
    for i in range(1, AHEAD):
        load_k(i).start()
        load_v(i).start()
    k_row = rope_slab(jnp.dot(normed, wk[...], preferred_element_type=F32), cos, sin).astype(BF16).astype(F32)
    v_row = jnp.dot(normed, wv[...], preferred_element_type=F32).astype(BF16).astype(F32)
    krow[...] = k_row
    vrow[...] = v_row
    knew[...] = k_row.T
    vnew[...] = v_row.T
    small(6).wait()
    for slab_idx in range(4):
        slab = jnp.dot(normed, wq[:, slab_idx * 128:(slab_idx + 1) * 128], preferred_element_type=F32)
        slab = rope_slab(slab, cos, sin).astype(BF16).astype(F32)
        turned = pltpu.roll(slab, HEAD, 1)
        for half in range(2):
            hg = slab_idx * 2 + half
            kv = hg // 4
            qrow[pl.ds(hg, ROWS, stride=8), :] = jnp.where(lane // HEAD == kv, slab if kv == half else turned, 0.0)
    small(7).wait()
    small(8).wait()

    def attend(i):
        load_k(i).wait()
        load_v(i).wait()

        @pl.when(i + AHEAD < STEPS)
        def _():
            load_k(i + AHEAD).start()
            load_v(i + AHEAD).start()

        @pl.when(i == 0)
        def _():
            load_o().start()

        lane8 = lax.broadcasted_iota(jnp.int32, (8, SMAX), 1)
        row16 = lax.broadcasted_iota(jnp.int32, (16, 128), 0)
        row8 = lax.broadcasted_iota(jnp.int32, (8, 128), 0)
        lane_o = lax.broadcasted_iota(jnp.int32, (8, 128), 1)
        scale = HEAD ** -0.5
        scores = []
        fresh = []
        for p in range(SEQS // 2):
            b = i * SEQS + 2 * p
            q2 = qrow[pl.ds(b * 8, 16), :]
            qb = jnp.concatenate([jnp.where(row16 < 8, q2, 0.0), jnp.where(row16 >= 8, q2, 0.0)], axis=1).astype(BF16)
            kk = kbuf[pl.ds(b, 2)].reshape(2 * KVD, SMAX)
            scores.append(jnp.dot(qb, kk, preferred_element_type=F32) * scale)
            for j in range(2):
                fresh.append(jnp.sum(q2[8 * j:8 * j + 8] * krow[pl.ds(b + j, 1), :], axis=-1, keepdims=True) * scale)
        for p in range(SEQS // 2):
            b = i * SEQS + 2 * p
            halves = []
            added = []
            for j in range(2):
                s = jnp.where(lane8 < seq_ref[0, b + j], scores[p][8 * j:8 * j + 8], -1e30)
                s_new = fresh[2 * p + j]
                peak = jnp.maximum(jnp.max(s, axis=-1, keepdims=True), s_new)
                e = jnp.exp(s - peak)
                e_new = jnp.exp(s_new - peak)
                denom = jnp.sum(e, axis=-1, keepdims=True) + e_new
                halves.append(e / denom)
                added.append((e_new / denom).astype(BF16).astype(F32) * vrow[pl.ds(b + j, 1), :])
            prob = jnp.concatenate(halves, axis=0).astype(BF16)
            vv = vbuf[pl.ds(b, 2)].reshape(2 * KVD, SMAX)
            mix = lax.dot_general(prob, vv, (((1,), (1,)), ((), ())), preferred_element_type=F32)
            for j in range(2):
                m = mix[8 * j:8 * j + 8, 128 * j:128 * j + 128] + added[j]
                orow[pl.ds((b + j) * 8, 8), :] = jnp.where((row8 < 4) == (lane_o < HEAD), m, pltpu.roll(m, HEAD, 1))

    def insert(i, carry):
        lane16 = lax.broadcasted_iota(jnp.int16, (KVD, SMAX), 1)
        shift = lax.rem(ROWS - i * SEQS, ROWS)
        for buf, new_ref in ((kbuf, knew), (vbuf, vnew)):
            new = pltpu.roll(new_ref[...], shift, 1)
            for j in range(SEQS):
                b = i * SEQS + j
                column = jnp.broadcast_to(new[:, j:j + 1], (KVD, 128)).astype(BF16)
                here = lane16 == seq_ref[0, b].astype(jnp.int16)
                buf[b] = jnp.where(here, jnp.concatenate([column, column], axis=1), buf[b])
        return carry

    def rows(rc):
        return pl.ds(pl.multiple_of(rc * RC, RC), RC)

    def copy1(rc):
        return remote(send1.at[rc], recv1.at[rc], sems1, 0, rc, sibling)

    def copy1_peer(rc):
        return remote(pair1.at[rc], peer1.at[rc], sems1, 1, rc, peer)

    def copy1_out(rc, half):
        return remote(mid.at[half, rows(rc)], mid.at[half, rows(rc)], sems1, 2, rc, sibling)

    def to_peer1(rc):
        copy1(rc).wait_recv()
        pair1[rc] = (own1[rc] + recv1[rc].astype(F32)).astype(BF16)
        copy1_peer(rc).start()

    def row_chunk(rc, carry):
        def step(i, c):
            attend(rc * (RC // SEQS) + i)
            return c

        lax.fori_loop(0, RC // SEQS, step, 0)
        parts = []
        lane_r = lax.broadcasted_iota(jnp.int32, (RC, 128), 1)
        for slab_idx in range(4):
            lower = orow[pl.ds(rc * RC * 8 + slab_idx * 2, RC, stride=8), :]
            upper = orow[pl.ds(rc * RC * 8 + slab_idx * 2 + 1, RC, stride=8), :]
            parts.append(jnp.where(lane_r < HEAD, lower, upper).astype(BF16))
        attn = jnp.concatenate(parts, axis=1)

        @pl.when(rc == 0)
        def _():
            load_o().wait()
            pl.semaphore_wait(barrier, 2)

        send1[rc] = jnp.dot(attn, wo[:, half_cols(1 - core)], preferred_element_type=F32).astype(BF16)
        copy1(rc).start()
        own1[rc] = jnp.dot(attn, wo[:, half_cols(core)], preferred_element_type=F32)

        @pl.when(rc > 0)
        def _():
            to_peer1(rc - 1)

        @pl.when(rc == NRC - 2)
        def _():
            for j in range(NCH):
                load(0, j).start()
                load(1, j).start()

        return carry

    lax.fori_loop(0, NRC, row_chunk, 0)
    for j in range(NCH):
        load(2, j).start()
    if not last:
        for i in range(3):
            load_next(i).start()
    lax.fori_loop(0, 1, insert, 0)
    to_peer1(NRC - 1)
    lax.fori_loop(1, STEPS, insert, 0)
    for rc in range(NRC):
        copy1_peer(rc).wait_recv()
        total = pair1[rc].astype(F32) + peer1[rc].astype(F32)
        residual = h_ref[rc * RC:(rc + 1) * RC, half_cols(core)]
        mid[core, rc * RC:(rc + 1) * RC] = (residual.astype(F32) + total).astype(BF16)
        copy1_out(rc, core).start()
    for rc in range(NRC):
        copy1_out(rc, 1 - core).wait_recv()

    hidden = jnp.concatenate([mid[0], mid[1]], axis=1)
    normed = norm_rows(hidden.astype(F32), gm[layer:layer + 1, :])
    for j in range(NCH):
        load(0, j).wait()
        load(1, j).wait()
    for j in range(NCH):
        gate = jnp.dot(normed, wg[:, j * CW:(j + 1) * CW], preferred_element_type=F32)
        up = jnp.dot(normed, wu[:, j * CW:(j + 1) * CW], preferred_element_type=F32)
        act[:, j * CW:(j + 1) * CW] = (gate * jax.nn.sigmoid(gate) * up).astype(BF16)
    for j in range(NCH):
        load(2, j).wait()

    def copy2(j):
        return remote(send2.at[j], recv2.at[j], sems2, 0, j, sibling)

    def copy2_peer(j):
        return remote(pair2.at[j], peer2.at[j], sems2, 1, j, peer)

    def copy2_out(j, half):
        return remote(last2.at[half * 2 + j], last2.at[half * 2 + j], sems2, 2, j, sibling)

    def down(j):
        return jnp.dot(act[...], wd[:, pl.ds(pl.multiple_of(j * CW, CW), CW)], preferred_element_type=F32)

    def to_sibling2(j):
        send2[j] = down(2 - core * 2 + j).astype(BF16)
        copy2(j).start()

    def to_peer2(j, own):
        copy2(j).wait_recv()
        pair2[j] = (own + recv2[j].astype(F32)).astype(BF16)
        copy2_peer(j).start()

    to_sibling2(0)
    own = down(core * 2)
    to_sibling2(1)
    to_peer2(0, own)
    to_peer2(1, down(core * 2 + 1))
    for j in range(2):
        copy2_peer(j).wait_recv()
        total = pair2[j].astype(F32) + peer2[j].astype(F32)
        last2[core * 2 + j] = (mid[core, :, j * CW:(j + 1) * CW].astype(F32) + total).astype(BF16)
        copy2_out(j, core).start()
    for j in range(2):
        copy2_out(j, 1 - core).wait_recv()
    for j in range(NCH):
        out_ref[:, j * CW:(j + 1) * CW] = last2[j]
    if not last:
        for i in range(3):
            load_next(i).wait()
    for rc in range(NRC):
        copy1(rc).wait_send()
        copy1_peer(rc).wait_send()
        copy1_out(rc, core).wait_send()
    for j in range(2):
        copy2(j).wait_send()
        copy2_peer(j).wait_send()
        copy2_out(j, core).wait_send()


def layer_call(layer, first, last, seq_lens, freq, hidden, g_attn, g_mlp, qkv, w_next, w_o, w_gate, w_up, w_down, k_cache, v_cache):
    tile = pltpu.VMEM((ROWS, KVD, SMAX), BF16)
    chunk1 = pltpu.VMEM((NRC, RC, HALF), BF16)
    chunk2 = pltpu.VMEM((2, ROWS, CW), BF16)
    weights = [pltpu.VMEM((D, QD), BF16), pltpu.VMEM((D, KVD), BF16), pltpu.VMEM((D, KVD), BF16)]
    space = pltpu.HBM if first else pltpu.VMEM
    near = HBM if first else VMEM
    hidden, *qkv = (pltpu.with_memory_space_constraint(x, space) for x in (hidden, *qkv))
    handed = [] if last or first else list(w_next)
    return pl.pallas_call(
        functools.partial(layer_kernel, layer, first, last),
        out_shape=[pltpu.VMEM((ROWS, D), BF16), tile, tile] + ([] if last else weights),
        in_specs=[HBM] * 3 + [near] + [HBM] * 2 + [near] * 3 + [HBM] * (6 + len(handed)),
        out_specs=[VMEM] * (3 if last else 6),
        scratch_shapes=([pltpu.VMEM((ROWS, D), BF16)] + weights if first else []) + [
            pltpu.SMEM((1, ROWS), jnp.int32),
            pltpu.VMEM((1, ROWS), jnp.int32),
            pltpu.VMEM((1, 128), F32),
            pltpu.VMEM(g_attn.shape, BF16),
            pltpu.VMEM(g_mlp.shape, BF16),
            pltpu.VMEM((QD, D), BF16),
            pltpu.VMEM((D, FF), BF16),
            pltpu.VMEM((D, FF), BF16),
            pltpu.VMEM((FF, D), BF16),
            pltpu.VMEM((KVD, ROWS), F32),
            pltpu.VMEM((KVD, ROWS), F32),
            pltpu.VMEM((ROWS, KVD), F32),
            pltpu.VMEM((ROWS, KVD), F32),
            pltpu.VMEM((ROWS * 8, 128), F32),
            pltpu.VMEM((ROWS * 8, 128), F32),
            pltpu.VMEM((NRC, RC, HALF), F32),
            chunk1, chunk1, chunk1, chunk1,
            pltpu.VMEM((2, ROWS, HALF), BF16),
            chunk2, chunk2, chunk2, chunk2,
            pltpu.VMEM((NCH, ROWS, CW), BF16),
            pltpu.VMEM((ROWS, FF), BF16),
            pltpu.SemaphoreType.DMA((9,)),
            pltpu.SemaphoreType.DMA((STEPS,)),
            pltpu.SemaphoreType.DMA((STEPS,)),
            pltpu.SemaphoreType.DMA((1,)),
            pltpu.SemaphoreType.DMA((3, NCH)),
            pltpu.SemaphoreType.DMA((3,)),
            pltpu.SemaphoreType.DMA((6, NRC)),
            pltpu.SemaphoreType.DMA((6, 2)),
        ],
        compiler_params=pltpu.CompilerParams(vmem_limit_bytes=(38 if first else 35) * 2 ** 20, collective_id=layer, has_side_effects=True),
        name=f"layer{layer}",
    )(seq_lens, seq_lens, freq, hidden, g_attn, g_mlp, *qkv, w_o, w_gate, w_up, w_down, k_cache, v_cache, *handed)


def write_kernel(layer, n_in, *refs):
    sources, results, sem = refs[:n_in], refs[-1 - n_in:-1], refs[-1]
    copies = []
    for n in range(2):
        for i in range(STEPS):
            part = pl.ds(i * SEQS, SEQS)
            copies.append(pltpu.make_async_copy(sources[n].at[part], results[n].at[layer, part], sem.at[n, i]))
    if n_in > 2:
        copies.append(pltpu.make_async_copy(sources[2], results[2], sem.at[2, 0]))
    for copy in copies:
        copy.start()
    for copy in copies:
        copy.wait()


def write_call(layer, layers, tiles, outs):
    cache = jax.ShapeDtypeStruct((layers, ROWS, KVD, SMAX), BF16)
    n_in = len(tiles)
    tiles = [pltpu.with_memory_space_constraint(x, pltpu.VMEM) for x in tiles]
    return pl.pallas_call(
        functools.partial(write_kernel, layer, n_in),
        out_shape=(cache, cache, jax.ShapeDtypeStruct((ROWS, D), BF16))[:n_in],
        in_specs=[VMEM] * n_in + [HBM] * len(outs),
        out_specs=(HBM,) * n_in,
        scratch_shapes=[pltpu.SemaphoreType.DMA((3, STEPS))],
        input_output_aliases={n_in: 0, n_in + 1: 1} if outs else {},
        compiler_params=pltpu.CompilerParams(vmem_limit_bytes=2 ** 20),
        name=f"write{layer}",
    )(*tiles, *outs)


def solution(mesh):
    cache_spec = P(None, "dp", None, "tp", None)
    col_spec = P(None, None, "tp")
    row_spec = P(None, "tp", None)
    in_specs = (P("dp", None), P("dp"), cache_spec, cache_spec, P(None, None), col_spec, col_spec, col_spec,
                row_spec, P(None, None), col_spec, col_spec, row_spec)
    out_specs = (P("dp", None), cache_spec, cache_spec)

    def local_step(hidden, seq_lens, k_cache, v_cache, g_attn, w_q, w_k, w_v, w_o, g_mlp, w_gate, w_up, w_down):
        layers = k_cache.shape[0]
        kt = k_cache.transpose(0, 1, 3, 4, 2).reshape(layers, ROWS, KVD, SMAX)
        vt = v_cache.transpose(0, 1, 3, 4, 2).reshape(layers, ROWS, KVD, SMAX)
        freq = jnp.asarray(np.tile(rope_freqs(HEAD), 4)[None, :])
        seq_row = seq_lens.reshape(1, ROWS)
        hidden, g_attn, w_q, w_k, w_v, w_o, g_mlp, w_gate, w_up, w_down, kt, vt, freq, seq_row = (
            pltpu.with_memory_space_constraint(x, pltpu.HBM)
            for x in (hidden, g_attn, w_q, w_k, w_v, w_o, g_mlp, w_gate, w_up, w_down, kt, vt, freq, seq_row))
        outs = ()
        qkv = (w_q, w_k, w_v)
        for layer in range(layers):
            hidden, k_tile, v_tile, *qkv = layer_call(layer, layer == 0, layer == layers - 1, seq_row, freq, hidden, g_attn, g_mlp, qkv,
                                                      (w_q, w_k, w_v), w_o, w_gate, w_up, w_down, kt, vt)
            if layer < layers - 1:
                outs = write_call(layer, layers, (k_tile, v_tile), outs)
                hidden, outs = lax.optimization_barrier((hidden, outs))
            else:
                *outs, hidden = write_call(layer, layers, (k_tile, v_tile, hidden), outs)

        def back(cache):
            return cache.reshape(layers, ROWS, 2, HEAD, SMAX).transpose(0, 1, 4, 2, 3)

        return hidden, back(outs[0]), back(outs[1])

    return jax.shard_map(local_step, mesh=mesh, in_specs=in_specs, out_specs=out_specs, check_vma=False)
```

```python
import functools

import jax
import jax.numpy as jnp
import numpy as np
from jax import lax
from jax.experimental import pallas as pl
from jax.experimental.pallas import tpu as pltpu
from jax.sharding import PartitionSpec as P

NORM_EPS = 1e-5
ROPE_THETA = 500000.0
ROPE_FACTOR = 8.0
LOW_FACTOR = 1.0
HIGH_FACTOR = 4.0
ORIG_CONTEXT = 8192.0

ROWS = 128
D = 2048
SMAX = 256
HEAD = 64
KVD = 128
QD = 512
FF = 2048
SEQS = 16
STEPS = ROWS // SEQS
CW = 512
NCH = D // CW
HALF = D // 2
RC = 32
NRC = ROWS // RC
AHEAD = 3
F32 = jnp.float32
BF16 = jnp.bfloat16
MESH = pl.DeviceIdType.MESH
VMEM = pl.BlockSpec(memory_space=pltpu.VMEM)
HBM = pl.BlockSpec(memory_space=pltpu.HBM)


def rope_freqs(head_dim):
    freq_expo = np.arange(0, head_dim, 2).astype(np.float32) / np.float32(head_dim)
    inv_freq = 1.0 / (ROPE_THETA ** freq_expo.astype(np.float64))
    wavelen = 2.0 * np.pi / inv_freq
    smooth = (ORIG_CONTEXT / wavelen - LOW_FACTOR) / (HIGH_FACTOR - LOW_FACTOR)
    blended = (1.0 - smooth) * inv_freq / ROPE_FACTOR + smooth * inv_freq
    return np.where(wavelen > ORIG_CONTEXT / LOW_FACTOR, inv_freq / ROPE_FACTOR,
                    np.where(wavelen < ORIG_CONTEXT / HIGH_FACTOR, inv_freq, blended)).astype(np.float32)


def norm_rows(hidden_f, gain):
    inv_rms = lax.rsqrt(jnp.mean(hidden_f * hidden_f, axis=-1, keepdims=True) + NORM_EPS)
    return (hidden_f * inv_rms * gain.astype(F32)).astype(BF16)


def rope_slab(slab, cos, sin):
    lane = lax.broadcasted_iota(jnp.int32, slab.shape, 1)
    other = jnp.where(lane % HEAD < HEAD // 2, pltpu.roll(slab, 128 - HEAD // 2, 1), pltpu.roll(slab, HEAD // 2, 1))
    return slab * cos + other * sin


def layer_kernel(layer, first, last, *refs):
    (seq_hbm, seqv_hbm, freq_hbm, h_in, ga_hbm, gm_hbm, wq_in, wk_in, wv_in, wo_hbm, wg_hbm, wu_hbm, wd_hbm, k_hbm, v_hbm) = refs[:15]
    refs = refs[15:]
    if not first:
        h_ref, wq, wk, wv = h_in, wq_in, wk_in, wv_in
    if not last:
        nq_hbm, nk_hbm, nv_hbm = (wq_in, wk_in, wv_in) if first else refs[:3]
        refs = refs if first else refs[3:]
    out_ref, kbuf, vbuf = refs[:3]
    refs = refs[3:]
    if not last:
        next_q, next_k, next_v = refs[:3]
        refs = refs[3:]
    if first:
        h_ref, wq, wk, wv = refs[:4]
        refs = refs[4:]
    (seq_ref, seqv, freq, ga, gm, wo, wg, wu, wd,
     knew, vnew, krow, vrow, qrow, orow, own1, send1, recv1, pair1, peer1, mid, send2, recv2, pair2, peer2, last2, act,
     sem, ksem, vsem, osem, wsem, nsem, sems1, sems2) = refs
    me = lax.axis_index("tp")
    core = lax.rem(me, 2)
    sibling = me + 1 - 2 * core
    peer = lax.rem(me + 2, 4)

    barrier = pltpu.get_barrier_semaphore()
    for other in (sibling, peer):
        pl.semaphore_signal(barrier, inc=1, device_id={"tp": other}, device_id_type=MESH)

    smalls = {0: (seqv_hbm, seqv), 1: (freq_hbm, freq), 3: (ga_hbm, ga), 7: (seq_hbm, seq_ref), 8: (gm_hbm, gm)}
    if first:
        smalls.update({2: (h_in, h_ref), 4: (wk_in.at[layer], wk), 5: (wv_in.at[layer], wv), 6: (wq_in.at[layer], wq)})

    class Small:
        def __init__(self, i):
            self.copy = pltpu.make_async_copy(*smalls[i], sem.at[i]) if i in smalls else None

        def start(self):
            if self.copy is not None:
                self.copy.start()

        def wait(self):
            if self.copy is not None:
                self.copy.wait()

    small = Small

    def load_next(i):
        src, dst = ((nq_hbm, next_q), (nk_hbm, next_k), (nv_hbm, next_v))[i]
        return pltpu.make_async_copy(src.at[layer + 1], dst, nsem.at[i])

    def load_k(i):
        return pltpu.make_async_copy(k_hbm.at[layer, pl.ds(i * SEQS, SEQS)], kbuf.at[pl.ds(i * SEQS, SEQS)], ksem.at[i])

    def load_v(i):
        return pltpu.make_async_copy(v_hbm.at[layer, pl.ds(i * SEQS, SEQS)], vbuf.at[pl.ds(i * SEQS, SEQS)], vsem.at[i])

    def load_o():
        return pltpu.make_async_copy(wo_hbm.at[layer], wo, osem.at[0])

    def load(kind, j):
        part = pl.ds(j * CW, CW)
        return pltpu.make_async_copy((wg_hbm, wu_hbm, wd_hbm)[kind].at[layer, part], (wg, wu, wd)[kind].at[part], wsem.at[kind, j])

    def half_cols(half):
        return pl.ds(pl.multiple_of(half * HALF, HALF), HALF)

    def remote(src, dst, sems, i, j, to):
        return pltpu.make_async_remote_copy(src_ref=src, dst_ref=dst, send_sem=sems.at[2 * i, j], recv_sem=sems.at[2 * i + 1, j],
                                            device_id={"tp": to}, device_id_type=MESH)

    for i in range(9):
        small(i).start()
    load_k(0).start()
    load_v(0).start()
    small(0).wait()
    small(1).wait()
    angle = jnp.broadcast_to(seqv[...].astype(F32), (ROWS, 128)).T * freq[...]
    cos = jnp.cos(angle)
    sin = jnp.sin(angle)
    lane = lax.broadcasted_iota(jnp.int32, (ROWS, 128), 1)
    sin = jnp.where(lane % HEAD < HEAD // 2, -sin, sin)
    small(2).wait()
    small(3).wait()
    normed = norm_rows(h_ref[...].astype(F32), ga[layer:layer + 1, :])
    small(4).wait()
    small(5).wait()
    for i in range(1, AHEAD):
        load_k(i).start()
        load_v(i).start()
    k_row = rope_slab(jnp.dot(normed, wk[...], preferred_element_type=F32), cos, sin).astype(BF16).astype(F32)
    v_row = jnp.dot(normed, wv[...], preferred_element_type=F32).astype(BF16).astype(F32)
    krow[...] = k_row
    vrow[...] = v_row
    knew[...] = k_row.T
    vnew[...] = v_row.T
    small(6).wait()
    for slab_idx in range(4):
        slab = jnp.dot(normed, wq[:, slab_idx * 128:(slab_idx + 1) * 128], preferred_element_type=F32)
        slab = rope_slab(slab, cos, sin).astype(BF16).astype(F32)
        turned = pltpu.roll(slab, HEAD, 1)
        for half in range(2):
            hg = slab_idx * 2 + half
            kv = hg // 4
            qrow[pl.ds(hg, ROWS, stride=8), :] = jnp.where(lane // HEAD == kv, slab if kv == half else turned, 0.0)
    small(7).wait()
    small(8).wait()

    def attend(i):
        load_k(i).wait()
        load_v(i).wait()

        @pl.when(i + AHEAD < STEPS)
        def _():
            load_k(i + AHEAD).start()
            load_v(i + AHEAD).start()

        @pl.when(i == 0)
        def _():
            load_o().start()

        lane8 = lax.broadcasted_iota(jnp.int32, (8, SMAX), 1)
        row16 = lax.broadcasted_iota(jnp.int32, (16, 128), 0)
        row8 = lax.broadcasted_iota(jnp.int32, (8, 128), 0)
        lane_o = lax.broadcasted_iota(jnp.int32, (8, 128), 1)
        scale = HEAD ** -0.5
        scores = []
        fresh = []
        for p in range(SEQS // 2):
            b = i * SEQS + 2 * p
            q2 = qrow[pl.ds(b * 8, 16), :]
            qb = jnp.concatenate([jnp.where(row16 < 8, q2, 0.0), jnp.where(row16 >= 8, q2, 0.0)], axis=1).astype(BF16)
            kk = kbuf[pl.ds(b, 2)].reshape(2 * KVD, SMAX)
            scores.append(jnp.dot(qb, kk, preferred_element_type=F32) * scale)
            for j in range(2):
                fresh.append(jnp.sum(q2[8 * j:8 * j + 8] * krow[pl.ds(b + j, 1), :], axis=-1, keepdims=True) * scale)
        for p in range(SEQS // 2):
            b = i * SEQS + 2 * p
            halves = []
            added = []
            for j in range(2):
                s = jnp.where(lane8 < seq_ref[0, b + j], scores[p][8 * j:8 * j + 8], -1e30)
                s_new = fresh[2 * p + j]
                peak = jnp.maximum(jnp.max(s, axis=-1, keepdims=True), s_new)
                e = jnp.exp(s - peak)
                e_new = jnp.exp(s_new - peak)
                denom = jnp.sum(e, axis=-1, keepdims=True) + e_new
                halves.append(e / denom)
                added.append((e_new / denom).astype(BF16).astype(F32) * vrow[pl.ds(b + j, 1), :])
            prob = jnp.concatenate(halves, axis=0).astype(BF16)
            vv = vbuf[pl.ds(b, 2)].reshape(2 * KVD, SMAX)
            mix = lax.dot_general(prob, vv, (((1,), (1,)), ((), ())), preferred_element_type=F32)
            for j in range(2):
                m = mix[8 * j:8 * j + 8, 128 * j:128 * j + 128] + added[j]
                orow[pl.ds((b + j) * 8, 8), :] = jnp.where((row8 < 4) == (lane_o < HEAD), m, pltpu.roll(m, HEAD, 1))

    def insert(i, carry):
        lane16 = lax.broadcasted_iota(jnp.int16, (KVD, SMAX), 1)
        shift = lax.rem(ROWS - i * SEQS, ROWS)
        for buf, new_ref in ((kbuf, knew), (vbuf, vnew)):
            new = pltpu.roll(new_ref[...], shift, 1)
            for j in range(SEQS):
                b = i * SEQS + j
                column = jnp.broadcast_to(new[:, j:j + 1], (KVD, 128)).astype(BF16)
                here = lane16 == seq_ref[0, b].astype(jnp.int16)
                buf[b] = jnp.where(here, jnp.concatenate([column, column], axis=1), buf[b])
        return carry

    def rows(rc):
        return pl.ds(pl.multiple_of(rc * RC, RC), RC)

    def copy1(rc):
        return remote(send1.at[rc], recv1.at[rc], sems1, 0, rc, sibling)

    def copy1_peer(rc):
        return remote(pair1.at[rc], peer1.at[rc], sems1, 1, rc, peer)

    def copy1_out(rc, half):
        return remote(mid.at[half, rows(rc)], mid.at[half, rows(rc)], sems1, 2, rc, sibling)

    def to_peer1(rc):
        copy1(rc).wait_recv()
        pair1[rc] = (own1[rc] + recv1[rc].astype(F32)).astype(BF16)
        copy1_peer(rc).start()

    def row_chunk(rc, carry):
        def step(i, c):
            @pl.when((i == RC // SEQS - 1) & (rc == 0))
            def _():
                pl.semaphore_wait(barrier, 2)

            attend(rc * (RC // SEQS) + i)

            @pl.when((i == 0) & (rc > 0))
            def _():
                to_peer1(rc - 1)

            return c

        lax.fori_loop(0, RC // SEQS, step, 0)
        parts = []
        lane_r = lax.broadcasted_iota(jnp.int32, (RC, 128), 1)
        for slab_idx in range(4):
            lower = orow[pl.ds(rc * RC * 8 + slab_idx * 2, RC, stride=8), :]
            upper = orow[pl.ds(rc * RC * 8 + slab_idx * 2 + 1, RC, stride=8), :]
            parts.append(jnp.where(lane_r < HEAD, lower, upper).astype(BF16))
        attn = jnp.concatenate(parts, axis=1)

        @pl.when(rc == 0)
        def _():
            load_o().wait()

        send1[rc] = jnp.dot(attn, wo[:, half_cols(1 - core)], preferred_element_type=F32).astype(BF16)
        copy1(rc).start()
        own1[rc] = jnp.dot(attn, wo[:, half_cols(core)], preferred_element_type=F32)

        @pl.when(rc == NRC - 2)
        def _():
            for j in range(NCH):
                load(0, j).start()
                load(1, j).start()

        return carry

    lax.fori_loop(0, NRC, row_chunk, 0)
    for j in range(NCH):
        load(2, j).start()
    if not last:
        for i in range(3):
            load_next(i).start()
    to_peer1(NRC - 1)
    for rc in range(NRC):
        copy1_peer(rc).wait_recv()
        total = pair1[rc].astype(F32) + peer1[rc].astype(F32)
        residual = h_ref[rc * RC:(rc + 1) * RC, half_cols(core)]
        mid[core, rc * RC:(rc + 1) * RC] = (residual.astype(F32) + total).astype(BF16)
        copy1_out(rc, core).start()
    for rc in range(NRC):
        copy1_out(rc, 1 - core).wait_recv()

    hidden = jnp.concatenate([mid[0], mid[1]], axis=1)
    normed = norm_rows(hidden.astype(F32), gm[layer:layer + 1, :])
    for j in range(NCH):
        load(0, j).wait()
        load(1, j).wait()
    for j in range(NCH):
        gate = jnp.dot(normed, wg[:, j * CW:(j + 1) * CW], preferred_element_type=F32)
        up = jnp.dot(normed, wu[:, j * CW:(j + 1) * CW], preferred_element_type=F32)
        act[:, j * CW:(j + 1) * CW] = (gate * jax.nn.sigmoid(gate) * up).astype(BF16)
    for j in range(NCH):
        load(2, j).wait()

    def copy2(j):
        return remote(send2.at[j], recv2.at[j], sems2, 0, j, sibling)

    def copy2_peer(j):
        return remote(pair2.at[j], peer2.at[j], sems2, 1, j, peer)

    def copy2_out(j, half):
        return remote(last2.at[half * 2 + j], last2.at[half * 2 + j], sems2, 2, j, sibling)

    def down(j):
        return jnp.dot(act[...], wd[:, pl.ds(pl.multiple_of(j * CW, CW), CW)], preferred_element_type=F32)

    def to_sibling2(j):
        send2[j] = down(2 - core * 2 + j).astype(BF16)
        copy2(j).start()

    def to_peer2(j, own):
        copy2(j).wait_recv()
        pair2[j] = (own + recv2[j].astype(F32)).astype(BF16)
        copy2_peer(j).start()

    to_sibling2(0)
    own = down(core * 2)
    to_sibling2(1)
    to_peer2(0, own)
    to_peer2(1, down(core * 2 + 1))
    lax.fori_loop(0, STEPS, insert, 0)
    for j in range(2):
        copy2_peer(j).wait_recv()
        total = pair2[j].astype(F32) + peer2[j].astype(F32)
        last2[core * 2 + j] = (mid[core, :, j * CW:(j + 1) * CW].astype(F32) + total).astype(BF16)
        copy2_out(j, core).start()
    for j in range(2):
        copy2_out(j, 1 - core).wait_recv()
    for j in range(NCH):
        out_ref[:, j * CW:(j + 1) * CW] = last2[j]
    if not last:
        for i in range(3):
            load_next(i).wait()
    for rc in range(NRC):
        copy1(rc).wait_send()
        copy1_peer(rc).wait_send()
        copy1_out(rc, core).wait_send()
    for j in range(2):
        copy2(j).wait_send()
        copy2_peer(j).wait_send()
        copy2_out(j, core).wait_send()


def layer_call(layer, first, last, seq_lens, freq, hidden, g_attn, g_mlp, qkv, w_next, w_o, w_gate, w_up, w_down, k_cache, v_cache):
    tile = pltpu.VMEM((ROWS, KVD, SMAX), BF16)
    chunk1 = pltpu.VMEM((NRC, RC, HALF), BF16)
    chunk2 = pltpu.VMEM((2, ROWS, CW), BF16)
    weights = [pltpu.VMEM((D, QD), BF16), pltpu.VMEM((D, KVD), BF16), pltpu.VMEM((D, KVD), BF16)]
    space = pltpu.HBM if first else pltpu.VMEM
    near = HBM if first else VMEM
    hidden, *qkv = (pltpu.with_memory_space_constraint(x, space) for x in (hidden, *qkv))
    handed = [] if last or first else list(w_next)
    return pl.pallas_call(
        functools.partial(layer_kernel, layer, first, last),
        out_shape=[pltpu.VMEM((ROWS, D), BF16), tile, tile] + ([] if last else weights),
        in_specs=[HBM] * 3 + [near] + [HBM] * 2 + [near] * 3 + [HBM] * (6 + len(handed)),
        out_specs=[VMEM] * (3 if last else 6),
        scratch_shapes=([pltpu.VMEM((ROWS, D), BF16)] + weights if first else []) + [
            pltpu.SMEM((1, ROWS), jnp.int32),
            pltpu.VMEM((1, ROWS), jnp.int32),
            pltpu.VMEM((1, 128), F32),
            pltpu.VMEM(g_attn.shape, BF16),
            pltpu.VMEM(g_mlp.shape, BF16),
            pltpu.VMEM((QD, D), BF16),
            pltpu.VMEM((D, FF), BF16),
            pltpu.VMEM((D, FF), BF16),
            pltpu.VMEM((FF, D), BF16),
            pltpu.VMEM((KVD, ROWS), F32),
            pltpu.VMEM((KVD, ROWS), F32),
            pltpu.VMEM((ROWS, KVD), F32),
            pltpu.VMEM((ROWS, KVD), F32),
            pltpu.VMEM((ROWS * 8, 128), F32),
            pltpu.VMEM((ROWS * 8, 128), F32),
            pltpu.VMEM((NRC, RC, HALF), F32),
            chunk1, chunk1, chunk1, chunk1,
            pltpu.VMEM((2, ROWS, HALF), BF16),
            chunk2, chunk2, chunk2, chunk2,
            pltpu.VMEM((NCH, ROWS, CW), BF16),
            pltpu.VMEM((ROWS, FF), BF16),
            pltpu.SemaphoreType.DMA((9,)),
            pltpu.SemaphoreType.DMA((STEPS,)),
            pltpu.SemaphoreType.DMA((STEPS,)),
            pltpu.SemaphoreType.DMA((1,)),
            pltpu.SemaphoreType.DMA((3, NCH)),
            pltpu.SemaphoreType.DMA((3,)),
            pltpu.SemaphoreType.DMA((6, NRC)),
            pltpu.SemaphoreType.DMA((6, 2)),
        ],
        compiler_params=pltpu.CompilerParams(vmem_limit_bytes=(38 if first else 35) * 2 ** 20, collective_id=layer, has_side_effects=True),
        name=f"layer{layer}",
    )(seq_lens, seq_lens, freq, hidden, g_attn, g_mlp, *qkv, w_o, w_gate, w_up, w_down, k_cache, v_cache, *handed)


def write_kernel(layer, n_in, *refs):
    sources, results, sem = refs[:n_in], refs[-1 - n_in:-1], refs[-1]
    copies = []
    for n in range(2):
        for i in range(STEPS):
            part = pl.ds(i * SEQS, SEQS)
            copies.append(pltpu.make_async_copy(sources[n].at[part], results[n].at[layer, part], sem.at[n, i]))
    if n_in > 2:
        copies.append(pltpu.make_async_copy(sources[2], results[2], sem.at[2, 0]))
    for copy in copies:
        copy.start()
    for copy in copies:
        copy.wait()


def write_call(layer, layers, tiles, outs):
    cache = jax.ShapeDtypeStruct((layers, ROWS, KVD, SMAX), BF16)
    n_in = len(tiles)
    tiles = [pltpu.with_memory_space_constraint(x, pltpu.VMEM) for x in tiles]
    return pl.pallas_call(
        functools.partial(write_kernel, layer, n_in),
        out_shape=(cache, cache, jax.ShapeDtypeStruct((ROWS, D), BF16))[:n_in],
        in_specs=[VMEM] * n_in + [HBM] * len(outs),
        out_specs=(HBM,) * n_in,
        scratch_shapes=[pltpu.SemaphoreType.DMA((3, STEPS))],
        input_output_aliases={n_in: 0, n_in + 1: 1} if outs else {},
        compiler_params=pltpu.CompilerParams(vmem_limit_bytes=2 ** 20),
        name=f"write{layer}",
    )(*tiles, *outs)


def solution(mesh):
    cache_spec = P(None, "dp", None, "tp", None)
    col_spec = P(None, None, "tp")
    row_spec = P(None, "tp", None)
    in_specs = (P("dp", None), P("dp"), cache_spec, cache_spec, P(None, None), col_spec, col_spec, col_spec,
                row_spec, P(None, None), col_spec, col_spec, row_spec)
    out_specs = (P("dp", None), cache_spec, cache_spec)

    def local_step(hidden, seq_lens, k_cache, v_cache, g_attn, w_q, w_k, w_v, w_o, g_mlp, w_gate, w_up, w_down):
        layers = k_cache.shape[0]
        kt = k_cache.transpose(0, 1, 3, 4, 2).reshape(layers, ROWS, KVD, SMAX)
        vt = v_cache.transpose(0, 1, 3, 4, 2).reshape(layers, ROWS, KVD, SMAX)
        freq = jnp.asarray(np.tile(rope_freqs(HEAD), 4)[None, :])
        seq_row = seq_lens.reshape(1, ROWS)
        hidden, g_attn, w_q, w_k, w_v, w_o, g_mlp, w_gate, w_up, w_down, kt, vt, freq, seq_row = (
            pltpu.with_memory_space_constraint(x, pltpu.HBM)
            for x in (hidden, g_attn, w_q, w_k, w_v, w_o, g_mlp, w_gate, w_up, w_down, kt, vt, freq, seq_row))
        outs = ()
        qkv = (w_q, w_k, w_v)
        for layer in range(layers):
            hidden, k_tile, v_tile, *qkv = layer_call(layer, layer == 0, layer == layers - 1, seq_row, freq, hidden, g_attn, g_mlp, qkv,
                                                      (w_q, w_k, w_v), w_o, w_gate, w_up, w_down, kt, vt)
            if layer < layers - 1:
                outs = write_call(layer, layers, (k_tile, v_tile), outs)
                hidden, outs = lax.optimization_barrier((hidden, outs))
            else:
                *outs, hidden = write_call(layer, layers, (k_tile, v_tile, hidden), outs)

        def back(cache):
            return cache.reshape(layers, ROWS, 2, HEAD, SMAX).transpose(0, 1, 4, 2, 3)

        return hidden, back(outs[0]), back(outs[1])

    return jax.shard_map(local_step, mesh=mesh, in_specs=in_specs, out_specs=out_specs, check_vma=False)
```

```python
import functools

import jax
import jax.numpy as jnp
import numpy as np
from jax import lax
from jax.experimental import pallas as pl
from jax.experimental.pallas import tpu as pltpu
from jax.sharding import PartitionSpec as P

NORM_EPS = 1e-5
ROPE_THETA = 500000.0
ROPE_FACTOR = 8.0
LOW_FACTOR = 1.0
HIGH_FACTOR = 4.0
ORIG_CONTEXT = 8192.0

ROWS = 128
D = 2048
SMAX = 256
HEAD = 64
KVD = 128
QD = 512
FF = 2048
SEQS = 16
STEPS = ROWS // SEQS
CW = 512
NCH = D // CW
HALF = D // 2
RC = 32
NRC = ROWS // RC
AHEAD = 4
F32 = jnp.float32
BF16 = jnp.bfloat16
MESH = pl.DeviceIdType.MESH
VMEM = pl.BlockSpec(memory_space=pltpu.VMEM)
HBM = pl.BlockSpec(memory_space=pltpu.HBM)


def rope_freqs(head_dim):
    freq_expo = np.arange(0, head_dim, 2).astype(np.float32) / np.float32(head_dim)
    inv_freq = 1.0 / (ROPE_THETA ** freq_expo.astype(np.float64))
    wavelen = 2.0 * np.pi / inv_freq
    smooth = (ORIG_CONTEXT / wavelen - LOW_FACTOR) / (HIGH_FACTOR - LOW_FACTOR)
    blended = (1.0 - smooth) * inv_freq / ROPE_FACTOR + smooth * inv_freq
    return np.where(wavelen > ORIG_CONTEXT / LOW_FACTOR, inv_freq / ROPE_FACTOR,
                    np.where(wavelen < ORIG_CONTEXT / HIGH_FACTOR, inv_freq, blended)).astype(np.float32)


def norm_rows(hidden_f, gain):
    inv_rms = lax.rsqrt(jnp.mean(hidden_f * hidden_f, axis=-1, keepdims=True) + NORM_EPS)
    return (hidden_f * inv_rms * gain.astype(F32)).astype(BF16)


def rope_slab(slab, cos, sin):
    lane = lax.broadcasted_iota(jnp.int32, slab.shape, 1)
    other = jnp.where(lane % HEAD < HEAD // 2, pltpu.roll(slab, 128 - HEAD // 2, 1), pltpu.roll(slab, HEAD // 2, 1))
    return slab * cos + other * sin


def layer_kernel(layer, first, last, *refs):
    (seq_hbm, seqv_hbm, freq_hbm, h_in, ga_hbm, gm_hbm, wq_in, wk_in, wv_in, wo_hbm, wg_hbm, wu_hbm, wd_hbm, k_hbm, v_hbm) = refs[:15]
    refs = refs[15:]
    if not first:
        h_ref, wq, wk, wv = h_in, wq_in, wk_in, wv_in
    if not last:
        nq_hbm, nk_hbm, nv_hbm = (wq_in, wk_in, wv_in) if first else refs[:3]
        refs = refs if first else refs[3:]
    out_ref, kbuf, vbuf = refs[:3]
    refs = refs[3:]
    if not last:
        next_q, next_k, next_v = refs[:3]
        refs = refs[3:]
    if first:
        h_ref, wq, wk, wv = refs[:4]
        refs = refs[4:]
    (seq_ref, seqv, freq, ga, gm, wo, wg, wu, wd,
     knew, vnew, krow, vrow, qrow, orow, own1, send1, recv1, pair1, peer1, mid, send2, recv2, pair2, peer2, last2, act,
     sem, ksem, vsem, osem, wsem, nsem, sems1, sems2) = refs
    me = lax.axis_index("tp")
    core = lax.rem(me, 2)
    sibling = me + 1 - 2 * core
    peer = lax.rem(me + 2, 4)

    barrier = pltpu.get_barrier_semaphore()
    for other in (sibling, peer):
        pl.semaphore_signal(barrier, inc=1, device_id={"tp": other}, device_id_type=MESH)

    smalls = {0: (seqv_hbm, seqv), 1: (freq_hbm, freq), 3: (ga_hbm, ga), 7: (seq_hbm, seq_ref), 8: (gm_hbm, gm)}
    if first:
        smalls.update({2: (h_in, h_ref), 4: (wk_in.at[layer], wk), 5: (wv_in.at[layer], wv), 6: (wq_in.at[layer], wq)})

    class Small:
        def __init__(self, i):
            self.copy = pltpu.make_async_copy(*smalls[i], sem.at[i]) if i in smalls else None

        def start(self):
            if self.copy is not None:
                self.copy.start()

        def wait(self):
            if self.copy is not None:
                self.copy.wait()

    small = Small

    def load_next(i):
        src, dst = ((nq_hbm, next_q), (nk_hbm, next_k), (nv_hbm, next_v))[i]
        return pltpu.make_async_copy(src.at[layer + 1], dst, nsem.at[i])

    def load_k(i):
        return pltpu.make_async_copy(k_hbm.at[layer, pl.ds(i * SEQS, SEQS)], kbuf.at[pl.ds(i * SEQS, SEQS)], ksem.at[i])

    def load_v(i):
        return pltpu.make_async_copy(v_hbm.at[layer, pl.ds(i * SEQS, SEQS)], vbuf.at[pl.ds(i * SEQS, SEQS)], vsem.at[i])

    def load_o():
        return pltpu.make_async_copy(wo_hbm.at[layer], wo, osem.at[0])

    def load(kind, j):
        part = pl.ds(j * CW, CW)
        return pltpu.make_async_copy((wg_hbm, wu_hbm, wd_hbm)[kind].at[layer, part], (wg, wu, wd)[kind].at[part], wsem.at[kind, j])

    def half_cols(half):
        return pl.ds(pl.multiple_of(half * HALF, HALF), HALF)

    def remote(src, dst, sems, i, j, to):
        return pltpu.make_async_remote_copy(src_ref=src, dst_ref=dst, send_sem=sems.at[2 * i, j], recv_sem=sems.at[2 * i + 1, j],
                                            device_id={"tp": to}, device_id_type=MESH)

    for i in range(9):
        small(i).start()
    load_k(0).start()
    load_v(0).start()
    small(0).wait()
    small(1).wait()
    angle = jnp.broadcast_to(seqv[...].astype(F32), (ROWS, 128)).T * freq[...]
    cos = jnp.cos(angle)
    sin = jnp.sin(angle)
    lane = lax.broadcasted_iota(jnp.int32, (ROWS, 128), 1)
    sin = jnp.where(lane % HEAD < HEAD // 2, -sin, sin)
    small(2).wait()
    small(3).wait()
    normed = norm_rows(h_ref[...].astype(F32), ga[layer:layer + 1, :])
    small(4).wait()
    small(5).wait()
    for i in range(1, AHEAD):
        load_k(i).start()
        load_v(i).start()
    k_row = rope_slab(jnp.dot(normed, wk[...], preferred_element_type=F32), cos, sin).astype(BF16).astype(F32)
    v_row = jnp.dot(normed, wv[...], preferred_element_type=F32).astype(BF16).astype(F32)
    krow[...] = k_row
    vrow[...] = v_row
    knew[...] = k_row.T
    vnew[...] = v_row.T
    small(6).wait()
    for slab_idx in range(4):
        slab = jnp.dot(normed, wq[:, slab_idx * 128:(slab_idx + 1) * 128], preferred_element_type=F32)
        slab = rope_slab(slab, cos, sin).astype(BF16).astype(F32)
        turned = pltpu.roll(slab, HEAD, 1)
        for half in range(2):
            hg = slab_idx * 2 + half
            kv = hg // 4
            qrow[pl.ds(hg, ROWS, stride=8), :] = jnp.where(lane // HEAD == kv, slab if kv == half else turned, 0.0)
    small(7).wait()
    small(8).wait()

    def attend(i):
        load_k(i).wait()
        load_v(i).wait()

        @pl.when(i + AHEAD < STEPS)
        def _():
            load_k(i + AHEAD).start()
            load_v(i + AHEAD).start()

        @pl.when(i == 0)
        def _():
            load_o().start()

        lane8 = lax.broadcasted_iota(jnp.int32, (8, SMAX), 1)
        row16 = lax.broadcasted_iota(jnp.int32, (16, 128), 0)
        row8 = lax.broadcasted_iota(jnp.int32, (8, 128), 0)
        lane_o = lax.broadcasted_iota(jnp.int32, (8, 128), 1)
        scale = HEAD ** -0.5
        scores = []
        fresh = []
        for p in range(SEQS // 2):
            b = i * SEQS + 2 * p
            q2 = qrow[pl.ds(b * 8, 16), :]
            qb = jnp.concatenate([jnp.where(row16 < 8, q2, 0.0), jnp.where(row16 >= 8, q2, 0.0)], axis=1).astype(BF16)
            kk = kbuf[pl.ds(b, 2)].reshape(2 * KVD, SMAX)
            scores.append(jnp.dot(qb, kk, preferred_element_type=F32) * scale)
            for j in range(2):
                fresh.append(jnp.sum(q2[8 * j:8 * j + 8] * krow[pl.ds(b + j, 1), :], axis=-1, keepdims=True) * scale)
        for p in range(SEQS // 2):
            b = i * SEQS + 2 * p
            halves = []
            added = []
            for j in range(2):
                s = jnp.where(lane8 < seq_ref[0, b + j], scores[p][8 * j:8 * j + 8], -1e30)
                s_new = fresh[2 * p + j]
                peak = jnp.maximum(jnp.max(s, axis=-1, keepdims=True), s_new)
                e = jnp.exp(s - peak)
                e_new = jnp.exp(s_new - peak)
                denom = jnp.sum(e, axis=-1, keepdims=True) + e_new
                halves.append(e / denom)
                added.append((e_new / denom).astype(BF16).astype(F32) * vrow[pl.ds(b + j, 1), :])
            prob = jnp.concatenate(halves, axis=0).astype(BF16)
            vv = vbuf[pl.ds(b, 2)].reshape(2 * KVD, SMAX)
            mix = lax.dot_general(prob, vv, (((1,), (1,)), ((), ())), preferred_element_type=F32)
            for j in range(2):
                m = mix[8 * j:8 * j + 8, 128 * j:128 * j + 128] + added[j]
                orow[pl.ds((b + j) * 8, 8), :] = jnp.where((row8 < 4) == (lane_o < HEAD), m, pltpu.roll(m, HEAD, 1))

    def insert(i, carry):
        lane16 = lax.broadcasted_iota(jnp.int16, (KVD, SMAX), 1)
        shift = lax.rem(ROWS - i * SEQS, ROWS)
        for buf, new_ref in ((kbuf, knew), (vbuf, vnew)):
            new = pltpu.roll(new_ref[...], shift, 1)
            for j in range(SEQS):
                b = i * SEQS + j
                column = jnp.broadcast_to(new[:, j:j + 1], (KVD, 128)).astype(BF16)
                here = lane16 == seq_ref[0, b].astype(jnp.int16)
                buf[b] = jnp.where(here, jnp.concatenate([column, column], axis=1), buf[b])
        return carry

    def rows(rc):
        return pl.ds(pl.multiple_of(rc * RC, RC), RC)

    def copy1(rc):
        return remote(send1.at[rc], recv1.at[rc], sems1, 0, rc, sibling)

    def copy1_peer(rc):
        return remote(pair1.at[rc], peer1.at[rc], sems1, 1, rc, peer)

    def copy1_out(rc, half):
        return remote(mid.at[half, rows(rc)], mid.at[half, rows(rc)], sems1, 2, rc, sibling)

    def to_peer1(rc):
        copy1(rc).wait_recv()
        pair1[rc] = (own1[rc] + recv1[rc].astype(F32)).astype(BF16)
        copy1_peer(rc).start()

    def row_chunk(rc, carry):
        def step(i, c):
            @pl.when((i == RC // SEQS - 1) & (rc == 0))
            def _():
                pl.semaphore_wait(barrier, 2)

            attend(rc * (RC // SEQS) + i)
            return c

        lax.fori_loop(0, RC // SEQS, step, 0)
        parts = []
        lane_r = lax.broadcasted_iota(jnp.int32, (RC, 128), 1)
        for slab_idx in range(4):
            lower = orow[pl.ds(rc * RC * 8 + slab_idx * 2, RC, stride=8), :]
            upper = orow[pl.ds(rc * RC * 8 + slab_idx * 2 + 1, RC, stride=8), :]
            parts.append(jnp.where(lane_r < HEAD, lower, upper).astype(BF16))
        attn = jnp.concatenate(parts, axis=1)

        @pl.when(rc == 0)
        def _():
            load_o().wait()

        send1[rc] = jnp.dot(attn, wo[:, half_cols(1 - core)], preferred_element_type=F32).astype(BF16)
        copy1(rc).start()

        @pl.when(rc > 0)
        def _():
            to_peer1(rc - 1)

        own1[rc] = jnp.dot(attn, wo[:, half_cols(core)], preferred_element_type=F32)

        @pl.when(rc == NRC - 2)
        def _():
            for j in range(NCH):
                load(0, j).start()
                load(1, j).start()

        return carry

    lax.fori_loop(0, NRC, row_chunk, 0)
    for j in range(NCH):
        load(2, j).start()
    if not last:
        for i in range(3):
            load_next(i).start()
    to_peer1(NRC - 1)
    for rc in range(NRC):
        copy1_peer(rc).wait_recv()
        total = pair1[rc].astype(F32) + peer1[rc].astype(F32)
        residual = h_ref[rc * RC:(rc + 1) * RC, half_cols(core)]
        mid[core, rc * RC:(rc + 1) * RC] = (residual.astype(F32) + total).astype(BF16)
        copy1_out(rc, core).start()
    for rc in range(NRC):
        copy1_out(rc, 1 - core).wait_recv()

    hidden = jnp.concatenate([mid[0], mid[1]], axis=1)
    normed = norm_rows(hidden.astype(F32), gm[layer:layer + 1, :])
    for j in range(NCH):
        load(0, j).wait()
        load(1, j).wait()
    for j in range(NCH):
        gate = jnp.dot(normed, wg[:, j * CW:(j + 1) * CW], preferred_element_type=F32)
        up = jnp.dot(normed, wu[:, j * CW:(j + 1) * CW], preferred_element_type=F32)
        act[:, j * CW:(j + 1) * CW] = (gate * jax.nn.sigmoid(gate) * up).astype(BF16)
    for j in range(NCH):
        load(2, j).wait()

    def copy2(j):
        return remote(send2.at[j], recv2.at[j], sems2, 0, j, sibling)

    def copy2_peer(j):
        return remote(pair2.at[j], peer2.at[j], sems2, 1, j, peer)

    def copy2_out(j, half):
        return remote(last2.at[half * 2 + j], last2.at[half * 2 + j], sems2, 2, j, sibling)

    def down(j):
        return jnp.dot(act[...], wd[:, pl.ds(pl.multiple_of(j * CW, CW), CW)], preferred_element_type=F32)

    def to_sibling2(j):
        send2[j] = down(2 - core * 2 + j).astype(BF16)
        copy2(j).start()

    def to_peer2(j, own):
        copy2(j).wait_recv()
        pair2[j] = (own + recv2[j].astype(F32)).astype(BF16)
        copy2_peer(j).start()

    to_sibling2(0)
    own = down(core * 2)
    to_sibling2(1)
    to_peer2(0, own)
    to_peer2(1, down(core * 2 + 1))
    lax.fori_loop(0, STEPS, insert, 0)
    for j in range(2):
        copy2_peer(j).wait_recv()
        total = pair2[j].astype(F32) + peer2[j].astype(F32)
        last2[core * 2 + j] = (mid[core, :, j * CW:(j + 1) * CW].astype(F32) + total).astype(BF16)
        copy2_out(j, core).start()
    for j in range(2):
        copy2_out(j, 1 - core).wait_recv()
    for j in range(NCH):
        out_ref[:, j * CW:(j + 1) * CW] = last2[j]
    if not last:
        for i in range(3):
            load_next(i).wait()
    for rc in range(NRC):
        copy1(rc).wait_send()
        copy1_peer(rc).wait_send()
        copy1_out(rc, core).wait_send()
    for j in range(2):
        copy2(j).wait_send()
        copy2_peer(j).wait_send()
        copy2_out(j, core).wait_send()


def layer_call(layer, first, last, seq_lens, freq, hidden, g_attn, g_mlp, qkv, w_next, w_o, w_gate, w_up, w_down, k_cache, v_cache):
    tile = pltpu.VMEM((ROWS, KVD, SMAX), BF16)
    chunk1 = pltpu.VMEM((NRC, RC, HALF), BF16)
    chunk2 = pltpu.VMEM((2, ROWS, CW), BF16)
    weights = [pltpu.VMEM((D, QD), BF16), pltpu.VMEM((D, KVD), BF16), pltpu.VMEM((D, KVD), BF16)]
    space = pltpu.HBM if first else pltpu.VMEM
    near = HBM if first else VMEM
    hidden, *qkv = (pltpu.with_memory_space_constraint(x, space) for x in (hidden, *qkv))
    handed = [] if last or first else list(w_next)
    return pl.pallas_call(
        functools.partial(layer_kernel, layer, first, last),
        out_shape=[pltpu.VMEM((ROWS, D), BF16), tile, tile] + ([] if last else weights),
        in_specs=[HBM] * 3 + [near] + [HBM] * 2 + [near] * 3 + [HBM] * (6 + len(handed)),
        out_specs=[VMEM] * (3 if last else 6),
        scratch_shapes=([pltpu.VMEM((ROWS, D), BF16)] + weights if first else []) + [
            pltpu.SMEM((1, ROWS), jnp.int32),
            pltpu.VMEM((1, ROWS), jnp.int32),
            pltpu.VMEM((1, 128), F32),
            pltpu.VMEM(g_attn.shape, BF16),
            pltpu.VMEM(g_mlp.shape, BF16),
            pltpu.VMEM((QD, D), BF16),
            pltpu.VMEM((D, FF), BF16),
            pltpu.VMEM((D, FF), BF16),
            pltpu.VMEM((FF, D), BF16),
            pltpu.VMEM((KVD, ROWS), F32),
            pltpu.VMEM((KVD, ROWS), F32),
            pltpu.VMEM((ROWS, KVD), F32),
            pltpu.VMEM((ROWS, KVD), F32),
            pltpu.VMEM((ROWS * 8, 128), F32),
            pltpu.VMEM((ROWS * 8, 128), F32),
            pltpu.VMEM((NRC, RC, HALF), F32),
            chunk1, chunk1, chunk1, chunk1,
            pltpu.VMEM((2, ROWS, HALF), BF16),
            chunk2, chunk2, chunk2, chunk2,
            pltpu.VMEM((NCH, ROWS, CW), BF16),
            pltpu.VMEM((ROWS, FF), BF16),
            pltpu.SemaphoreType.DMA((9,)),
            pltpu.SemaphoreType.DMA((STEPS,)),
            pltpu.SemaphoreType.DMA((STEPS,)),
            pltpu.SemaphoreType.DMA((1,)),
            pltpu.SemaphoreType.DMA((3, NCH)),
            pltpu.SemaphoreType.DMA((3,)),
            pltpu.SemaphoreType.DMA((6, NRC)),
            pltpu.SemaphoreType.DMA((6, 2)),
        ],
        compiler_params=pltpu.CompilerParams(vmem_limit_bytes=(38 if first else 35) * 2 ** 20, collective_id=layer, has_side_effects=True),
        name=f"layer{layer}",
    )(seq_lens, seq_lens, freq, hidden, g_attn, g_mlp, *qkv, w_o, w_gate, w_up, w_down, k_cache, v_cache, *handed)


def write_kernel(layer, n_in, *refs):
    sources, results, sem = refs[:n_in], refs[-1 - n_in:-1], refs[-1]
    copies = []
    for n in range(2):
        for i in range(STEPS):
            part = pl.ds(i * SEQS, SEQS)
            copies.append(pltpu.make_async_copy(sources[n].at[part], results[n].at[layer, part], sem.at[n, i]))
    if n_in > 2:
        copies.append(pltpu.make_async_copy(sources[2], results[2], sem.at[2, 0]))
    for copy in copies:
        copy.start()
    for copy in copies:
        copy.wait()


def write_call(layer, layers, tiles, outs):
    cache = jax.ShapeDtypeStruct((layers, ROWS, KVD, SMAX), BF16)
    n_in = len(tiles)
    tiles = [pltpu.with_memory_space_constraint(x, pltpu.VMEM) for x in tiles]
    return pl.pallas_call(
        functools.partial(write_kernel, layer, n_in),
        out_shape=(cache, cache, jax.ShapeDtypeStruct((ROWS, D), BF16))[:n_in],
        in_specs=[VMEM] * n_in + [HBM] * len(outs),
        out_specs=(HBM,) * n_in,
        scratch_shapes=[pltpu.SemaphoreType.DMA((3, STEPS))],
        input_output_aliases={n_in: 0, n_in + 1: 1} if outs else {},
        compiler_params=pltpu.CompilerParams(vmem_limit_bytes=2 ** 20),
        name=f"write{layer}",
    )(*tiles, *outs)


def solution(mesh):
    cache_spec = P(None, "dp", None, "tp", None)
    col_spec = P(None, None, "tp")
    row_spec = P(None, "tp", None)
    in_specs = (P("dp", None), P("dp"), cache_spec, cache_spec, P(None, None), col_spec, col_spec, col_spec,
                row_spec, P(None, None), col_spec, col_spec, row_spec)
    out_specs = (P("dp", None), cache_spec, cache_spec)

    def local_step(hidden, seq_lens, k_cache, v_cache, g_attn, w_q, w_k, w_v, w_o, g_mlp, w_gate, w_up, w_down):
        layers = k_cache.shape[0]
        kt = k_cache.transpose(0, 1, 3, 4, 2).reshape(layers, ROWS, KVD, SMAX)
        vt = v_cache.transpose(0, 1, 3, 4, 2).reshape(layers, ROWS, KVD, SMAX)
        freq = jnp.asarray(np.tile(rope_freqs(HEAD), 4)[None, :])
        seq_row = seq_lens.reshape(1, ROWS)
        hidden, g_attn, w_q, w_k, w_v, w_o, g_mlp, w_gate, w_up, w_down, kt, vt, freq, seq_row = (
            pltpu.with_memory_space_constraint(x, pltpu.HBM)
            for x in (hidden, g_attn, w_q, w_k, w_v, w_o, g_mlp, w_gate, w_up, w_down, kt, vt, freq, seq_row))
        outs = ()
        qkv = (w_q, w_k, w_v)
        for layer in range(layers):
            hidden, k_tile, v_tile, *qkv = layer_call(layer, layer == 0, layer == layers - 1, seq_row, freq, hidden, g_attn, g_mlp, qkv,
                                                      (w_q, w_k, w_v), w_o, w_gate, w_up, w_down, kt, vt)
            if layer < layers - 1:
                outs = write_call(layer, layers, (k_tile, v_tile), outs)
                hidden, outs = lax.optimization_barrier((hidden, outs))
            else:
                *outs, hidden = write_call(layer, layers, (k_tile, v_tile, hidden), outs)

        def back(cache):
            return cache.reshape(layers, ROWS, 2, HEAD, SMAX).transpose(0, 1, 4, 2, 3)

        return hidden, back(outs[0]), back(outs[1])

    return jax.shard_map(local_step, mesh=mesh, in_specs=in_specs, out_specs=out_specs, check_vma=False)
```

```python
import functools

import jax
import jax.numpy as jnp
import numpy as np
from jax import lax
from jax.experimental import pallas as pl
from jax.experimental.pallas import tpu as pltpu
from jax.sharding import PartitionSpec as P

NORM_EPS = 1e-5
ROPE_THETA = 500000.0
ROPE_FACTOR = 8.0
LOW_FACTOR = 1.0
HIGH_FACTOR = 4.0
ORIG_CONTEXT = 8192.0

ROWS = 128
D = 2048
SMAX = 256
HEAD = 64
KVD = 128
QD = 512
FF = 2048
SEQS = 16
STEPS = ROWS // SEQS
CW = 512
NCH = D // CW
HALF = D // 2
RC = 32
NRC = ROWS // RC
AHEAD = 3
F32 = jnp.float32
BF16 = jnp.bfloat16
MESH = pl.DeviceIdType.MESH
VMEM = pl.BlockSpec(memory_space=pltpu.VMEM)
HBM = pl.BlockSpec(memory_space=pltpu.HBM)


def rope_freqs(head_dim):
    freq_expo = np.arange(0, head_dim, 2).astype(np.float32) / np.float32(head_dim)
    inv_freq = 1.0 / (ROPE_THETA ** freq_expo.astype(np.float64))
    wavelen = 2.0 * np.pi / inv_freq
    smooth = (ORIG_CONTEXT / wavelen - LOW_FACTOR) / (HIGH_FACTOR - LOW_FACTOR)
    blended = (1.0 - smooth) * inv_freq / ROPE_FACTOR + smooth * inv_freq
    return np.where(wavelen > ORIG_CONTEXT / LOW_FACTOR, inv_freq / ROPE_FACTOR,
                    np.where(wavelen < ORIG_CONTEXT / HIGH_FACTOR, inv_freq, blended)).astype(np.float32)


def norm_rows(hidden_f, gain):
    inv_rms = lax.rsqrt(jnp.mean(hidden_f * hidden_f, axis=-1, keepdims=True) + NORM_EPS)
    return (hidden_f * inv_rms * gain.astype(F32)).astype(BF16)


def rope_slab(slab, cos, sin):
    lane = lax.broadcasted_iota(jnp.int32, slab.shape, 1)
    other = jnp.where(lane % HEAD < HEAD // 2, pltpu.roll(slab, 128 - HEAD // 2, 1), pltpu.roll(slab, HEAD // 2, 1))
    return slab * cos + other * sin


def layer_kernel(layer, first, last, *refs):
    (seq_hbm, seqv_hbm, freq_hbm, h_in, ga_hbm, gm_hbm, wq_in, wk_in, wv_in, wo_hbm, wg_hbm, wu_hbm, wd_hbm, k_hbm, v_hbm) = refs[:15]
    refs = refs[15:]
    if not first:
        h_ref, wq, wk, wv = h_in, wq_in, wk_in, wv_in
    if not last:
        nq_hbm, nk_hbm, nv_hbm = (wq_in, wk_in, wv_in) if first else refs[:3]
        refs = refs if first else refs[3:]
    out_ref, kbuf, vbuf = refs[:3]
    refs = refs[3:]
    if not last:
        next_q, next_k, next_v = refs[:3]
        refs = refs[3:]
    if first:
        h_ref, wq, wk, wv = refs[:4]
        refs = refs[4:]
    (seq_ref, seqv, freq, ga, gm, wo, wg, wu, wd,
     knew, vnew, krow, vrow, qrow, orow, own1, send1, recv1, pair1, peer1, mid, send2, recv2, pair2, peer2, last2, act,
     sem, ksem, vsem, osem, wsem, nsem, sems1, sems2) = refs
    me = lax.axis_index("tp")
    core = lax.rem(me, 2)
    sibling = me + 1 - 2 * core
    peer = lax.rem(me + 2, 4)

    barrier = pltpu.get_barrier_semaphore()
    for other in (sibling, peer):
        pl.semaphore_signal(barrier, inc=1, device_id={"tp": other}, device_id_type=MESH)

    smalls = {0: (seqv_hbm, seqv), 1: (freq_hbm, freq), 3: (ga_hbm, ga), 7: (seq_hbm, seq_ref), 8: (gm_hbm, gm)}
    if first:
        smalls.update({2: (h_in, h_ref), 4: (wk_in.at[layer], wk), 5: (wv_in.at[layer], wv), 6: (wq_in.at[layer], wq)})

    class Small:
        def __init__(self, i):
            self.copy = pltpu.make_async_copy(*smalls[i], sem.at[i]) if i in smalls else None

        def start(self):
            if self.copy is not None:
                self.copy.start()

        def wait(self):
            if self.copy is not None:
                self.copy.wait()

    small = Small

    def load_next(i):
        src, dst = ((nq_hbm, next_q), (nk_hbm, next_k), (nv_hbm, next_v))[i]
        return pltpu.make_async_copy(src.at[layer + 1], dst, nsem.at[i])

    def load_k(i):
        return pltpu.make_async_copy(k_hbm.at[layer, pl.ds(i * SEQS, SEQS)], kbuf.at[pl.ds(i * SEQS, SEQS)], ksem.at[i])

    def load_v(i):
        return pltpu.make_async_copy(v_hbm.at[layer, pl.ds(i * SEQS, SEQS)], vbuf.at[pl.ds(i * SEQS, SEQS)], vsem.at[i])

    def load_o():
        return pltpu.make_async_copy(wo_hbm.at[layer], wo, osem.at[0])

    def load(kind, j):
        part = pl.ds(j * CW, CW)
        return pltpu.make_async_copy((wg_hbm, wu_hbm, wd_hbm)[kind].at[layer, part], (wg, wu, wd)[kind].at[part], wsem.at[kind, j])

    def half_cols(half):
        return pl.ds(pl.multiple_of(half * HALF, HALF), HALF)

    def remote(src, dst, sems, i, j, to):
        return pltpu.make_async_remote_copy(src_ref=src, dst_ref=dst, send_sem=sems.at[2 * i, j], recv_sem=sems.at[2 * i + 1, j],
                                            device_id={"tp": to}, device_id_type=MESH)

    for i in range(9):
        small(i).start()
    load_k(0).start()
    load_v(0).start()
    small(0).wait()
    small(1).wait()
    angle = jnp.broadcast_to(seqv[...].astype(F32), (ROWS, 128)).T * freq[...]
    cos = jnp.cos(angle)
    sin = jnp.sin(angle)
    lane = lax.broadcasted_iota(jnp.int32, (ROWS, 128), 1)
    sin = jnp.where(lane % HEAD < HEAD // 2, -sin, sin)
    small(2).wait()
    small(3).wait()
    normed = norm_rows(h_ref[...].astype(F32), ga[layer:layer + 1, :])
    small(4).wait()
    small(5).wait()
    load_k(1).start()
    load_v(1).start()
    k_row = rope_slab(jnp.dot(normed, wk[...], preferred_element_type=F32), cos, sin).astype(BF16).astype(F32)
    v_row = jnp.dot(normed, wv[...], preferred_element_type=F32).astype(BF16).astype(F32)
    krow[...] = k_row
    vrow[...] = v_row
    knew[...] = k_row.T
    vnew[...] = v_row.T
    small(6).wait()
    for slab_idx in range(4):
        slab = jnp.dot(normed, wq[:, slab_idx * 128:(slab_idx + 1) * 128], preferred_element_type=F32)
        slab = rope_slab(slab, cos, sin).astype(BF16).astype(F32)
        turned = pltpu.roll(slab, HEAD, 1)
        for half in range(2):
            hg = slab_idx * 2 + half
            kv = hg // 4
            qrow[pl.ds(hg, ROWS, stride=8), :] = jnp.where(lane // HEAD == kv, slab if kv == half else turned, 0.0)
    small(7).wait()
    small(8).wait()

    def attend(i):
        load_k(i).wait()
        load_v(i).wait()

        @pl.when(i == 0)
        def _():
            load_o().start()
            for n in range(2, AHEAD):
                load_k(n).start()
                load_v(n).start()

        @pl.when(i + AHEAD < STEPS)
        def _():
            load_k(i + AHEAD).start()
            load_v(i + AHEAD).start()

        lane8 = lax.broadcasted_iota(jnp.int32, (8, SMAX), 1)
        row16 = lax.broadcasted_iota(jnp.int32, (16, 128), 0)
        row8 = lax.broadcasted_iota(jnp.int32, (8, 128), 0)
        lane_o = lax.broadcasted_iota(jnp.int32, (8, 128), 1)
        scale = HEAD ** -0.5
        scores = []
        fresh = []
        for p in range(SEQS // 2):
            b = i * SEQS + 2 * p
            q2 = qrow[pl.ds(b * 8, 16), :]
            qb = jnp.concatenate([jnp.where(row16 < 8, q2, 0.0), jnp.where(row16 >= 8, q2, 0.0)], axis=1).astype(BF16)
            kk = kbuf[pl.ds(b, 2)].reshape(2 * KVD, SMAX)
            scores.append(jnp.dot(qb, kk, preferred_element_type=F32) * scale)
            for j in range(2):
                fresh.append(jnp.sum(q2[8 * j:8 * j + 8] * krow[pl.ds(b + j, 1), :], axis=-1, keepdims=True) * scale)
        for p in range(SEQS // 2):
            b = i * SEQS + 2 * p
            halves = []
            added = []
            for j in range(2):
                s = jnp.where(lane8 < seq_ref[0, b + j], scores[p][8 * j:8 * j + 8], -1e30)
                s_new = fresh[2 * p + j]
                peak = jnp.maximum(jnp.max(s, axis=-1, keepdims=True), s_new)
                e = jnp.exp(s - peak)
                e_new = jnp.exp(s_new - peak)
                denom = jnp.sum(e, axis=-1, keepdims=True) + e_new
                halves.append(e / denom)
                added.append((e_new / denom).astype(BF16).astype(F32) * vrow[pl.ds(b + j, 1), :])
            prob = jnp.concatenate(halves, axis=0).astype(BF16)
            vv = vbuf[pl.ds(b, 2)].reshape(2 * KVD, SMAX)
            mix = lax.dot_general(prob, vv, (((1,), (1,)), ((), ())), preferred_element_type=F32)
            for j in range(2):
                m = mix[8 * j:8 * j + 8, 128 * j:128 * j + 128] + added[j]
                orow[pl.ds((b + j) * 8, 8), :] = jnp.where((row8 < 4) == (lane_o < HEAD), m, pltpu.roll(m, HEAD, 1))

    def insert(i, carry):
        lane16 = lax.broadcasted_iota(jnp.int16, (KVD, SMAX), 1)
        shift = lax.rem(ROWS - i * SEQS, ROWS)
        for buf, new_ref in ((kbuf, knew), (vbuf, vnew)):
            new = pltpu.roll(new_ref[...], shift, 1)
            for j in range(SEQS):
                b = i * SEQS + j
                column = jnp.broadcast_to(new[:, j:j + 1], (KVD, 128)).astype(BF16)
                here = lane16 == seq_ref[0, b].astype(jnp.int16)
                buf[b] = jnp.where(here, jnp.concatenate([column, column], axis=1), buf[b])
        return carry

    def rows(rc):
        return pl.ds(pl.multiple_of(rc * RC, RC), RC)

    def copy1(rc):
        return remote(send1.at[rc], recv1.at[rc], sems1, 0, rc, sibling)

    def copy1_peer(rc):
        return remote(pair1.at[rc], peer1.at[rc], sems1, 1, rc, peer)

    def copy1_out(rc, half):
        return remote(mid.at[half, rows(rc)], mid.at[half, rows(rc)], sems1, 2, rc, sibling)

    def to_peer1(rc):
        copy1(rc).wait_recv()
        pair1[rc] = (own1[rc] + recv1[rc].astype(F32)).astype(BF16)
        copy1_peer(rc).start()

    def row_chunk(rc, carry):
        def step(i, c):
            @pl.when((i == RC // SEQS - 1) & (rc == 0))
            def _():
                pl.semaphore_wait(barrier, 2)

            attend(rc * (RC // SEQS) + i)

            @pl.when((i == 0) & (rc > 0))
            def _():
                to_peer1(rc - 1)

            return c

        lax.fori_loop(0, RC // SEQS, step, 0)
        parts = []
        lane_r = lax.broadcasted_iota(jnp.int32, (RC, 128), 1)
        for slab_idx in range(4):
            lower = orow[pl.ds(rc * RC * 8 + slab_idx * 2, RC, stride=8), :]
            upper = orow[pl.ds(rc * RC * 8 + slab_idx * 2 + 1, RC, stride=8), :]
            parts.append(jnp.where(lane_r < HEAD, lower, upper).astype(BF16))
        attn = jnp.concatenate(parts, axis=1)

        @pl.when(rc == 0)
        def _():
            load_o().wait()

        send1[rc] = jnp.dot(attn, wo[:, half_cols(1 - core)], preferred_element_type=F32).astype(BF16)
        copy1(rc).start()
        own1[rc] = jnp.dot(attn, wo[:, half_cols(core)], preferred_element_type=F32)

        @pl.when(rc == NRC - 2)
        def _():
            for j in range(NCH):
                load(0, j).start()
                load(1, j).start()

        return carry

    lax.fori_loop(0, NRC, row_chunk, 0)
    for j in range(NCH):
        load(2, j).start()
    if not last:
        for i in range(3):
            load_next(i).start()
    to_peer1(NRC - 1)
    for rc in range(NRC):
        copy1_peer(rc).wait_recv()
        total = pair1[rc].astype(F32) + peer1[rc].astype(F32)
        residual = h_ref[rc * RC:(rc + 1) * RC, half_cols(core)]
        mid[core, rc * RC:(rc + 1) * RC] = (residual.astype(F32) + total).astype(BF16)
        copy1_out(rc, core).start()
    for rc in range(NRC):
        copy1_out(rc, 1 - core).wait_recv()

    hidden = jnp.concatenate([mid[0], mid[1]], axis=1)
    normed = norm_rows(hidden.astype(F32), gm[layer:layer + 1, :])
    for j in range(NCH):
        load(0, j).wait()
        load(1, j).wait()
    for j in range(NCH):
        gate = jnp.dot(normed, wg[:, j * CW:(j + 1) * CW], preferred_element_type=F32)
        up = jnp.dot(normed, wu[:, j * CW:(j + 1) * CW], preferred_element_type=F32)
        act[:, j * CW:(j + 1) * CW] = (gate * jax.nn.sigmoid(gate) * up).astype(BF16)
    for j in range(NCH):
        load(2, j).wait()

    def copy2(j):
        return remote(send2.at[j], recv2.at[j], sems2, 0, j, sibling)

    def copy2_peer(j):
        return remote(pair2.at[j], peer2.at[j], sems2, 1, j, peer)

    def copy2_out(j, half):
        return remote(last2.at[half * 2 + j], last2.at[half * 2 + j], sems2, 2, j, sibling)

    def down(j):
        return jnp.dot(act[...], wd[:, pl.ds(pl.multiple_of(j * CW, CW), CW)], preferred_element_type=F32)

    def to_sibling2(j):
        send2[j] = down(2 - core * 2 + j).astype(BF16)
        copy2(j).start()

    def to_peer2(j, own):
        copy2(j).wait_recv()
        pair2[j] = (own + recv2[j].astype(F32)).astype(BF16)
        copy2_peer(j).start()

    to_sibling2(0)
    own = down(core * 2)
    to_sibling2(1)
    to_peer2(0, own)
    to_peer2(1, down(core * 2 + 1))
    lax.fori_loop(0, STEPS, insert, 0)
    for j in range(2):
        copy2_peer(j).wait_recv()
        total = pair2[j].astype(F32) + peer2[j].astype(F32)
        last2[core * 2 + j] = (mid[core, :, j * CW:(j + 1) * CW].astype(F32) + total).astype(BF16)
        copy2_out(j, core).start()
    for j in range(2):
        copy2_out(j, 1 - core).wait_recv()
    for j in range(NCH):
        out_ref[:, j * CW:(j + 1) * CW] = last2[j]
    if not last:
        for i in range(3):
            load_next(i).wait()
    for rc in range(NRC):
        copy1(rc).wait_send()
        copy1_peer(rc).wait_send()
        copy1_out(rc, core).wait_send()
    for j in range(2):
        copy2(j).wait_send()
        copy2_peer(j).wait_send()
        copy2_out(j, core).wait_send()


def layer_call(layer, first, last, seq_lens, freq, hidden, g_attn, g_mlp, qkv, w_next, w_o, w_gate, w_up, w_down, k_cache, v_cache):
    tile = pltpu.VMEM((ROWS, KVD, SMAX), BF16)
    chunk1 = pltpu.VMEM((NRC, RC, HALF), BF16)
    chunk2 = pltpu.VMEM((2, ROWS, CW), BF16)
    weights = [pltpu.VMEM((D, QD), BF16), pltpu.VMEM((D, KVD), BF16), pltpu.VMEM((D, KVD), BF16)]
    space = pltpu.HBM if first else pltpu.VMEM
    near = HBM if first else VMEM
    hidden, *qkv = (pltpu.with_memory_space_constraint(x, space) for x in (hidden, *qkv))
    handed = [] if last or first else list(w_next)
    return pl.pallas_call(
        functools.partial(layer_kernel, layer, first, last),
        out_shape=[pltpu.VMEM((ROWS, D), BF16), tile, tile] + ([] if last else weights),
        in_specs=[HBM] * 3 + [near] + [HBM] * 2 + [near] * 3 + [HBM] * (6 + len(handed)),
        out_specs=[VMEM] * (3 if last else 6),
        scratch_shapes=([pltpu.VMEM((ROWS, D), BF16)] + weights if first else []) + [
            pltpu.SMEM((1, ROWS), jnp.int32),
            pltpu.VMEM((1, ROWS), jnp.int32),
            pltpu.VMEM((1, 128), F32),
            pltpu.VMEM(g_attn.shape, BF16),
            pltpu.VMEM(g_mlp.shape, BF16),
            pltpu.VMEM((QD, D), BF16),
            pltpu.VMEM((D, FF), BF16),
            pltpu.VMEM((D, FF), BF16),
            pltpu.VMEM((FF, D), BF16),
            pltpu.VMEM((KVD, ROWS), F32),
            pltpu.VMEM((KVD, ROWS), F32),
            pltpu.VMEM((ROWS, KVD), F32),
            pltpu.VMEM((ROWS, KVD), F32),
            pltpu.VMEM((ROWS * 8, 128), F32),
            pltpu.VMEM((ROWS * 8, 128), F32),
            pltpu.VMEM((NRC, RC, HALF), F32),
            chunk1, chunk1, chunk1, chunk1,
            pltpu.VMEM((2, ROWS, HALF), BF16),
            chunk2, chunk2, chunk2, chunk2,
            pltpu.VMEM((NCH, ROWS, CW), BF16),
            pltpu.VMEM((ROWS, FF), BF16),
            pltpu.SemaphoreType.DMA((9,)),
            pltpu.SemaphoreType.DMA((STEPS,)),
            pltpu.SemaphoreType.DMA((STEPS,)),
            pltpu.SemaphoreType.DMA((1,)),
            pltpu.SemaphoreType.DMA((3, NCH)),
            pltpu.SemaphoreType.DMA((3,)),
            pltpu.SemaphoreType.DMA((6, NRC)),
            pltpu.SemaphoreType.DMA((6, 2)),
        ],
        compiler_params=pltpu.CompilerParams(vmem_limit_bytes=(38 if first else 35) * 2 ** 20, collective_id=layer, has_side_effects=True),
        name=f"layer{layer}",
    )(seq_lens, seq_lens, freq, hidden, g_attn, g_mlp, *qkv, w_o, w_gate, w_up, w_down, k_cache, v_cache, *handed)


def write_kernel(layer, n_in, *refs):
    sources, results, sem = refs[:n_in], refs[-1 - n_in:-1], refs[-1]
    copies = []
    for n in range(2):
        for i in range(STEPS):
            part = pl.ds(i * SEQS, SEQS)
            copies.append(pltpu.make_async_copy(sources[n].at[part], results[n].at[layer, part], sem.at[n, i]))
    if n_in > 2:
        copies.append(pltpu.make_async_copy(sources[2], results[2], sem.at[2, 0]))
    for copy in copies:
        copy.start()
    for copy in copies:
        copy.wait()


def write_call(layer, layers, tiles, outs):
    cache = jax.ShapeDtypeStruct((layers, ROWS, KVD, SMAX), BF16)
    n_in = len(tiles)
    tiles = [pltpu.with_memory_space_constraint(x, pltpu.VMEM) for x in tiles]
    return pl.pallas_call(
        functools.partial(write_kernel, layer, n_in),
        out_shape=(cache, cache, jax.ShapeDtypeStruct((ROWS, D), BF16))[:n_in],
        in_specs=[VMEM] * n_in + [HBM] * len(outs),
        out_specs=(HBM,) * n_in,
        scratch_shapes=[pltpu.SemaphoreType.DMA((3, STEPS))],
        input_output_aliases={n_in: 0, n_in + 1: 1} if outs else {},
        compiler_params=pltpu.CompilerParams(vmem_limit_bytes=2 ** 20),
        name=f"write{layer}",
    )(*tiles, *outs)


def solution(mesh):
    cache_spec = P(None, "dp", None, "tp", None)
    col_spec = P(None, None, "tp")
    row_spec = P(None, "tp", None)
    in_specs = (P("dp", None), P("dp"), cache_spec, cache_spec, P(None, None), col_spec, col_spec, col_spec,
                row_spec, P(None, None), col_spec, col_spec, row_spec)
    out_specs = (P("dp", None), cache_spec, cache_spec)

    def local_step(hidden, seq_lens, k_cache, v_cache, g_attn, w_q, w_k, w_v, w_o, g_mlp, w_gate, w_up, w_down):
        layers = k_cache.shape[0]
        kt = k_cache.transpose(0, 1, 3, 4, 2).reshape(layers, ROWS, KVD, SMAX)
        vt = v_cache.transpose(0, 1, 3, 4, 2).reshape(layers, ROWS, KVD, SMAX)
        freq = jnp.asarray(np.tile(rope_freqs(HEAD), 4)[None, :])
        seq_row = seq_lens.reshape(1, ROWS)
        hidden, g_attn, w_q, w_k, w_v, w_o, g_mlp, w_gate, w_up, w_down, kt, vt, freq, seq_row = (
            pltpu.with_memory_space_constraint(x, pltpu.HBM)
            for x in (hidden, g_attn, w_q, w_k, w_v, w_o, g_mlp, w_gate, w_up, w_down, kt, vt, freq, seq_row))
        outs = ()
        qkv = (w_q, w_k, w_v)
        for layer in range(layers):
            hidden, k_tile, v_tile, *qkv = layer_call(layer, layer == 0, layer == layers - 1, seq_row, freq, hidden, g_attn, g_mlp, qkv,
                                                      (w_q, w_k, w_v), w_o, w_gate, w_up, w_down, kt, vt)
            if layer < layers - 1:
                outs = write_call(layer, layers, (k_tile, v_tile), outs)
                hidden, outs = lax.optimization_barrier((hidden, outs))
            else:
                *outs, hidden = write_call(layer, layers, (k_tile, v_tile, hidden), outs)

        def back(cache):
            return cache.reshape(layers, ROWS, 2, HEAD, SMAX).transpose(0, 1, 4, 2, 3)

        return hidden, back(outs[0]), back(outs[1])

    return jax.shard_map(local_step, mesh=mesh, in_specs=in_specs, out_specs=out_specs, check_vma=False)
```
